32 devices in a mesh: radar: 4 (over x, core), tile: 8 (over z, y).
Axes of the slice: x: 2, y: 2, z: 4, core: 2. Of those that a mesh axis runs over, the one named last changes fastest.
Arguments:
- background: float32 [3, 128, 32, 1024], P(None, 'tile', None, 'radar'), may hold values from -6 to 6
- interp: bfloat16 [2048, 128, 128], P(('radar', 'tile')), may hold values from -0.5 to 0.5
- beam: bfloat16 [2048, 3, 128], P(('radar', 'tile')), may hold values from -1 to 1
- observed: bfloat16 [2048, 128], P(('radar', 'tile')), may hold values from -6 to 6
- cell_block: int32 [2048], P(('radar', 'tile')), may hold values from 0 to 1023
- sweep_count: int32 [32, 32], P(('radar', 'tile')), may hold values from 0 to 2, as said below
Outputs:
- wind_field: float32 [3, 128, 32, 1024], P(None, 'tile', None, 'radar')
- strain: float32 [6, 128, 32, 1024], P(None, 'tile', None, 'radar')
- cost_trace: float32 [2], replicated
The draws below stay inside these ranges and needn't reach their ends.
Inputs may be any that keep to these rules, and one draw needn't show every extreme that they name: `cell_block`: the cell block, within the owner's 16 x 32 x 256 cells of one component, read by a slot. `sweep_count`: every source device has an owning device to which all 2 of its slots are live.
All inputs are finite; a program needn't handle non-finite values.
Results may differ from the reference program's by a relative error of at most 0.0014.
Values may be sent and summed in bfloat16 or wider, within the bound.
No kernel may reach another device: no remote copies, remote signals or barrier semaphores. Data moves between devices by JAX's collectives and lax.ppermute only.
A program may use at most 64 MiB of HBM per device.

```python
import jax
import jax.numpy as jnp
from jax import lax

CX = 16
CY = 256
NZ = 32
GATE = 128
CAP = 2
ITERS = 2
NDEV = 32
BLOCKS = 2048
NX = 128
NY = 1024
N_RADAR = 4
N_TILE = 8


def draw_sweep_count(key, part):
    first_key, second_key = jax.random.split(jax.random.fold_in(key, 11))
    counts = jax.random.randint(first_key, (NDEV, NDEV), 0, CAP + 1)
    full_owner = jax.random.randint(second_key, (NDEV,), 0, NDEV)
    chosen = jnp.arange(NDEV)[None, :] == full_owner[:, None]
    return jnp.where(chosen, CAP, counts).astype(jnp.int32)


def set_ends(entries, rng, smallest, largest):
    longest = entries.shape.index(max(entries.shape))
    spots = []
    for shift in (0, 1):
        where = [jax.random.randint(jax.random.fold_in(rng, axis), (), 0, length) for axis, length in enumerate(entries.shape)]
        where[longest] = (where[longest] + shift) % entries.shape[longest]
        spots.append(tuple(where))
    return entries.at[spots[0]].set(smallest).at[spots[1]].set(largest)


def levels(own_key, dims, cuts, low, largest):
    loudness, own = 1.0, jax.random.fold_in(own_key, 6)
    for axis_at, parts in cuts:
        steps = jnp.exp(jax.random.uniform(jax.random.fold_in(own, axis_at), (parts,), jnp.float32, low / len(cuts), largest / len(cuts)))
        loudness = loudness * jnp.repeat(steps, dims[axis_at] // parts).reshape([-1 if axis == axis_at else 1 for axis in range(len(dims))])
    return loudness


def normal_values(own_key, dims, width, bound, shards=(), held_as=jnp.bfloat16):
    values = jax.random.normal(own_key, dims, jnp.float32) * width
    if len(shards) > 0:
        values = levels(own_key, dims, shards, -0.22, 0.18) * values
    return jnp.clip(values, min=-bound, max=bound).astype(held_as)


def setup_inputs(seed: int = 0) -> dict:
    streams_of = jax.random.split(jax.random.key(seed), 7)
    return {
        "background": normal_values(streams_of[0], (3, NX, NZ, NY), 1.0, 6.0, ((1, 8), (3, 4)), jnp.float32),
        "interp": normal_values(streams_of[1], (BLOCKS, GATE, GATE), GATE ** -0.5, 0.5, ((0, 32),)),
        "beam": jnp.clip(jax.random.uniform(streams_of[2], (BLOCKS, 3, GATE), jnp.float32, -1.0, 1.0) * levels(streams_of[2], (BLOCKS, 3, GATE), ((0, 32),), -0.4, 0.0), -1.0, 1.0).astype(jnp.bfloat16),
        "observed": normal_values(streams_of[3], (BLOCKS, GATE), 1.0, 6.0, ((0, 32),)),
        "cell_block": set_ends(jax.random.randint(streams_of[4], (BLOCKS,), 0, CX * NZ * CY // GATE), jax.random.fold_in(streams_of[4], 1), 0, (CX * NZ * CY // GATE) - 1).astype(jnp.int32),
        "sweep_count": draw_sweep_count(jax.random.fold_in(streams_of[6], 71), 0),
    }


BACKGROUND_WEIGHT = 0.5
DIVERGENCE_WEIGHT = 1.0
STEP_LENGTH = 0.3
EPSILON = 1e-06

def central(values, which_axis):
    extent = values.shape[which_axis]
    widths = [(0, 0)] * values.ndim
    widths[which_axis] = (1, 1)
    padded = jnp.pad(values, widths)
    upper_part = lax.slice_in_dim(padded, 2, extent + 2, axis=which_axis)
    lower_part = lax.slice_in_dim(padded, 0, extent, axis=which_axis)
    return 0.5 * (upper_part - lower_part)

def to_blocks(grid_field):
    blocked = grid_field.reshape(3, N_TILE, CX, NZ, N_RADAR, CY // GATE, GATE)
    blocked = blocked.transpose(4, 1, 0, 2, 3, 5, 6)
    return blocked.reshape(N_RADAR * N_TILE, 3, CX * NZ * (CY // GATE), GATE)

def from_blocks(blocked):
    shaped = blocked.reshape(N_RADAR, N_TILE, 3, CX, NZ, CY // GATE, GATE)
    shaped = shaped.transpose(2, 1, 3, 4, 0, 5, 6)
    return shaped.reshape(3, N_TILE * CX, NZ, N_RADAR * CY)

def observation_term(wind_field, interp, beam, observed, cell_block, sweep_count):
    devices = N_RADAR * N_TILE
    blocked = to_blocks(wind_field).astype(jnp.bfloat16)
    weights = interp.reshape(devices, devices, CAP, GATE, GATE)
    beam_rows = beam.reshape(devices, devices, CAP, 3, GATE)
    looked = observed.reshape(devices, devices, CAP, GATE)
    indices = cell_block.reshape(devices, devices, CAP).astype(jnp.int32)
    alive_mask = (jnp.arange(CAP, dtype=jnp.int32)[None, None, :] < sweep_count[:, :, None]).astype(jnp.float32)
    owners = jnp.arange(devices, dtype=jnp.int32)[:, None]

    def one_source(pieces):
        weight_src, beam_src, looked_src, index_src, alive_src = pieces
        cell_rows = lax.optimization_barrier(blocked[owners, :, index_src])
        weight_full = weight_src.astype(jnp.float32)
        projected = jnp.einsum('dskc,dsgc->dskg', cell_rows.astype(jnp.float32), weight_full)
        beam_values = beam_src.astype(jnp.float32)
        radial = lax.optimization_barrier(jnp.sum(beam_values * projected, axis=2))
        misfit = alive_src[..., None] * (radial - looked_src.astype(jnp.float32))
        adjoint = lax.optimization_barrier((beam_values * misfit[:, :, None, :]).astype(jnp.bfloat16))
        returned = jnp.einsum('dskg,dsgc->dskc', adjoint.astype(jnp.float32), weight_full)
        return (0.5 * jnp.sum(misfit * misfit), returned)
    misfit_cost, returned_all = lax.map(one_source, (weights, beam_rows, looked, indices, alive_mask))
    owner_index = jnp.broadcast_to(owners[None, :, :], indices.shape)
    gradient = jnp.zeros((devices, 3, CX * NZ * (CY // GATE), GATE), jnp.float32)
    gradient = gradient.at[owner_index, :, indices].add(returned_all)
    return (jnp.sum(misfit_cost), from_blocks(gradient))

def reference(background, interp, beam, observed, cell_block, sweep_count):
    wind_field = background
    trace = []
    for step_index in range(ITERS):
        obs_cost, obs_grad = observation_term(wind_field, interp, beam, observed, cell_block, sweep_count)
        spread = central(wind_field[0], 0) + central(wind_field[1], 2) + central(wind_field[2], 1)
        offset = wind_field - background
        push = jnp.stack([-central(spread, 0), -central(spread, 2), -central(spread, 1)])
        gradient = obs_grad + BACKGROUND_WEIGHT * offset + DIVERGENCE_WEIGHT * push
        total_cost = obs_cost + 0.5 * BACKGROUND_WEIGHT * jnp.sum(offset * offset) + 0.5 * DIVERGENCE_WEIGHT * jnp.sum(spread * spread)
        scale = jnp.sqrt(jnp.sum(gradient * gradient) / gradient.size + EPSILON)
        wind_field = wind_field - STEP_LENGTH * gradient / scale
        trace.append(total_cost / (N_RADAR * N_TILE * N_RADAR * N_TILE * CAP * GATE))
    east_wind, north_wind, upward_wind = (wind_field[0], wind_field[1], wind_field[2])
    strain = jnp.stack([central(east_wind, 0), central(north_wind, 2), central(upward_wind, 1), 0.5 * (central(east_wind, 2) + central(north_wind, 0)), 0.5 * (central(east_wind, 1) + central(upward_wind, 0)), 0.5 * (central(north_wind, 1) + central(upward_wind, 2))])
    return (wind_field, strain, jnp.stack(trace))
```

```python
import jax
import jax.numpy as jnp
from jax import lax
from jax.sharding import PartitionSpec as P

ITERS = 2


BACKGROUND_WEIGHT = 0.5
DIVERGENCE_WEIGHT = 1.0
STEP_LENGTH = 0.3
EPSILON = 1e-06


def with_halo(x, sides, width):
    for axis, dim in sides:
        size, length = (lax.axis_size(axis), x.shape[dim])
        up = [(i, (i + 1) % size) for i in range(size - 1)]
        down = [(j, i) for i, j in up]
        last = lax.slice_in_dim(x, length - width, length, axis=dim)
        first = lax.slice_in_dim(x, 0, width, axis=dim)
        before = lax.ppermute(last, axis, up)
        after = lax.ppermute(first, axis, down)
        x = jnp.concatenate([before, x, after], axis=dim)
    return x


def vertical_diff(values):
    padded = jnp.pad(values, ((0, 0), (1, 1), (0, 0)))
    return 0.5 * (padded[:, 2:, :] - padded[:, :-2, :])


def along_x(values):
    return 0.5 * (values[2:, :, 1:-1] - values[:-2, :, 1:-1])


def along_y(values):
    return 0.5 * (values[1:-1, :, 2:] - values[1:-1, :, :-2])


def along_z(values):
    return vertical_diff(values[1:-1, :, 1:-1])


def observe(cell_rows, weights, beam_rows, looked, alive_mask):
    projected = jnp.einsum("knc,ngc->nkg", cell_rows, weights, preferred_element_type=jnp.float32)
    beam_values = beam_rows.astype(jnp.float32)
    radial = jnp.sum(beam_values * projected, axis=1)
    misfit = alive_mask[:, None] * (radial - looked.astype(jnp.float32))
    adjoint = (beam_values * misfit[:, None, :]).astype(jnp.bfloat16)
    returned = jnp.einsum("nkg,ngc->knc", adjoint, weights, preferred_element_type=jnp.float32)
    return (0.5 * jnp.sum(misfit * misfit), returned)


def total_of(first, second, devices):
    lane = lax.broadcasted_iota(jnp.int32, (devices, 128), 1)
    row = jnp.where(lane == 0, first, jnp.where(lane == 1, second, 0.0))
    rows = lax.all_to_all(row, ("radar", "tile"), split_axis=0, concat_axis=0, tiled=True)
    sums = jnp.sum(rows, axis=0)
    return sums[0], sums[1]


def spread_cycle(wind_field, tile_count, radar_count):
    width_x = wind_field.shape[1]
    width_y = wind_field.shape[3]
    rim = with_halo(wind_field, (("radar", 3), ("tile", 1)), 2)
    cycle = along_x(rim[0]) + along_y(rim[1]) + along_z(rim[2])
    row_place = lax.axis_index("tile") * width_x - 1 + jnp.arange(width_x + 2, dtype=jnp.int32)
    col_place = lax.axis_index("radar") * width_y - 1 + jnp.arange(width_y + 2, dtype=jnp.int32)
    row_inside = (row_place >= 0) & (row_place < width_x * tile_count)
    col_inside = (col_place >= 0) & (col_place < width_y * radar_count)
    inside = row_inside[:, None, None] & col_inside[None, None, :]
    cycle = jnp.where(inside, cycle, 0.0)
    spread = cycle[1:-1, :, 1:-1]
    push = jnp.stack([-along_x(cycle), -along_y(cycle), -vertical_diff(spread)])
    return (spread, push)


def shards(background, interp, beam, observed, cell_block, sweep_count):
    radar_count = lax.axis_size("radar")
    tile_count = lax.axis_size("tile")
    devices = radar_count * tile_count
    width_x = background.shape[1]
    levels = background.shape[2]
    width_y = background.shape[3]
    slots = interp.shape[0] // devices
    gate_size = interp.shape[1]
    block_total = width_x * levels * width_y // gate_size
    total_cells = 3 * width_x * levels * width_y * devices
    total_gates = interp.shape[0] * devices * gate_size
    own_index = cell_block.reshape(devices, slots)
    own_alive = (
        jnp.arange(slots, dtype=jnp.int32)[None, :] < sweep_count.reshape(devices)[:, None]
    ).astype(jnp.int32)
    packed = jnp.stack([own_index, own_alive], 1)
    asked = lax.all_to_all(packed, ("radar", "tile"), split_axis=0, concat_axis=0, tiled=True)
    asked_index = asked[:, 0, :].reshape(-1)
    asked_alive = asked[:, 1, :].reshape(-1).astype(jnp.float32)
    got_weights, got_beam, got_looked = (
        lax.all_to_all(
            interp.reshape(devices, slots, gate_size, gate_size),
            ("radar", "tile"),
            split_axis=0,
            concat_axis=0,
            tiled=True,
        ),
        lax.all_to_all(
            beam.reshape(devices, slots, 3, gate_size),
            ("radar", "tile"),
            split_axis=0,
            concat_axis=0,
            tiled=True,
        ),
        lax.all_to_all(
            observed.reshape(devices, slots, gate_size),
            ("radar", "tile"),
            split_axis=0,
            concat_axis=0,
            tiled=True,
        ),
    )
    got_weights = got_weights.reshape(devices * slots, gate_size, gate_size)
    got_beam = got_beam.reshape(devices * slots, 3, gate_size)
    got_looked = got_looked.reshape(devices * slots, gate_size)
    wind_field = background
    trace = []
    for step_index in range(ITERS):
        flat = wind_field.reshape(3, block_total, gate_size)
        empty = jnp.zeros((3, block_total, gate_size), jnp.float32)
        chosen = flat[:, asked_index, :].astype(jnp.bfloat16)
        obs_cost, returned = observe(chosen, got_weights, got_beam, got_looked, asked_alive)
        obs_cost, obs_flat = (obs_cost, empty.at[:, asked_index, :].add(returned))
        obs_grad = obs_flat.reshape(wind_field.shape)
        spread, push = spread_cycle(wind_field, tile_count, radar_count)
        offset = wind_field - background
        gradient = obs_grad + BACKGROUND_WEIGHT * offset + DIVERGENCE_WEIGHT * push
        local_cost = (
            obs_cost
            + 0.5 * BACKGROUND_WEIGHT * jnp.sum(offset * offset)
            + 0.5 * DIVERGENCE_WEIGHT * jnp.sum(spread * spread)
        )
        cost_sum, square_sum = total_of(local_cost, jnp.sum(gradient * gradient), devices)
        scale = jnp.sqrt(square_sum / total_cells + EPSILON)
        wind_field = wind_field - STEP_LENGTH * gradient / scale
        trace.append(cost_sum / total_gates)
    faces = with_halo(wind_field, (("radar", 3), ("tile", 1)), 1)
    east_wind, north_wind, upward_wind = (faces[0], faces[1], faces[2])
    strain = jnp.stack(
        [
            along_x(east_wind),
            along_y(north_wind),
            along_z(upward_wind),
            0.5 * (along_y(east_wind) + along_x(north_wind)),
            0.5 * (along_z(east_wind) + along_x(upward_wind)),
            0.5 * (along_z(north_wind) + along_y(upward_wind)),
        ]
    )
    return (wind_field, strain, jnp.stack(trace))


def solution(mesh):
    placed = (
        P(None, "tile", None, "radar"),
        P(("radar", "tile"), None, None),
        P(("radar", "tile"), None, None),
        P(("radar", "tile"), None),
        P(("radar", "tile")),
        P(("radar", "tile"), None),
    )
    return jax.shard_map(
        shards,
        mesh=mesh,
        in_specs=placed,
        out_specs=(P(None, "tile", None, "radar"), P(None, "tile", None, "radar"), P()),
        check_vma=False,
    )
```

```python
import functools

import jax
import jax.numpy as jnp
from jax import lax
from jax.experimental import pallas as pl
from jax.experimental.pallas import tpu as pltpu
from jax.sharding import PartitionSpec as P

BACKGROUND_WEIGHT = 0.5
DIVERGENCE_WEIGHT = 1.0
STEP_LENGTH = 0.3
EPSILON = 1e-06

AXES = ("radar", "tile")
LANES = 128
F32 = jnp.float32
BF16 = jnp.bfloat16

COL_WY, COL_WX, COL_PART = 0, 1, 2
ROW_WX, ROW_PART, ROW_CORNER = 0, 1, 2


def exchange(x):
    return lax.all_to_all(x, AXES, split_axis=0, concat_axis=0, tiled=True)


def shifted(x, axis, step):
    size = lax.axis_size(axis)
    pairs = [(i, i + step) for i in range(size) if 0 <= i + step < size]
    return lax.ppermute(x, axis, pairs)


def iota(shape, dim):
    return lax.broadcasted_iota(jnp.int32, shape, dim)


def diff_levels(a, period):
    rows = a.shape[0]
    level = lax.rem(iota(a.shape, 0), jnp.int32(period))
    above = jnp.where(level == period - 1, 0.0, pltpu.roll(a, rows - 1, 0))
    below = jnp.where(level == 0, 0.0, pltpu.roll(a, 1, 0))
    return above - below


def diff_columns(a, left, right):
    width = a.shape[1]
    lane = iota(a.shape, 1)
    after = jnp.where(lane == width - 1, right, pltpu.roll(a, width - 1, 1))
    before = jnp.where(lane == 0, left, pltpu.roll(a, 1, 1))
    return after - before


def to_rows(columns):
    fill = jnp.zeros((LANES - columns.shape[0], columns.shape[1]), F32)
    return jnp.concatenate([columns, fill], axis=0).T


def from_fields(fields, rows):
    lane = iota((rows, LANES), 1)
    out = jnp.zeros((rows, LANES), F32)
    for f, field in enumerate(fields):
        out = jnp.where(lane == f, field, out)
    return out


def sum_rows(a):
    total = a[:, :LANES]
    for start in range(LANES, a.shape[1], LANES):
        total = total + a[:, start : start + LANES]
    return jnp.sum(total, axis=0, keepdims=True)


def own_place():
    return lax.axis_index("radar") * lax.axis_size("tile") + lax.axis_index("tile")


def block_at(index, runs):
    return lax.div(index, jnp.int32(runs)), lax.rem(index, jnp.int32(runs))


def read_block(ref, k, row, run):
    line = ref[k, pl.ds(row, 1), :]
    out = line[:, :LANES]
    for h in range(1, ref.shape[2] // LANES):
        out = jnp.where(run == h, line[:, h * LANES : (h + 1) * LANES], out)
    return out


def edge_columns(w_ref, left_out, right_out, scratch, levels):
    rows, width = w_ref.shape[1], w_ref.shape[2]
    cells = rows // levels
    for out, start, side in ((left_out, 0, 0), (right_out, width - LANES, 1)):
        lanes = slice(start, start + LANES)
        for x in range(cells):
            here = slice(x * levels, (x + 1) * levels)
            wx, wy, wz = (w_ref[k, here, lanes] for k in range(3))
            part = diff_levels(wz, levels)
            if x + 1 < cells:
                part = part + w_ref[0, (x + 1) * levels : (x + 2) * levels, lanes]
            if x > 0:
                part = part - w_ref[0, (x - 1) * levels : x * levels, lanes]
            if side == 0:
                part = 0.5 * (part[:, 0:1] + wy[:, 1:2])
                fields = (wy[:, 0:1], wx[:, 0:1], part)
            else:
                part = 0.5 * (part[:, LANES - 1 :] - wy[:, LANES - 2 : LANES - 1])
                fields = (wy[:, LANES - 1 :], wx[:, LANES - 1 :], part)
            scratch[here, :] = from_fields(fields, levels)
        out[...] = scratch[...].T[:8]


def edge_columns_kernel(levels, w_ref, left_out, right_out, scratch):
    edge_columns(w_ref, left_out, right_out, scratch, levels)


def edge_rows_kernel(levels, w_ref, left_ref, right_ref, up_out, down_out):
    rows, width = w_ref.shape[1], w_ref.shape[2]
    lane = iota((levels, width), 1)
    for out, first, tail in ((up_out, 0, False), (down_out, rows - levels, True)):
        here = slice(first, first + levels)
        base = first // LANES * LANES
        take = slice(first - base, first - base + levels)
        left = to_rows(left_ref[:, base : base + LANES])[take]
        right = to_rows(right_ref[:, base : base + LANES])[take]
        part = diff_levels(w_ref[2, here, :], levels)
        part = part + diff_columns(
            w_ref[1, here, :], left[:, COL_WY : COL_WY + 1], right[:, COL_WY : COL_WY + 1]
        )
        if tail:
            part = part - w_ref[0, first - levels : first, :]
        else:
            part = part + w_ref[0, levels : 2 * levels, :]
        out[ROW_WX] = w_ref[0, here, :]
        out[ROW_PART] = 0.5 * part
        out[ROW_CORNER] = jnp.where(
            lane == 0,
            left[:, COL_WX : COL_WX + 1],
            jnp.where(lane == width - 1, right[:, COL_WX : COL_WX + 1], 0.0),
        )


def cycle_kernel(levels, w_ref, left_ref, right_ref, above_ref, below_ref, push_out, spread_out, total_out, ring, left_rows, right_rows):
    rows, width = w_ref.shape[1], w_ref.shape[2]
    cells = rows // levels
    left_rows[...] = to_rows(left_ref[...])
    right_rows[...] = to_rows(right_ref[...])
    has_left = jnp.where(lax.axis_index("radar") > 0, 1.0, 0.0)
    has_right = jnp.where(lax.axis_index("radar") < lax.axis_size("radar") - 1, 1.0, 0.0)
    has_above = jnp.where(lax.axis_index("tile") > 0, 1.0, 0.0)
    has_below = jnp.where(lax.axis_index("tile") < lax.axis_size("tile") - 1, 1.0, 0.0)
    first, last = slice(0, levels), slice(rows - levels, rows)
    ring[0:levels, :] = has_above * (above_ref[ROW_PART] + 0.5 * w_ref[0, first, :])
    ring[rows + levels : rows + 2 * levels, :] = has_below * (below_ref[ROW_PART] - 0.5 * w_ref[0, last, :])
    total = jnp.zeros((levels, width), F32)
    for x in range(cells):
        here = slice(x * levels, (x + 1) * levels)
        after = w_ref[0, (x + 1) * levels : (x + 2) * levels, :] if x + 1 < cells else below_ref[ROW_WX]
        before = w_ref[0, (x - 1) * levels : x * levels, :] if x > 0 else above_ref[ROW_WX]
        spread = 0.5 * (
            (after - before)
            + diff_columns(
                w_ref[1, here, :],
                left_rows[here, COL_WY : COL_WY + 1],
                right_rows[here, COL_WY : COL_WY + 1],
            )
            + diff_levels(w_ref[2, here, :], levels)
        )
        ring[(x + 1) * levels : (x + 2) * levels, :] = spread
        spread_out[here, :] = spread
        total = total + spread * spread
    total_out[...] = jnp.broadcast_to(0.5 * DIVERGENCE_WEIGHT * sum_rows(total), total_out.shape)
    for x in range(cells):
        here = slice(x * levels, (x + 1) * levels)
        left = left_rows[here, COL_PART : COL_PART + 1] + 0.5 * w_ref[1, here, 0:1]
        right = right_rows[here, COL_PART : COL_PART + 1] - 0.5 * w_ref[1, here, width - 1 : width]
        if x == 0:
            left = left - 0.5 * above_ref[ROW_CORNER, :, 0:1]
            right = right - 0.5 * above_ref[ROW_CORNER, :, width - 1 : width]
        if x == cells - 1:
            left = left + 0.5 * below_ref[ROW_CORNER, :, 0:1]
            right = right + 0.5 * below_ref[ROW_CORNER, :, width - 1 : width]
        spread = ring[(x + 1) * levels : (x + 2) * levels, :]
        after = ring[(x + 2) * levels : (x + 3) * levels, :]
        before = ring[x * levels : (x + 1) * levels, :]
        push_out[0, here, :] = (-0.5 * DIVERGENCE_WEIGHT) * (after - before)
        push_out[1, here, :] = (-0.5 * DIVERGENCE_WEIGHT) * diff_columns(spread, has_left * left, has_right * right)
        push_out[2, here, :] = (-0.5 * DIVERGENCE_WEIGHT) * diff_levels(spread, levels)


def for_slots(count, body, step=4):
    def run(i, carry):
        for j in range(step):
            body(i * step + j)
        return carry

    lax.fori_loop(0, count // step, run, 0)


def pick_kernel(slots, asked_ref, w_ref, out_ref, rows_ref):
    me = own_place()
    runs = w_ref.shape[2] // LANES
    rows_ref[...] = jnp.zeros_like(rows_ref)

    def one(s):
        for p in range(slots):
            row, run = block_at(asked_ref[s, me * slots + p], runs)
            for k in range(3):
                rows_ref[s, 3 * p + k : 3 * p + k + 1, :] = read_block(w_ref, k, row, run)

    for_slots(out_ref.shape[0], one)
    out_ref[...] = rows_ref[...].astype(out_ref.dtype)


def project(cells_of, weights_ref, proj_ref, sources, slots, height):
    def one(s):
        weights = weights_ref[pl.ds(s * slots, slots)].reshape(slots * LANES, LANES)
        seen = lax.dot_general(cells_of(s), weights, (((1,), (1,)), ((), ())), preferred_element_type=F32)
        here = pl.ds(pl.multiple_of(s * height, height), height)
        for p in range(slots):
            proj_ref[p, here, :] = seen[:, p * LANES : (p + 1) * LANES]

    for_slots(sources, one)


def radial(proj_ref, sight_ref, p, sources, height):
    total = jnp.zeros((sources, LANES), F32)
    for k in range(3):
        total = total + sight_ref[3 * p + k] * proj_ref[p, pl.ds(3 * p + k, sources, stride=height), :]
    return total


def give_back(misfits, weights_ref, sight_ref, adj_ref, out_ref, sources, slots, height):
    adj_ref[...] = jnp.zeros_like(adj_ref)
    for p in range(slots):
        for k in range(3):
            adj_ref[p, pl.ds(3 * p + k, sources, stride=height), :] = sight_ref[3 * p + k] * misfits[p]

    def one(s):
        weights = weights_ref[pl.ds(s * slots, slots)].reshape(slots * LANES, LANES)
        here = pl.ds(pl.multiple_of(s * height, height), height)
        adjoint = jnp.concatenate([adj_ref[p, here, :] for p in range(slots)], axis=1).astype(BF16)
        out_ref[s] = lax.dot_general(adjoint, weights, (((1,), (0,)), ((), ())), preferred_element_type=F32)

    for_slots(sources, one)


def first_source_kernel(slots, cells_ref, weights_ref, sight_ref, returned_out, misfit_out, cost_out, proj_ref, adj_ref):
    sources, height = cells_ref.shape[0], cells_ref.shape[1]
    project(lambda s: cells_ref[s].astype(BF16), weights_ref, proj_ref, sources, slots, height)
    misfits = []
    cost = jnp.zeros((1, LANES), F32)
    for p in range(slots):
        misfit = radial(proj_ref, sight_ref, p, sources, height) - sight_ref[3 * slots + p]
        misfit_out[p] = misfit
        cost = cost + 0.5 * jnp.sum(misfit * misfit, axis=0, keepdims=True)
        misfits.append(misfit)
    cost_out[...] = jnp.broadcast_to(cost, cost_out.shape)
    give_back(misfits, weights_ref, sight_ref, adj_ref, returned_out, sources, slots, height)


def second_source_kernel(slots, total_cells, total_gates, got_ref, weights_ref, sight_ref, misfit_ref, returned_out, step_out, cost_out, done_out, proj_ref, adj_ref):
    sources, height = got_ref.shape[0], got_ref.shape[1]
    project(lambda s: got_ref[s].astype(BF16), weights_ref, proj_ref, sources, slots, height)
    squares = jnp.sum(got_ref[:, 3 * slots, :], axis=0, keepdims=True)
    squares = jnp.sum(squares, axis=1, keepdims=True)
    costs = jnp.sum(got_ref[:, 3 * slots + 1, :], axis=0, keepdims=True)
    costs = jnp.sum(costs, axis=1, keepdims=True)
    step = STEP_LENGTH / jnp.sqrt(squares / total_cells + EPSILON)
    step_out[...] = jnp.broadcast_to(step, step_out.shape)
    done_out[...] = jnp.broadcast_to(costs / total_gates, done_out.shape)
    misfits = []
    cost = jnp.zeros((1, LANES), F32)
    for p in range(slots):
        misfit = misfit_ref[p] - step * radial(proj_ref, sight_ref, p, sources, height)
        cost = cost + 0.5 * jnp.sum(misfit * misfit, axis=0, keepdims=True)
        misfits.append(misfit)
    cost_out[...] = jnp.broadcast_to(cost, cost_out.shape)
    give_back(misfits, weights_ref, sight_ref, adj_ref, returned_out, sources, slots, height)


def scatter_rows(slots, asked_ref, returned_ref, out_ref):
    me = own_place()
    runs = out_ref.shape[2] // LANES
    place = iota((8, LANES), 0)

    def one(s):
        for p in range(slots):
            row, run = block_at(asked_ref[s, me * slots + p], runs)
            within = lax.rem(row, jnp.int32(8))
            base = pl.multiple_of(row - within, 8)
            lanes = pl.ds(pl.multiple_of(run * LANES, LANES), LANES)
            for k in range(3):
                line = returned_ref[s, 3 * p + k : 3 * p + k + 1, :]
                out_ref[k, pl.ds(base, 8), lanes] += jnp.where(place == within, line, 0.0)

    for_slots(returned_ref.shape[0], one)


def square_sum(values_ref, levels):
    rows, width = values_ref.shape[1], values_ref.shape[2]
    total = jnp.zeros((levels, width), F32)
    for k in range(3):
        for x in range(rows // levels):
            piece = values_ref[k, x * levels : (x + 1) * levels, :]
            total = total + piece * piece
    return sum_rows(total)


def first_owner_kernel(slots, levels, asked_ref, returned_ref, push_ref, seen_cost_ref, spread_cost_ref, gradient_out, give_out, left_out, right_out, scratch):
    gradient_out[...] = push_ref[...]
    scatter_rows(slots, asked_ref, returned_ref, gradient_out)
    give_out[...] = jnp.zeros_like(give_out)
    me = own_place()
    runs = gradient_out.shape[2] // LANES

    def one(s):
        for p in range(slots):
            row, run = block_at(asked_ref[s, me * slots + p], runs)
            for k in range(3):
                give_out[s, 3 * p + k : 3 * p + k + 1, :] = read_block(gradient_out, k, row, run)

    for_slots(give_out.shape[0], one)
    sources = give_out.shape[0]
    give_out[:, 3 * slots, :] = jnp.broadcast_to(square_sum(gradient_out, levels), (sources, LANES))
    cost = seen_cost_ref[0:1, :] + spread_cost_ref[0:1, :]
    give_out[:, 3 * slots + 1, :] = jnp.broadcast_to(cost, (sources, LANES))
    edge_columns(gradient_out, left_out, right_out, scratch, levels)


def rest_kernel(levels, background_ref, gradient_ref, push_ref, bent_ref, spread_ref, bent_spread_ref, step_ref, rest_out, wind_out, cost_out):
    rows, width = gradient_ref.shape[1], gradient_ref.shape[2]
    step = step_ref[0:1, 0:1]
    offset_cost = jnp.zeros((levels, width), F32)
    spread_cost = jnp.zeros((levels, width), F32)
    for x in range(rows // levels):
        here = slice(x * levels, (x + 1) * levels)
        spread = spread_ref[here, :] - step * bent_spread_ref[here, :]
        spread_cost = spread_cost + spread * spread
        for k in range(3):
            offset = step * gradient_ref[k, here, :]
            offset_cost = offset_cost + offset * offset
            wind_out[k, here, :] = background_ref[k, here, :] - offset
            rest_out[k, here, :] = push_ref[k, here, :] - (BACKGROUND_WEIGHT * offset + step * bent_ref[k, here, :])
    cost = (0.5 * BACKGROUND_WEIGHT) * offset_cost + (0.5 * DIVERGENCE_WEIGHT) * spread_cost
    cost_out[...] = jnp.broadcast_to(sum_rows(cost), cost_out.shape)


def second_owner_kernel(slots, levels, asked_ref, returned_ref, rest_ref, wind_ref, seen_cost_ref, rest_cost_ref, gradient_out, give_out, up_out, down_out, left_out, right_out, scratch):
    gradient_out[...] = rest_ref[...]
    scatter_rows(slots, asked_ref, returned_ref, gradient_out)
    rows, width = gradient_out.shape[1], gradient_out.shape[2]
    half = LANES // 2
    squares = square_sum(gradient_out, levels)
    cost = seen_cost_ref[0:1, :] + rest_cost_ref[0:1, :]
    lane = iota((1, LANES), 1)
    squares = squares + pltpu.roll(squares, half, 1)
    cost = cost + pltpu.roll(cost, half, 1)
    give_out[...] = jnp.broadcast_to(jnp.where(lane < half, squares, cost), give_out.shape)
    for k in range(3):
        up_out[k] = wind_ref[k, 0:levels, :]
        up_out[3 + k] = gradient_out[k, 0:levels, :]
        down_out[k] = wind_ref[k, rows - levels : rows, :]
        down_out[3 + k] = gradient_out[k, rows - levels : rows, :]
    for out, column in ((left_out, 0), (right_out, width - 1)):
        for x in range(rows // levels):
            here = slice(x * levels, (x + 1) * levels)
            fields = [wind_ref[k, here, column : column + 1] for k in range(3)]
            fields += [gradient_out[k, here, column : column + 1] for k in range(3)]
            scratch[here, :] = from_fields(fields, levels)
        out[...] = scratch[...].T[:8]


def final_kernel(levels, total_cells, total_gates, sums_ref, first_cost_ref, wind_ref, gradient_ref, left_ref, right_ref, above_ref, below_ref, wind_out, strain_out, cost_out, left_rows, right_rows):
    rows, width = wind_ref.shape[1], wind_ref.shape[2]
    cells = rows // levels
    half = LANES // 2
    sums = jnp.sum(sums_ref[...], axis=0, keepdims=True)
    lane = iota((1, LANES), 1)
    squares = jnp.sum(jnp.where(lane < half, sums, 0.0), axis=1, keepdims=True)
    cost = jnp.sum(jnp.where(lane < half, 0.0, sums), axis=1, keepdims=True) / total_gates
    step = STEP_LENGTH / jnp.sqrt(squares / total_cells + EPSILON)
    out_lane = iota(cost_out.shape, 1)
    cost_out[...] = jnp.where(out_lane == 0, first_cost_ref[...], cost)
    left_rows[...] = to_rows(left_ref[...])
    right_rows[...] = to_rows(right_ref[...])
    for x in range(cells):
        here = slice(x * levels, (x + 1) * levels)
        for k in range(3):
            wind_out[k, here, :] = wind_ref[k, here, :] - step * gradient_ref[k, here, :]
    for x in range(cells):
        here = slice(x * levels, (x + 1) * levels)
        along = []
        for k in range(3):
            value = wind_out[k, here, :]
            if x + 1 < cells:
                after = wind_out[k, (x + 1) * levels : (x + 2) * levels, :]
            else:
                after = below_ref[k] - step * below_ref[3 + k]
            if x > 0:
                before = wind_out[k, (x - 1) * levels : x * levels, :]
            else:
                before = above_ref[k] - step * above_ref[3 + k]
            left = left_rows[here, k : k + 1] - step * left_rows[here, 3 + k : 4 + k]
            right = right_rows[here, k : k + 1] - step * right_rows[here, 3 + k : 4 + k]
            along.append((after - before, diff_columns(value, left, right), diff_levels(value, levels)))
        (xx, xy, xz), (yx, yy, yz), (zx, zy, zz) = along
        strain_out[0, here, :] = 0.5 * xx
        strain_out[1, here, :] = 0.5 * yy
        strain_out[2, here, :] = 0.5 * zz
        strain_out[3, here, :] = 0.25 * (xy + yx)
        strain_out[4, here, :] = 0.25 * (xz + zx)
        strain_out[5, here, :] = 0.25 * (yz + zy)


def shape(*dims, dtype=F32):
    return jax.ShapeDtypeStruct(dims, dtype)


VMEM = pl.BlockSpec(memory_space=pltpu.VMEM)
SMEM = pl.BlockSpec(memory_space=pltpu.SMEM)


def call(kernel, name, out_shape, args, scratch=(), scalars=0, flops=100000):
    return pl.pallas_call(
        kernel,
        name=name,
        out_shape=out_shape,
        in_specs=[SMEM] * scalars + [VMEM] * (len(args) - scalars),
        out_specs=jax.tree.map(lambda _: VMEM, out_shape),
        scratch_shapes=list(scratch),
        compiler_params=pltpu.CompilerParams(vmem_limit_bytes=32 * 1024 * 1024),
        cost_estimate=pl.CostEstimate(flops=flops, bytes_accessed=1 << 20, transcendentals=0),
    )(*args)


def shards(background, interp, beam, observed, cell_block, sweep_count):
    radar_count = lax.axis_size("radar")
    tile_count = lax.axis_size("tile")
    devices = radar_count * tile_count
    width_x, levels, width_y = background.shape[1:]
    slots = interp.shape[0] // devices
    gate_size = interp.shape[1]
    rows = width_x * levels
    height = -(-(3 * slots + 2) // 8) * 8
    total_cells = float(3 * rows * width_y * devices)
    total_gates = float(interp.shape[0] * devices * gate_size)
    field = background.reshape(3, rows, width_y)
    lanes = -(-devices * slots // LANES) * LANES
    line = jnp.pad(cell_block, (0, lanes - devices * slots))
    asked = exchange(jnp.broadcast_to(line[None, :], (devices, lanes)))

    live = (jnp.arange(slots, dtype=jnp.int32)[:, None, None] < sweep_count.reshape(1, devices, 1)).astype(F32)
    sight = beam.reshape(devices, slots, 3, gate_size).transpose(1, 2, 0, 3).astype(F32) * live[:, None]
    seen = observed.reshape(devices, slots, gate_size).transpose(1, 0, 2).astype(F32) * live
    sight = jnp.concatenate([sight.reshape(3 * slots, devices, gate_size), seen], axis=0)

    edges = (shape(8, rows), shape(8, rows))
    row_edges = (shape(3, levels, width_y), shape(3, levels, width_y))
    grid = shape(3, rows, width_y)
    line_out = shape(8, LANES)
    side = pltpu.VMEM((rows, LANES), F32)

    def cycle(values, sides):
        left = shifted(sides[1], "radar", 1)
        right = shifted(sides[0], "radar", -1)
        up, down = call(functools.partial(edge_rows_kernel, levels), "edge_rows", row_edges, (values, left, right))
        above = shifted(down, "tile", 1)
        below = shifted(up, "tile", -1)
        return call(
            functools.partial(cycle_kernel, levels),
            "cycle",
            (grid, shape(rows, width_y), line_out),
            (values, left, right, above, below),
            (pltpu.VMEM((rows + 2 * levels, width_y), F32), side, side),
        )

    sides = call(functools.partial(edge_columns_kernel, levels), "edge_columns", edges, (field,), (side,))
    push, spread, spread_cost = cycle(field, sides)

    cells = call(
        functools.partial(pick_kernel, slots),
        "pick",
        shape(devices, height, LANES, dtype=BF16),
        (asked, field),
        (pltpu.VMEM((devices, height, LANES), F32),),
        scalars=1,
    )
    cells = exchange(cells)
    products = (
        pltpu.VMEM((slots, devices * height, LANES), F32),
        pltpu.VMEM((slots, devices * height, LANES), F32),
    )
    returned, misfit, seen_cost = call(
        functools.partial(first_source_kernel, slots),
        "first_source",
        (shape(devices, height, LANES), shape(slots, devices, LANES), line_out),
        (cells, interp, sight),
        products,
    )
    returned = exchange(returned)
    gradient, give, left, right = call(
        functools.partial(first_owner_kernel, slots, levels),
        "first_owner",
        (grid, shape(devices, height, LANES)) + edges,
        (asked, returned, push, seen_cost, spread_cost),
        (side,),
        scalars=1,
    )
    got = exchange(give)
    bent, bent_spread, _ = cycle(gradient, (left, right))
    returned, step, seen_cost, first_cost = call(
        functools.partial(second_source_kernel, slots, total_cells, total_gates),
        "second_source",
        (shape(devices, height, LANES), line_out, line_out, line_out),
        (got, interp, sight, misfit),
        products,
    )
    returned = exchange(returned)
    rest, wind, rest_cost = call(
        functools.partial(rest_kernel, levels),
        "rest",
        (grid, grid, line_out),
        (field, gradient, push, bent, spread, bent_spread, step),
    )
    six_rows = (shape(6, levels, width_y), shape(6, levels, width_y))
    gradient, give, up, down, left, right = call(
        functools.partial(second_owner_kernel, slots, levels),
        "second_owner",
        (grid, shape(devices, LANES)) + six_rows + edges,
        (asked, returned, rest, wind, seen_cost, rest_cost),
        (side,),
        scalars=1,
    )
    sums = exchange(give)
    from_left = shifted(right, "radar", 1)
    from_right = shifted(left, "radar", -1)
    above = shifted(down, "tile", 1)
    below = shifted(up, "tile", -1)
    wind, strain, costs = call(
        functools.partial(final_kernel, levels, total_cells, total_gates),
        "final",
        (grid, shape(6, rows, width_y), line_out),
        (sums, first_cost, wind, gradient, from_left, from_right, above, below),
        (side, side),
    )
    return (
        wind.reshape(background.shape),
        strain.reshape(6, width_x, levels, width_y),
        costs[0, :2],
    )


def solution(mesh):
    placed = (
        P(None, "tile", None, "radar"),
        P(("radar", "tile"), None, None),
        P(("radar", "tile"), None, None),
        P(("radar", "tile"), None),
        P(("radar", "tile")),
        P(("radar", "tile"), None),
    )
    return jax.shard_map(
        shards,
        mesh=mesh,
        in_specs=placed,
        out_specs=(P(None, "tile", None, "radar"), P(None, "tile", None, "radar"), P()),
        check_vma=False,
    )
```

```python
import functools

import jax
import jax.numpy as jnp
from jax import lax
from jax.experimental import pallas as pl
from jax.experimental.pallas import tpu as pltpu
from jax.sharding import PartitionSpec as P


BACKGROUND_WEIGHT = 0.5
DIVERGENCE_WEIGHT = 1.0
STEP_LENGTH = 0.3
EPSILON = 1e-06

AXES = ("radar", "tile")
LANES = 128
PARTS = 4
F32 = jnp.float32
BF16 = jnp.bfloat16

COL_WY, COL_WX, COL_PART = 0, 1, 2
ROW_WX, ROW_PART = 0, 1
CORNERS = ((-1, -1), (-1, 1), (1, -1), (1, 1))


def exchange(x):
    return lax.all_to_all(x, AXES, split_axis=0, concat_axis=0, tiled=True)


def shifted(x, axis, step):
    size = lax.axis_size(axis)
    pairs = [(i, i + step) for i in range(size) if 0 <= i + step < size]
    return lax.ppermute(x, axis, pairs)


class Pieces:
    def __init__(self, source, target, sems, parts, at=0):
        rows = source.shape[-2]
        self.share = rows // parts
        self.copies = []
        self.seen = 0
        for i in range(parts):
            here = pl.ds(i * self.share, self.share)
            there = pl.ds(at + i * self.share, self.share)
            lead = (slice(None),) * (len(source.shape) - 2)
            self.copies.append(pltpu.make_async_copy(source.at[lead + (here,)], target.at[lead + (there,)], sems.at[i]))

    def start(self):
        for copy in self.copies:
            copy.start()
        return self

    def until(self, row):
        while self.seen < len(self.copies) and self.seen * self.share < row:
            self.copies[self.seen].wait()
            self.seen += 1

    def filled(self, row):
        while self.seen < len(self.copies) and (self.seen + 1) * self.share <= row:
            self.copies[self.seen].start()
            self.seen += 1

    def finish(self):
        for copy in self.copies:
            copy.wait()


class OutPieces(Pieces):
    def __init__(self, source, target, sems, parts, at=0):
        rows = target.shape[-2]
        self.share = rows // parts
        self.copies = []
        self.seen = 0
        for i in range(parts):
            here = pl.ds(at + i * self.share, self.share)
            there = pl.ds(i * self.share, self.share)
            lead = (slice(None),) * (len(source.shape) - 2)
            self.copies.append(pltpu.make_async_copy(source.at[lead + (here,)], target.at[lead + (there,)], sems.at[i]))


def iota(shape, dim):
    return lax.broadcasted_iota(jnp.int32, shape, dim)


def diff_levels(a, period):
    rows = a.shape[0]
    level = lax.rem(iota(a.shape, 0), jnp.int32(period))
    above = jnp.where(level == period - 1, 0.0, pltpu.roll(a, rows - 1, 0))
    below = jnp.where(level == 0, 0.0, pltpu.roll(a, 1, 0))
    return above - below


def diff_columns(a, left, right):
    width = a.shape[1]
    lane = iota(a.shape, 1)
    after = jnp.where(lane == width - 1, right, pltpu.roll(a, width - 1, 1))
    before = jnp.where(lane == 0, left, pltpu.roll(a, 1, 1))
    return after - before


def to_rows(columns):
    fill = jnp.zeros((LANES - columns.shape[0], columns.shape[1]), F32)
    return jnp.concatenate([columns, fill], axis=0).T


def sum_rows(a):
    total = a[:, :LANES]
    for start in range(LANES, a.shape[1], LANES):
        total = total + a[:, start : start + LANES]
    return jnp.sum(total, axis=0, keepdims=True)


def paired(first, second):
    half = LANES // 2
    lower = iota((1, LANES), 1) < half
    return jnp.where(lower, first + pltpu.roll(first, half, 1), second + pltpu.roll(second, half, 1))


def halves(line):
    lower = iota((1, LANES), 1) < LANES // 2
    return (
        jnp.sum(jnp.where(lower, line, 0.0), axis=1, keepdims=True),
        jnp.sum(jnp.where(lower, 0.0, line), axis=1, keepdims=True),
    )


def own_place():
    return lax.axis_index("radar") * lax.axis_size("tile") + lax.axis_index("tile")


def neighbour(along_tile, along_radar):
    tile = lax.axis_index("tile") + along_tile
    radar = lax.axis_index("radar") + along_radar
    exists = (tile >= 0) & (tile < lax.axis_size("tile")) & (radar >= 0) & (radar < lax.axis_size("radar"))
    return exists, jnp.where(exists, radar * lax.axis_size("tile") + tile, own_place())


def corner_lines(w_ref, levels):
    rows, width = w_ref.shape[1], w_ref.shape[2]
    lane = iota((levels, LANES), 1)
    packed = jnp.zeros((levels, LANES), F32)
    for c, (along_tile, along_radar) in enumerate(CORNERS):
        here = slice(0, levels) if along_tile < 0 else slice(rows - levels, rows)
        lanes, at = (slice(0, LANES), 0) if along_radar < 0 else (slice(width - LANES, width), LANES - 1)
        for k in range(2):
            packed = lane_column(packed, lane, w_ref[k, here, lanes], at, 2 * c + k)
    turned = jnp.concatenate([packed, jnp.zeros((LANES - levels, LANES), F32)], axis=0).T
    return [
        turned[2 * c : 2 * c + 1] + pltpu.roll(turned[2 * c + 1 : 2 * c + 2], levels, 1) for c in range(len(CORNERS))
    ]


def corner_columns(line_from, levels):
    lines = []
    for along_tile, along_radar in CORNERS:
        exists, place = neighbour(along_tile, along_radar)
        lines.append(jnp.where(exists, line_from(place), 0.0))
    fill = jnp.zeros((LANES - len(CORNERS), LANES), F32)
    turned = jnp.concatenate(lines + [fill], axis=0).T
    return [(turned[0:levels, c : c + 1], turned[levels : 2 * levels, c : c + 1]) for c in range(len(CORNERS))]


def block_at(index, runs):
    if runs & (runs - 1) == 0:
        return lax.shift_right_logical(index, jnp.int32(runs.bit_length() - 1)), index & (runs - 1)
    return lax.div(index, jnp.int32(runs)), lax.rem(index, jnp.int32(runs))


def read_block(ref, k, row, run):
    line = ref[k, pl.ds(row, 1), :]
    out = line[:, :LANES]
    for h in range(1, ref.shape[2] // LANES):
        out = jnp.where(run == h, line[:, h * LANES : (h + 1) * LANES], out)
    return out


def lane_column(packed, lane, tile, at, to):
    moved = tile if at == to else pltpu.roll(tile, (to - at) % LANES, 1)
    return jnp.where(lane == to, moved, packed)


def edges_kernel(levels, w_hbm, left_out, right_out, up_out, down_out, w_ref, scratch, sem):
    copy = pltpu.make_async_copy(w_hbm, w_ref, sem)
    copy.start()
    copy.wait()
    rows, width = w_ref.shape[1], w_ref.shape[2]
    lane = iota((levels, LANES), 1)
    last = slice(width - LANES, width)
    for x in range(rows // levels):
        here = slice(x * levels, (x + 1) * levels)
        packed = jnp.where(lane < LANES // 2, w_ref[1, here, :LANES], w_ref[1, here, last])
        packed = lane_column(packed, lane, w_ref[0, here, :LANES], 0, 2)
        packed = lane_column(packed, lane, w_ref[2, here, :LANES], 0, 3)
        packed = lane_column(packed, lane, w_ref[0, here, last], LANES - 1, LANES - 3)
        packed = lane_column(packed, lane, w_ref[2, here, last], LANES - 1, LANES - 4)
        scratch[here, :] = packed
    turned = scratch[...].T
    place = iota((1, rows), 1)
    level = lax.rem(place, jnp.int32(levels))

    def partial(wx, wz):
        part = jnp.where(level == levels - 1, 0.0, pltpu.roll(wz, rows - 1, 1))
        part = part - jnp.where(level == 0, 0.0, pltpu.roll(wz, 1, 1))
        part = part + jnp.where(place >= rows - levels, 0.0, pltpu.roll(wx, rows - levels, 1))
        return part - jnp.where(place < levels, 0.0, pltpu.roll(wx, levels, 1))

    near, far = turned[0:8], turned[LANES - 8 : LANES]
    for out, wy, inner, wx, wz in (
        (left_out, near[0:1], near[1:2], near[2:3], near[3:4]),
        (right_out, far[7:8], -far[6:7], far[5:6], far[4:5]),
    ):
        out[...] = jnp.zeros_like(out)
        out[COL_WY : COL_WY + 1, :] = wy
        out[COL_WX : COL_WX + 1, :] = wx
        out[COL_PART : COL_PART + 1, :] = 0.5 * (inner + partial(wx, wz))
    for out, first in ((up_out, 0), (down_out, rows - levels)):
        here = slice(first, first + levels)
        part = diff_levels(w_ref[2, here, :], levels) + diff_columns(w_ref[1, here, :], 0.0, 0.0)
        if first > 0:
            part = part - w_ref[0, first - levels : first, :]
        else:
            part = part + w_ref[0, levels : 2 * levels, :]
        out[ROW_WX] = w_ref[0, here, :]
        out[ROW_PART] = 0.5 * part


def cycle(levels, w_ref, left_ref, right_ref, above_ref, below_ref, corners, ring, left_rows, right_rows, need, take_spread, take_push):
    rows, width = w_ref.shape[1], w_ref.shape[2]
    cells = rows // levels
    left_rows[...] = to_rows(left_ref[...])
    right_rows[...] = to_rows(right_ref[...])
    has_left = jnp.where(lax.axis_index("radar") > 0, 1.0, 0.0)
    has_right = jnp.where(lax.axis_index("radar") < lax.axis_size("radar") - 1, 1.0, 0.0)
    has_above = jnp.where(lax.axis_index("tile") > 0, 1.0, 0.0)
    has_below = jnp.where(lax.axis_index("tile") < lax.axis_size("tile") - 1, 1.0, 0.0)
    above_left, above_right, below_left, below_right = corners
    lane = iota((levels, width), 1)

    def ends(left, right):
        return jnp.where(lane == 0, -0.5 * left, jnp.where(lane == width - 1, 0.5 * right, 0.0))

    first, last = slice(0, levels), slice(rows - levels, rows)
    for x in range(cells):
        here = slice(x * levels, (x + 1) * levels)
        need(min(rows, (x + 2) * levels))
        after = w_ref[0, (x + 1) * levels : (x + 2) * levels, :] if x + 1 < cells else below_ref[ROW_WX]
        before = w_ref[0, (x - 1) * levels : x * levels, :] if x > 0 else above_ref[ROW_WX]
        spread = 0.5 * (
            (after - before)
            + diff_columns(
                w_ref[1, here, :],
                left_rows[here, COL_WY : COL_WY + 1],
                right_rows[here, COL_WY : COL_WY + 1],
            )
            + diff_levels(w_ref[2, here, :], levels)
        )
        ring[(x + 1) * levels : (x + 2) * levels, :] = spread
        take_spread(here, spread)
    above = above_ref[ROW_PART] + 0.5 * w_ref[0, first, :] + ends(above_left[1], above_right[1])
    below = below_ref[ROW_PART] - 0.5 * w_ref[0, last, :] + ends(below_left[1], below_right[1])
    ring[0:levels, :] = has_above * above
    ring[rows + levels : rows + 2 * levels, :] = has_below * below
    for x in range(cells):
        here = slice(x * levels, (x + 1) * levels)
        left = left_rows[here, COL_PART : COL_PART + 1] + 0.5 * w_ref[1, here, 0:1]
        right = right_rows[here, COL_PART : COL_PART + 1] - 0.5 * w_ref[1, here, width - 1 : width]
        if x == 0:
            left = left - 0.5 * above_left[0]
            right = right - 0.5 * above_right[0]
        if x == cells - 1:
            left = left + 0.5 * below_left[0]
            right = right + 0.5 * below_right[0]
        spread = ring[(x + 1) * levels : (x + 2) * levels, :]
        after = ring[(x + 2) * levels : (x + 3) * levels, :]
        before = ring[x * levels : (x + 1) * levels, :]
        take_push(0, here, (-0.5 * DIVERGENCE_WEIGHT) * (after - before))
        take_push(1, here, (-0.5 * DIVERGENCE_WEIGHT) * diff_columns(spread, has_left * left, has_right * right))
        take_push(2, here, (-0.5 * DIVERGENCE_WEIGHT) * diff_levels(spread, levels))


def first_cycle_kernel(levels, slots, w_hbm, left_ref, right_ref, above_ref, below_ref, cells_ref, push_hbm, spread_hbm, total_out, w_ref, push, ring, left_rows, right_rows, total, sems):
    fields = Pieces(w_hbm, w_ref, sems.at[0], PARTS).start()
    total[...] = jnp.zeros_like(total)
    spreads = OutPieces(ring, spread_hbm, sems.at[1], PARTS, levels)
    pushes = OutPieces(push, push_hbm, sems.at[2], PARTS)

    def line_from(place):
        block = cells_ref[pl.ds(place, 1)].reshape(cells_ref.shape[1:]).astype(F32)
        first = block[3 * slots : 3 * slots + 1]
        return first + pltpu.roll(first, LANES // 2, 1) + block[3 * slots + 1 : 3 * slots + 2]

    def take_spread(here, spread):
        total[...] += spread * spread
        spreads.filled(here.stop)

    def take_push(k, here, value):
        push[k, here, :] = value
        if k == 2:
            pushes.filled(here.stop)

    corners = corner_columns(line_from, levels)
    cycle(levels, w_ref, left_ref, right_ref, above_ref, below_ref, corners, ring, left_rows, right_rows, fields.until, take_spread, take_push)
    total_out[...] = jnp.broadcast_to(0.5 * DIVERGENCE_WEIGHT * sum_rows(total[...]), total_out.shape)
    spreads.finish()
    pushes.finish()


def second_cycle_kernel(levels, slots, w_hbm, left_ref, right_ref, above_ref, below_ref, got_ref, background_hbm, push_hbm, spread_hbm, step_ref, rest_hbm, wind_hbm, total_out, w_ref, background, push, spread, ring, left_rows, right_rows, total, sems):
    fields = Pieces(w_hbm, w_ref, sems.at[0], PARTS).start()
    spreads = Pieces(spread_hbm, spread, sems.at[1], PARTS).start()
    pushes = Pieces(push_hbm, push, sems.at[2], PARTS).start()
    backgrounds = Pieces(background_hbm, background, sems.at[3], PARTS).start()
    rests = OutPieces(push, rest_hbm, sems.at[4], PARTS)
    winds = OutPieces(background, wind_hbm, sems.at[5], PARTS)
    total[...] = jnp.zeros_like(total)
    step = step_ref[0:1, 0:1]

    def line_from(place):
        return got_ref[place, 3 * slots + 1 : 3 * slots + 2, :]

    def take_spread(here, bent):
        spreads.until(here.stop)
        value = spread[here, :] - step * bent
        total[...] += (0.5 * DIVERGENCE_WEIGHT) * (value * value)

    def take_push(k, here, bent):
        pushes.until(here.stop)
        backgrounds.until(here.stop)
        offset = step * w_ref[k, here, :]
        total[...] += (0.5 * BACKGROUND_WEIGHT) * (offset * offset)
        background[k, here, :] = background[k, here, :] - offset
        push[k, here, :] = push[k, here, :] - (BACKGROUND_WEIGHT * offset + step * bent)
        if k == 2:
            rests.filled(here.stop)
            winds.filled(here.stop)

    corners = corner_columns(line_from, levels)
    cycle(levels, w_ref, left_ref, right_ref, above_ref, below_ref, corners, ring, left_rows, right_rows, fields.until, take_spread, take_push)
    total_out[...] = jnp.broadcast_to(sum_rows(total[...]), total_out.shape)
    rests.finish()
    winds.finish()


def for_slots(count, body, step=4):
    def run(i, carry):
        for j in range(step):
            body(i * step + j)
        return carry

    lax.fori_loop(0, count // step, run, 0)


def ask(asked_hbm, asked_ref, sem):
    return pltpu.make_async_copy(asked_hbm.at[:, 0, :], asked_ref, sem)


def pick_kernel(slots, levels, asked_hbm, w_ref, out_ref, rows_ref, asked_ref, ask_sem):
    asking = ask(asked_hbm, asked_ref, ask_sem)
    asking.start()
    me = own_place()
    runs = w_ref.shape[2] // LANES
    rows_ref[...] = jnp.zeros_like(rows_ref)
    asking.wait()

    def one(s):
        for p in range(slots):
            row, run = block_at(asked_ref[s, me * slots + p], runs)
            for k in range(3):
                rows_ref[s, 3 * p + k : 3 * p + k + 1, :] = read_block(w_ref, k, row, run)

    for_slots(out_ref.shape[0], one)
    for (along_tile, along_radar), line in zip(CORNERS, corner_lines(w_ref, levels)):
        exists, place = neighbour(along_tile, along_radar)
        high = line.astype(BF16).astype(F32)
        middle = (line - high).astype(BF16).astype(F32)

        @pl.when(exists)
        def _():
            rows_ref[place, 3 * slots : 3 * slots + 1, :] = high + pltpu.roll(middle, LANES // 2, 1)
            rows_ref[place, 3 * slots + 1 : 3 * slots + 2, :] = line - high - middle

    out_ref[...] = rows_ref[...].astype(out_ref.dtype)


def project(cells_of, weights_ref, proj_ref, sources, slots, height):
    def one(s):
        weights = weights_ref[pl.ds(s * slots, slots)].reshape(slots * LANES, LANES)
        seen = lax.dot_general(cells_of(s), weights, (((1,), (1,)), ((), ())), preferred_element_type=F32)
        here = pl.ds(pl.multiple_of(s * height, height), height)
        for p in range(slots):
            proj_ref[p, here, :] = seen[:, p * LANES : (p + 1) * LANES]

    for_slots(sources, one)


def radial(proj_ref, sight_ref, p, sources, height):
    total = jnp.zeros((sources, LANES), F32)
    for k in range(3):
        total = total + sight_ref[3 * p + k] * proj_ref[p, pl.ds(3 * p + k, sources, stride=height), :]
    return total


def give_back(misfits, weights_ref, sight_ref, adj_ref, out_ref, sources, slots, height):
    adj_ref[...] = jnp.zeros_like(adj_ref)
    for p in range(slots):
        for k in range(3):
            adj_ref[p, pl.ds(3 * p + k, sources, stride=height), :] = sight_ref[3 * p + k] * misfits[p]

    def one(s):
        weights = weights_ref[pl.ds(s * slots, slots)].reshape(slots * LANES, LANES)
        here = pl.ds(pl.multiple_of(s * height, height), height)
        adjoint = jnp.concatenate([adj_ref[p, here, :] for p in range(slots)], axis=1).astype(BF16)
        out_ref[s] = lax.dot_general(adjoint, weights, (((1,), (0,)), ((), ())), preferred_element_type=F32)

    for_slots(sources, one)


def first_source_kernel(slots, cells_ref, weights_ref, sight_ref, returned_out, misfit_out, cost_out, proj_ref, adj_ref):
    sources, height = cells_ref.shape[0], cells_ref.shape[1]
    project(lambda s: cells_ref[s].astype(BF16), weights_ref, proj_ref, sources, slots, height)
    misfits = []
    cost = jnp.zeros((1, LANES), F32)
    for p in range(slots):
        misfit = radial(proj_ref, sight_ref, p, sources, height) - sight_ref[3 * slots + p]
        misfit_out[p] = misfit
        cost = cost + 0.5 * jnp.sum(misfit * misfit, axis=0, keepdims=True)
        misfits.append(misfit)
    cost_out[...] = jnp.broadcast_to(cost, cost_out.shape)
    give_back(misfits, weights_ref, sight_ref, adj_ref, returned_out, sources, slots, height)


def second_source_kernel(slots, total_cells, total_gates, got_ref, weights_ref, sight_ref, misfit_ref, returned_out, step_out, cost_out, done_out, proj_ref, adj_ref):
    sources, height = got_ref.shape[0], got_ref.shape[1]
    project(lambda s: got_ref[s].astype(BF16), weights_ref, proj_ref, sources, slots, height)
    squares, costs = halves(jnp.sum(got_ref[:, 3 * slots, :], axis=0, keepdims=True))
    step = STEP_LENGTH / jnp.sqrt(squares / total_cells + EPSILON)
    step_out[...] = jnp.broadcast_to(step, step_out.shape)
    done_out[...] = jnp.broadcast_to(costs / total_gates, done_out.shape)
    misfits = []
    cost = jnp.zeros((1, LANES), F32)
    for p in range(slots):
        misfit = misfit_ref[p] - step * radial(proj_ref, sight_ref, p, sources, height)
        cost = cost + 0.5 * jnp.sum(misfit * misfit, axis=0, keepdims=True)
        misfits.append(misfit)
    cost_out[...] = jnp.broadcast_to(cost, cost_out.shape)
    give_back(misfits, weights_ref, sight_ref, adj_ref, returned_out, sources, slots, height)


def scatter_rows(slots, asked_ref, returned_ref, out_ref):
    me = own_place()
    runs = out_ref.shape[2] // LANES
    place = iota((8, LANES), 0)

    def one(s):
        for p in range(slots):
            row, run = block_at(asked_ref[s, me * slots + p], runs)
            within = lax.rem(row, jnp.int32(8))
            base = pl.multiple_of(row - within, 8)
            lanes = pl.ds(pl.multiple_of(run * LANES, LANES), LANES)
            held = [out_ref[k, pl.ds(base, 8), lanes] for k in range(3)]
            for k in range(3):
                line = returned_ref[s, 3 * p + k : 3 * p + k + 1, :]
                held[k] = held[k] + jnp.where(place == within, line, 0.0)
            for k in range(3):
                out_ref[k, pl.ds(base, 8), lanes] = held[k]

    for_slots(returned_ref.shape[0], one)


def gather_gradient(slots, levels, asked_hbm, asked_ref, returned_ref, rest_hbm, rest, gradient_ref, gradient_hbm, sems):
    rows, width = gradient_ref.shape[1], gradient_ref.shape[2]
    cells = rows // levels
    copy = pltpu.make_async_copy(rest_hbm, rest, sems.at[cells])
    asking = ask(asked_hbm, asked_ref, sems.at[cells + 1])
    asking.start()
    copy.start()
    gradient_ref[...] = jnp.zeros_like(gradient_ref)
    asking.wait()
    scatter_rows(slots, asked_ref, returned_ref, gradient_ref)
    copy.wait()
    total = jnp.zeros((levels, width), F32)
    copies = []
    for x in range(cells):
        here = slice(x * levels, (x + 1) * levels)
        for k in range(3):
            piece = gradient_ref[k, here, :] + rest[k, here, :]
            gradient_ref[k, here, :] = piece
            total = total + piece * piece
        if gradient_hbm is not None:
            copies.append(pltpu.make_async_copy(gradient_ref.at[:, here], gradient_hbm.at[:, here], sems.at[x]))
            copies[-1].start()
    return sum_rows(total), copies


def first_owner_kernel(slots, levels, asked_hbm, returned_ref, push_hbm, seen_cost_ref, spread_cost_ref, gradient_hbm, give_out, push, gradient, asked_ref, sems):
    squares, copies = gather_gradient(
        slots, levels, asked_hbm, asked_ref, returned_ref, push_hbm, push, gradient, gradient_hbm, sems
    )
    sources = give_out.shape[0]
    sums = paired(squares, seen_cost_ref[0:1, :] + spread_cost_ref[0:1, :])
    give_out[...] = jnp.zeros_like(give_out)
    give_out[:, 3 * slots, :] = jnp.broadcast_to(sums, (sources, LANES))
    me = own_place()
    runs = gradient.shape[2] // LANES

    def one(s):
        for p in range(slots):
            row, run = block_at(asked_ref[s, me * slots + p], runs)
            for k in range(3):
                give_out[s, 3 * p + k : 3 * p + k + 1, :] = read_block(gradient, k, row, run)

    for_slots(sources, one)
    for (along_tile, along_radar), line in zip(CORNERS, corner_lines(gradient, levels)):
        exists, place = neighbour(along_tile, along_radar)

        @pl.when(exists)
        def _():
            give_out[place, 3 * slots + 1 : 3 * slots + 2, :] = line

    for copy in copies:
        copy.wait()


def second_owner_kernel(slots, levels, asked_hbm, returned_ref, rest_hbm, seen_cost_ref, rest_cost_ref, gradient_out, give_out, rest, asked_ref, sems):
    squares, _ = gather_gradient(
        slots, levels, asked_hbm, asked_ref, returned_ref, rest_hbm, rest, gradient_out, None, sems
    )
    sums = paired(squares, seen_cost_ref[0:1, :] + rest_cost_ref[0:1, :])
    give_out[...] = jnp.broadcast_to(sums, give_out.shape)


def final_edges_kernel(levels, wind_ref, gradient_ref, up_out, down_out, left_out, right_out, scratch):
    rows, width = wind_ref.shape[1], wind_ref.shape[2]
    fields = [(wind_ref, k) for k in range(3)] + [(gradient_ref, k) for k in range(3)]
    for f, (ref, k) in enumerate(fields):
        up_out[f] = ref[k, 0:levels, :]
        down_out[f] = ref[k, rows - levels : rows, :]
    lane = iota((levels, LANES), 1)
    for x in range(rows // levels):
        here = slice(x * levels, (x + 1) * levels)
        packed = jnp.zeros((levels, LANES), F32)
        for f, (ref, k) in enumerate(fields):
            packed = lane_column(packed, lane, ref[k, here, :LANES], 0, f)
            packed = lane_column(packed, lane, ref[k, here, width - LANES :], LANES - 1, LANES - 8 + f)
        scratch[here, :] = packed
    turned = scratch[...].T
    left_out[...] = turned[0:8]
    right_out[...] = turned[LANES - 8 : LANES]


def final_kernel(levels, total_cells, total_gates, sums_ref, first_cost_ref, wind_hbm, gradient_ref, left_ref, right_ref, above_ref, below_ref, wind_out, strain_out, cost_out, left_rows, right_rows, wind, strain, sems):
    rows = gradient_ref.shape[1]
    cells = rows // levels
    winds = Pieces(wind_hbm, wind, sems.at[0], PARTS).start()
    wind_outs = OutPieces(wind, wind_out, sems.at[1], PARTS)
    strain_outs = OutPieces(strain, strain_out, sems.at[2], PARTS)
    squares, cost = halves(jnp.sum(sums_ref[:, 0, :], axis=0, keepdims=True))
    cost = cost / total_gates
    step = STEP_LENGTH / jnp.sqrt(squares / total_cells + EPSILON)
    out_lane = iota(cost_out.shape, 1)
    cost_out[...] = jnp.where(out_lane == 0, first_cost_ref[...], cost)
    left_rows[...] = to_rows(left_ref[...])
    right_rows[...] = to_rows(right_ref[...])

    def settle(x):
        here = slice(x * levels, (x + 1) * levels)
        winds.until(here.stop)
        for k in range(3):
            wind[k, here, :] = wind[k, here, :] - step * gradient_ref[k, here, :]
        wind_outs.filled(here.stop)

    settle(0)
    for x in range(cells):
        here = slice(x * levels, (x + 1) * levels)
        if x + 1 < cells:
            settle(x + 1)
        along = []
        for k in range(3):
            value = wind[k, here, :]
            if x + 1 < cells:
                after = wind[k, (x + 1) * levels : (x + 2) * levels, :]
            else:
                after = below_ref[k] - step * below_ref[3 + k]
            if x > 0:
                before = wind[k, (x - 1) * levels : x * levels, :]
            else:
                before = above_ref[k] - step * above_ref[3 + k]
            left = left_rows[here, k : k + 1] - step * left_rows[here, 3 + k : 4 + k]
            right = right_rows[here, k : k + 1] - step * right_rows[here, 3 + k : 4 + k]
            along.append((after - before, diff_columns(value, left, right), diff_levels(value, levels)))
        (xx, xy, xz), (yx, yy, yz), (zx, zy, zz) = along
        strain[0, here, :] = 0.5 * xx
        strain[1, here, :] = 0.5 * yy
        strain[2, here, :] = 0.5 * zz
        strain[3, here, :] = 0.25 * (xy + yx)
        strain[4, here, :] = 0.25 * (xz + zx)
        strain[5, here, :] = 0.25 * (yz + zy)
        strain_outs.filled(here.stop)
    wind_outs.finish()
    strain_outs.finish()


def shape(*dims, dtype=F32):
    return jax.ShapeDtypeStruct(dims, dtype)


VMEM = pl.BlockSpec(memory_space=pltpu.VMEM)
SMEM = pl.BlockSpec(memory_space=pltpu.SMEM)
ANY = pl.BlockSpec(memory_space=pl.ANY)


def call(kernel, out_shape, args, scratch=(), scalars=0, raw=(), out_raw=(), chip=(), out_chip=(), flops=2000000, limit=16):
    single = not isinstance(out_shape, tuple)
    outs = (out_shape,) if single else out_shape
    held = [
        x if i < scalars or i in chip else pltpu.with_memory_space_constraint(x, pltpu.HBM)
        for i, x in enumerate(args)
    ]
    placed = tuple(o if i in out_chip else pltpu.HBM(o.shape, o.dtype) for i, o in enumerate(outs))
    specs = tuple(ANY if i in out_raw else VMEM for i in range(len(outs)))
    return pl.pallas_call(
        kernel,
        out_shape=placed[0] if single else placed,
        in_specs=[SMEM if i < scalars else ANY if i in raw else VMEM for i in range(len(args))],
        out_specs=specs[0] if single else specs,
        scratch_shapes=list(scratch),
        compiler_params=pltpu.CompilerParams(vmem_limit_bytes=limit * 1024 * 1024),
        cost_estimate=pl.CostEstimate(flops=flops, bytes_accessed=1 << 20, transcendentals=0),
    )(*held)


def shards(background, interp, beam, observed, cell_block, sweep_count):
    radar_count = lax.axis_size("radar")
    tile_count = lax.axis_size("tile")
    devices = radar_count * tile_count
    width_x, levels, width_y = background.shape[1:]
    slots = interp.shape[0] // devices
    gate_size = interp.shape[1]
    rows = width_x * levels
    height = -(-(3 * slots + 2) // 8) * 8
    total_cells = float(3 * rows * width_y * devices)
    total_gates = float(interp.shape[0] * devices * gate_size)
    field = background.reshape(3, rows, width_y)
    lanes = -(-devices * slots // LANES) * LANES
    line = jnp.pad(cell_block, (0, lanes - devices * slots))
    asked = exchange(jnp.broadcast_to(line[None, None, :], (devices, 8, lanes)))

    live = (jnp.arange(slots, dtype=jnp.int32)[:, None, None] < sweep_count.reshape(1, devices, 1)).astype(F32)
    sight = beam.reshape(devices, slots, 3, gate_size).transpose(1, 2, 0, 3).astype(F32) * live[:, None]
    seen = observed.reshape(devices, slots, gate_size).transpose(1, 0, 2).astype(F32) * live
    sight = jnp.concatenate([sight.reshape(3 * slots, devices, gate_size), seen], axis=0)

    edges = (shape(8, rows), shape(8, rows))
    row_edges = (shape(2, levels, width_y), shape(2, levels, width_y))
    grid = shape(3, rows, width_y)
    line_out = shape(8, LANES)
    side = pltpu.VMEM((rows, LANES), F32)
    whole = pltpu.VMEM((3, rows, width_y), F32)
    plane = pltpu.VMEM((rows, width_y), F32)
    ring = pltpu.VMEM((rows + 2 * levels, width_y), F32)
    strip = pltpu.VMEM((levels, width_y), F32)
    semaphores = pltpu.SemaphoreType.DMA
    places = pltpu.SMEM((devices, lanes), jnp.int32)

    def halo(left, right, up, down):
        from_left = shifted(right, "radar", 1)
        from_right = shifted(left, "radar", -1)
        above = shifted(down, "tile", 1)
        below = shifted(up, "tile", -1)
        return from_left, from_right, above, below

    def edges_of(values):
        out = call(
            functools.partial(edges_kernel, levels), edges + row_edges, (values,), (whole, side, semaphores), raw=(0,)
        )
        return halo(*out)

    around = edges_of(field)
    cells = call(
        functools.partial(pick_kernel, slots, levels),
        shape(devices, height, LANES, dtype=BF16),
        (asked, field),
        (pltpu.VMEM((devices, height, LANES), F32), places, semaphores),
        chip=(0, 1),
        raw=(0,),
    )
    cells = exchange(cells)
    products = (
        pltpu.VMEM((slots, devices * height, LANES), F32),
        pltpu.VMEM((slots, devices * height, LANES), F32),
    )
    returned, misfit, seen_cost = call(
        functools.partial(first_source_kernel, slots),
        (shape(devices, height, LANES), shape(slots, devices, LANES), line_out),
        (cells, interp, sight),
        products,
        chip=(0, 1, 2),
        out_chip=(1, 2),
    )
    returned = exchange(returned)
    push, spread, spread_cost = call(
        functools.partial(first_cycle_kernel, levels, slots),
        (grid, shape(rows, width_y), line_out),
        (field,) + around + (cells,),
        (whole, whole, ring, side, side, strip, semaphores((3, PARTS))),
        chip=(1, 2, 3, 4, 5),
        raw=(0,),
        out_raw=(0, 1),
    )
    gradient, give = call(
        functools.partial(first_owner_kernel, slots, levels),
        (grid, shape(devices, height, LANES)),
        (asked, returned, push, seen_cost, spread_cost),
        (whole, whole, places, semaphores((width_x + 2,))),
        chip=(0, 1),
        raw=(0, 2),
        out_raw=(0,),
    )
    got = exchange(give)
    around = edges_of(gradient)
    returned, step, seen_cost, first_cost = call(
        functools.partial(second_source_kernel, slots, total_cells, total_gates),
        (shape(devices, height, LANES), line_out, line_out, line_out),
        (got, interp, sight, misfit),
        products,
        chip=(0, 1, 2, 3),
        out_chip=(1, 2, 3),
    )
    returned = exchange(returned)
    rest, wind, rest_cost = call(
        functools.partial(second_cycle_kernel, levels, slots),
        (grid, grid, line_out),
        (gradient,) + around + (got, field, push, spread, step),
        (whole, whole, whole, plane, ring, side, side, strip, semaphores((6, PARTS))),
        chip=(1, 2, 3, 4, 5, 9),
        raw=(0, 6, 7, 8),
        out_raw=(0, 1),
        out_chip=(2,),
    )
    gradient, give = call(
        functools.partial(second_owner_kernel, slots, levels),
        (grid, shape(devices, 8, LANES)),
        (asked, returned, rest, seen_cost, rest_cost),
        (whole, places, semaphores((width_x + 2,))),
        chip=(0, 1, 3, 4),
        raw=(0, 2),
        out_chip=(0,),
    )
    sums = exchange(give)
    six_rows = (shape(6, levels, width_y), shape(6, levels, width_y))
    up, down, left, right = call(
        functools.partial(final_edges_kernel, levels), six_rows + edges, (wind, gradient), (side,), chip=(0, 1)
    )
    around = halo(left, right, up, down)
    wind, strain, costs = call(
        functools.partial(final_kernel, levels, total_cells, total_gates),
        (grid, shape(6, rows, width_y), line_out),
        (sums, first_cost, wind, gradient) + around,
        (
            side,
            side,
            pltpu.VMEM((3, rows, width_y), F32),
            pltpu.VMEM((6, rows, width_y), F32),
            semaphores((3, PARTS)),
        ),
        chip=(0, 3, 4, 5, 6, 7),
        raw=(2,),
        out_raw=(0, 1),
        out_chip=(2,),
    )
    return (
        wind.reshape(background.shape),
        strain.reshape(6, width_x, levels, width_y),
        costs[0, :2],
    )


def solution(mesh):
    placed = (
        P(None, "tile", None, "radar"),
        P(("radar", "tile"), None, None),
        P(("radar", "tile"), None, None),
        P(("radar", "tile"), None),
        P(("radar", "tile")),
        P(("radar", "tile"), None),
    )

    return jax.shard_map(
        shards,
        mesh=mesh,
        in_specs=placed,
        out_specs=(P(None, "tile", None, "radar"), P(None, "tile", None, "radar"), P()),
        check_vma=False,
    )
```

```python
import functools

import jax
import jax.numpy as jnp
from jax import lax
from jax.experimental import pallas as pl
from jax.experimental.pallas import tpu as pltpu
from jax.sharding import PartitionSpec as P


BACKGROUND_WEIGHT = 0.5
DIVERGENCE_WEIGHT = 1.0
STEP_LENGTH = 0.3
EPSILON = 1e-06

AXES = ("radar", "tile")
LANES = 128
PARTS = 4
FINAL_PARTS = 8
F32 = jnp.float32
BF16 = jnp.bfloat16

COL_WY, COL_WX, COL_PART = 0, 1, 2
ROW_WX, ROW_PART = 0, 1
CORNERS = ((-1, -1), (-1, 1), (1, -1), (1, 1))


def exchange(x):
    return lax.all_to_all(x, AXES, split_axis=0, concat_axis=0, tiled=True)


def shifted(x, axis, step):
    size = lax.axis_size(axis)
    pairs = [(i, i + step) for i in range(size) if 0 <= i + step < size]
    return lax.ppermute(x, axis, pairs)


class Pieces:
    def __init__(self, source, target, sems, parts, at=0):
        rows = source.shape[-2]
        self.share = rows // parts
        self.copies = []
        self.seen = 0
        for i in range(parts):
            here = pl.ds(i * self.share, self.share)
            there = pl.ds(at + i * self.share, self.share)
            lead = (slice(None),) * (len(source.shape) - 2)
            self.copies.append(pltpu.make_async_copy(source.at[lead + (here,)], target.at[lead + (there,)], sems.at[i]))

    def start(self):
        for copy in self.copies:
            copy.start()
        return self

    def until(self, row):
        while self.seen < len(self.copies) and self.seen * self.share < row:
            self.copies[self.seen].wait()
            self.seen += 1

    def filled(self, row):
        while self.seen < len(self.copies) and (self.seen + 1) * self.share <= row:
            self.copies[self.seen].start()
            self.seen += 1

    def finish(self):
        for copy in self.copies:
            copy.wait()


class OutPieces(Pieces):
    def __init__(self, source, target, sems, parts, at=0):
        rows = target.shape[-2]
        self.share = rows // parts
        self.copies = []
        self.seen = 0
        for i in range(parts):
            here = pl.ds(at + i * self.share, self.share)
            there = pl.ds(i * self.share, self.share)
            lead = (slice(None),) * (len(source.shape) - 2)
            self.copies.append(pltpu.make_async_copy(source.at[lead + (here,)], target.at[lead + (there,)], sems.at[i]))


def iota(shape, dim):
    return lax.broadcasted_iota(jnp.int32, shape, dim)


def diff_levels(a, period):
    rows = a.shape[0]
    level = lax.rem(iota(a.shape, 0), jnp.int32(period))
    above = jnp.where(level == period - 1, 0.0, pltpu.roll(a, rows - 1, 0))
    below = jnp.where(level == 0, 0.0, pltpu.roll(a, 1, 0))
    return above - below


def diff_columns(a, left, right):
    width = a.shape[1]
    lane = iota(a.shape, 1)
    after = jnp.where(lane == width - 1, right, pltpu.roll(a, width - 1, 1))
    before = jnp.where(lane == 0, left, pltpu.roll(a, 1, 1))
    return after - before


def to_rows(columns):
    fill = jnp.zeros((LANES - columns.shape[0], columns.shape[1]), F32)
    return jnp.concatenate([columns, fill], axis=0).T


def sum_rows(a):
    total = a[:, :LANES]
    for start in range(LANES, a.shape[1], LANES):
        total = total + a[:, start : start + LANES]
    return jnp.sum(total, axis=0, keepdims=True)


def paired(first, second):
    half = LANES // 2
    lower = iota((1, LANES), 1) < half
    return jnp.where(lower, first + pltpu.roll(first, half, 1), second + pltpu.roll(second, half, 1))


def halves(line):
    lower = iota((1, LANES), 1) < LANES // 2
    return (
        jnp.sum(jnp.where(lower, line, 0.0), axis=1, keepdims=True),
        jnp.sum(jnp.where(lower, 0.0, line), axis=1, keepdims=True),
    )


def own_place():
    return lax.axis_index("radar") * lax.axis_size("tile") + lax.axis_index("tile")


def neighbour(along_tile, along_radar):
    tile = lax.axis_index("tile") + along_tile
    radar = lax.axis_index("radar") + along_radar
    exists = (tile >= 0) & (tile < lax.axis_size("tile")) & (radar >= 0) & (radar < lax.axis_size("radar"))
    return exists, jnp.where(exists, radar * lax.axis_size("tile") + tile, own_place())


def corner_lines(w_ref, levels):
    rows, width = w_ref.shape[1], w_ref.shape[2]
    lane = iota((levels, LANES), 1)
    packed = jnp.zeros((levels, LANES), F32)
    for c, (along_tile, along_radar) in enumerate(CORNERS):
        here = slice(0, levels) if along_tile < 0 else slice(rows - levels, rows)
        lanes, at = (slice(0, LANES), 0) if along_radar < 0 else (slice(width - LANES, width), LANES - 1)
        for k in range(2):
            packed = lane_column(packed, lane, w_ref[k, here, lanes], at, 2 * c + k)
    turned = jnp.concatenate([packed, jnp.zeros((LANES - levels, LANES), F32)], axis=0).T
    return [
        turned[2 * c : 2 * c + 1] + pltpu.roll(turned[2 * c + 1 : 2 * c + 2], levels, 1) for c in range(len(CORNERS))
    ]


def corner_columns(line_from, levels):
    lines = []
    for along_tile, along_radar in CORNERS:
        exists, place = neighbour(along_tile, along_radar)
        lines.append(jnp.where(exists, line_from(place), 0.0))
    fill = jnp.zeros((LANES - len(CORNERS), LANES), F32)
    turned = jnp.concatenate(lines + [fill], axis=0).T
    return [(turned[0:levels, c : c + 1], turned[levels : 2 * levels, c : c + 1]) for c in range(len(CORNERS))]


def block_at(index, runs):
    if runs & (runs - 1) == 0:
        return lax.shift_right_logical(index, jnp.int32(runs.bit_length() - 1)), index & (runs - 1)
    return lax.div(index, jnp.int32(runs)), lax.rem(index, jnp.int32(runs))


def read_block(ref, k, row, run):
    line = ref[k, pl.ds(row, 1), :]
    out = line[:, :LANES]
    for h in range(1, ref.shape[2] // LANES):
        out = jnp.where(run == h, line[:, h * LANES : (h + 1) * LANES], out)
    return out


def lane_column(packed, lane, tile, at, to):
    moved = tile if at == to else pltpu.roll(tile, (to - at) % LANES, 1)
    return jnp.where(lane == to, moved, packed)


def edges_kernel(levels, w_ref, left_out, right_out, up_out, down_out, scratch):
    rows, width = w_ref.shape[1], w_ref.shape[2]
    lane = iota((levels, LANES), 1)
    last = slice(width - LANES, width)
    for x in range(rows // levels):
        here = slice(x * levels, (x + 1) * levels)
        packed = jnp.where(lane < LANES // 2, w_ref[1, here, :LANES], w_ref[1, here, last])
        packed = lane_column(packed, lane, w_ref[0, here, :LANES], 0, 2)
        packed = lane_column(packed, lane, w_ref[2, here, :LANES], 0, 3)
        packed = lane_column(packed, lane, w_ref[0, here, last], LANES - 1, LANES - 3)
        packed = lane_column(packed, lane, w_ref[2, here, last], LANES - 1, LANES - 4)
        scratch[here, :] = packed
    turned = scratch[...].T
    place = iota((1, rows), 1)
    level = lax.rem(place, jnp.int32(levels))

    def partial(wx, wz):
        part = jnp.where(level == levels - 1, 0.0, pltpu.roll(wz, rows - 1, 1))
        part = part - jnp.where(level == 0, 0.0, pltpu.roll(wz, 1, 1))
        part = part + jnp.where(place >= rows - levels, 0.0, pltpu.roll(wx, rows - levels, 1))
        return part - jnp.where(place < levels, 0.0, pltpu.roll(wx, levels, 1))

    near, far = turned[0:8], turned[LANES - 8 : LANES]
    for out, wy, inner, wx, wz in (
        (left_out, near[0:1], near[1:2], near[2:3], near[3:4]),
        (right_out, far[7:8], -far[6:7], far[5:6], far[4:5]),
    ):
        out[...] = jnp.zeros_like(out)
        out[COL_WY : COL_WY + 1, :] = wy
        out[COL_WX : COL_WX + 1, :] = wx
        out[COL_PART : COL_PART + 1, :] = 0.5 * (inner + partial(wx, wz))
    for out, first in ((up_out, 0), (down_out, rows - levels)):
        here = slice(first, first + levels)
        part = diff_levels(w_ref[2, here, :], levels) + diff_columns(w_ref[1, here, :], 0.0, 0.0)
        if first > 0:
            part = part - w_ref[0, first - levels : first, :]
        else:
            part = part + w_ref[0, levels : 2 * levels, :]
        out[ROW_WX] = w_ref[0, here, :]
        out[ROW_PART] = 0.5 * part


def cycle(levels, w_ref, left_ref, right_ref, above_ref, below_ref, corners, ring, left_rows, right_rows, need, take_spread, take_push):
    rows, width = w_ref.shape[1], w_ref.shape[2]
    cells = rows // levels
    left_rows[...] = to_rows(left_ref[...])
    right_rows[...] = to_rows(right_ref[...])
    has_left = jnp.where(lax.axis_index("radar") > 0, 1.0, 0.0)
    has_right = jnp.where(lax.axis_index("radar") < lax.axis_size("radar") - 1, 1.0, 0.0)
    has_above = jnp.where(lax.axis_index("tile") > 0, 1.0, 0.0)
    has_below = jnp.where(lax.axis_index("tile") < lax.axis_size("tile") - 1, 1.0, 0.0)
    above_left, above_right, below_left, below_right = corners
    lane = iota((levels, width), 1)

    def ends(left, right):
        return jnp.where(lane == 0, -0.5 * left, jnp.where(lane == width - 1, 0.5 * right, 0.0))

    first, last = slice(0, levels), slice(rows - levels, rows)
    for x in range(cells):
        here = slice(x * levels, (x + 1) * levels)
        need(min(rows, (x + 2) * levels))
        after = w_ref[0, (x + 1) * levels : (x + 2) * levels, :] if x + 1 < cells else below_ref[ROW_WX]
        before = w_ref[0, (x - 1) * levels : x * levels, :] if x > 0 else above_ref[ROW_WX]
        spread = 0.5 * (
            (after - before)
            + diff_columns(
                w_ref[1, here, :],
                left_rows[here, COL_WY : COL_WY + 1],
                right_rows[here, COL_WY : COL_WY + 1],
            )
            + diff_levels(w_ref[2, here, :], levels)
        )
        ring[(x + 1) * levels : (x + 2) * levels, :] = spread
        take_spread(here, spread)
    above = above_ref[ROW_PART] + 0.5 * w_ref[0, first, :] + ends(above_left[1], above_right[1])
    below = below_ref[ROW_PART] - 0.5 * w_ref[0, last, :] + ends(below_left[1], below_right[1])
    ring[0:levels, :] = has_above * above
    ring[rows + levels : rows + 2 * levels, :] = has_below * below
    for x in range(cells):
        here = slice(x * levels, (x + 1) * levels)
        left = left_rows[here, COL_PART : COL_PART + 1] + 0.5 * w_ref[1, here, 0:1]
        right = right_rows[here, COL_PART : COL_PART + 1] - 0.5 * w_ref[1, here, width - 1 : width]
        if x == 0:
            left = left - 0.5 * above_left[0]
            right = right - 0.5 * above_right[0]
        if x == cells - 1:
            left = left + 0.5 * below_left[0]
            right = right + 0.5 * below_right[0]
        spread = ring[(x + 1) * levels : (x + 2) * levels, :]
        after = ring[(x + 2) * levels : (x + 3) * levels, :]
        before = ring[x * levels : (x + 1) * levels, :]
        take_push(0, here, (-0.5 * DIVERGENCE_WEIGHT) * (after - before))
        take_push(1, here, (-0.5 * DIVERGENCE_WEIGHT) * diff_columns(spread, has_left * left, has_right * right))
        take_push(2, here, (-0.5 * DIVERGENCE_WEIGHT) * diff_levels(spread, levels))


def first_cycle_kernel(levels, slots, w_hbm, left_ref, right_ref, above_ref, below_ref, cells_ref, push_hbm, spread_hbm, total_out, w_ref, push, ring, left_rows, right_rows, total, sems):
    fields = Pieces(w_hbm, w_ref, sems.at[0], PARTS).start()
    total[...] = jnp.zeros_like(total)
    spreads = OutPieces(ring, spread_hbm, sems.at[1], PARTS, levels)
    pushes = OutPieces(push, push_hbm, sems.at[2], PARTS)

    def line_from(place):
        block = cells_ref[pl.ds(place, 1)].reshape(cells_ref.shape[1:]).astype(F32)
        first = block[3 * slots : 3 * slots + 1]
        return first + pltpu.roll(first, LANES // 2, 1) + block[3 * slots + 1 : 3 * slots + 2]

    def take_spread(here, spread):
        total[...] += spread * spread
        spreads.filled(here.stop)

    def take_push(k, here, value):
        push[k, here, :] = value
        if k == 2:
            pushes.filled(here.stop)

    corners = corner_columns(line_from, levels)
    cycle(levels, w_ref, left_ref, right_ref, above_ref, below_ref, corners, ring, left_rows, right_rows, fields.until, take_spread, take_push)
    total_out[...] = jnp.broadcast_to(0.5 * DIVERGENCE_WEIGHT * sum_rows(total[...]), total_out.shape)
    spreads.finish()
    pushes.finish()


def second_cycle_kernel(levels, slots, w_hbm, left_ref, right_ref, above_ref, below_ref, got_ref, background_hbm, push_hbm, spread_hbm, step_ref, rest_hbm, wind_hbm, total_out, w_ref, background, push, spread, ring, left_rows, right_rows, total, sems):
    fields = Pieces(w_hbm, w_ref, sems.at[0], PARTS).start()
    spreads = Pieces(spread_hbm, spread, sems.at[1], PARTS).start()
    pushes = Pieces(push_hbm, push, sems.at[2], PARTS).start()
    backgrounds = Pieces(background_hbm, background, sems.at[3], PARTS).start()
    rests = OutPieces(push, rest_hbm, sems.at[4], PARTS)
    winds = OutPieces(background, wind_hbm, sems.at[5], PARTS)
    total[...] = jnp.zeros_like(total)
    step = step_ref[0:1, 0:1]

    def line_from(place):
        return got_ref[place, 3 * slots + 1 : 3 * slots + 2, :]

    def take_spread(here, bent):
        spreads.until(here.stop)
        value = spread[here, :] - step * bent
        total[...] += (0.5 * DIVERGENCE_WEIGHT) * (value * value)

    def take_push(k, here, bent):
        pushes.until(here.stop)
        backgrounds.until(here.stop)
        offset = step * w_ref[k, here, :]
        total[...] += (0.5 * BACKGROUND_WEIGHT) * (offset * offset)
        background[k, here, :] = background[k, here, :] - offset
        push[k, here, :] = push[k, here, :] - (BACKGROUND_WEIGHT * offset + step * bent)
        if k == 2:
            rests.filled(here.stop)
            winds.filled(here.stop)

    corners = corner_columns(line_from, levels)
    cycle(levels, w_ref, left_ref, right_ref, above_ref, below_ref, corners, ring, left_rows, right_rows, fields.until, take_spread, take_push)
    total_out[...] = jnp.broadcast_to(sum_rows(total[...]), total_out.shape)
    rests.finish()
    winds.finish()


def for_slots(count, body, step=8):
    step = min(step, count)

    def run(i, carry):
        for j in range(step):
            body(i * step + j)
        return carry

    lax.fori_loop(0, count // step, run, 0)


def ask_kernel(places_ref, out_ref):
    line = places_ref[...]
    if line.shape[1] < out_ref.shape[2]:
        line = jnp.concatenate([line, jnp.zeros((1, out_ref.shape[2] - line.shape[1]), jnp.int32)], axis=1)
    out_ref[...] = jnp.broadcast_to(line[None], out_ref.shape)


def ask(asked_hbm, asked_ref, sem):
    return pltpu.make_async_copy(asked_hbm.at[:, 0, :], asked_ref, sem)


def pick_kernel(slots, levels, asked_hbm, w_ref, out_ref, rows_ref, asked_ref, ask_sem):
    asking = ask(asked_hbm, asked_ref, ask_sem)
    asking.start()
    me = own_place()
    runs = w_ref.shape[2] // LANES
    rows_ref[...] = jnp.zeros_like(rows_ref)
    asking.wait()

    def one(s):
        for p in range(slots):
            row, run = block_at(asked_ref[s, me * slots + p], runs)
            for k in range(3):
                rows_ref[s, 3 * p + k : 3 * p + k + 1, :] = read_block(w_ref, k, row, run)

    for_slots(out_ref.shape[0], one)
    for (along_tile, along_radar), line in zip(CORNERS, corner_lines(w_ref, levels)):
        exists, place = neighbour(along_tile, along_radar)
        high = line.astype(BF16).astype(F32)
        middle = (line - high).astype(BF16).astype(F32)

        @pl.when(exists)
        def _():
            rows_ref[place, 3 * slots : 3 * slots + 1, :] = high + pltpu.roll(middle, LANES // 2, 1)
            rows_ref[place, 3 * slots + 1 : 3 * slots + 2, :] = line - high - middle

    out_ref[...] = rows_ref[...].astype(out_ref.dtype)


def weights_kernel(source, target, sem):
    copy = pltpu.make_async_copy(source, target, sem)
    copy.start()
    copy.wait()


def project(cells_of, weights_ref, proj_ref, sources, slots, height):
    def one(s):
        weights = weights_ref[pl.ds(s * slots, slots)].reshape(slots * LANES, LANES)
        seen = lax.dot_general(cells_of(s), weights, (((1,), (1,)), ((), ())), preferred_element_type=F32)
        here = pl.ds(pl.multiple_of(s * height, height), height)
        for p in range(slots):
            proj_ref[p, here, :] = seen[:, p * LANES : (p + 1) * LANES]

    for_slots(sources, one, 16)


def radial(proj_ref, sight_ref, p, sources, height):
    total = jnp.zeros((sources, LANES), F32)
    for k in range(3):
        total = total + sight_ref[3 * p + k] * proj_ref[p, pl.ds(3 * p + k, sources, stride=height), :]
    return total


def give_back(misfits, weights_ref, sight_ref, adj_ref, line_ref, out_ref, sources, slots, height):
    adj_ref[...] = jnp.zeros_like(adj_ref)
    cost = jnp.zeros((sources, LANES), F32)
    for p in range(slots):
        cost = cost + 0.5 * (misfits[p] * misfits[p])
        for k in range(3):
            adj_ref[p, pl.ds(3 * p + k, sources, stride=height), :] = sight_ref[3 * p + k] * misfits[p]
    high = cost.astype(BF16).astype(F32)
    line_ref[...] = jnp.zeros_like(line_ref)
    line_ref[pl.ds(3 * slots, sources, stride=height), :] = high
    line_ref[pl.ds(3 * slots + 1, sources, stride=height), :] = cost - high

    def one(s):
        weights = weights_ref[pl.ds(s * slots, slots)].reshape(slots * LANES, LANES)
        here = pl.ds(pl.multiple_of(s * height, height), height)
        adjoint = jnp.concatenate([adj_ref[p, here, :] for p in range(slots)], axis=1).astype(BF16)
        product = lax.dot_general(adjoint, weights, (((1,), (0,)), ((), ())), preferred_element_type=F32)
        out_ref[s] = (product + line_ref[here, :]).astype(out_ref.dtype)

    for_slots(sources, one, 16)


def first_source_kernel(slots, cells_ref, weights_ref, sight_ref, returned_out, misfit_out, proj_ref, adj_ref, line_ref):
    sources, height = cells_ref.shape[0], cells_ref.shape[1]
    project(lambda s: cells_ref[s].astype(BF16), weights_ref, proj_ref, sources, slots, height)
    misfits = []
    for p in range(slots):
        misfit = radial(proj_ref, sight_ref, p, sources, height) - sight_ref[3 * slots + p]
        misfit_out[p] = misfit
        misfits.append(misfit)
    give_back(misfits, weights_ref, sight_ref, adj_ref, line_ref, returned_out, sources, slots, height)


def second_source_kernel(slots, total_cells, total_gates, got_ref, weights_ref, sight_ref, misfit_ref, returned_out, step_out, cost_out, proj_ref, adj_ref, line_ref):
    sources, height = got_ref.shape[0], got_ref.shape[1]
    project(lambda s: got_ref[s].astype(BF16), weights_ref, proj_ref, sources, slots, height)
    squares, costs = halves(jnp.sum(got_ref[:, 3 * slots, :], axis=0, keepdims=True))
    step = STEP_LENGTH / jnp.sqrt(squares / total_cells + EPSILON)
    step_out[...] = jnp.broadcast_to(step, step_out.shape)
    cost_out[...] = jnp.broadcast_to(costs / total_gates, cost_out.shape)
    misfits = [
        misfit_ref[p] - step * radial(proj_ref, sight_ref, p, sources, height) for p in range(slots)
    ]
    give_back(misfits, weights_ref, sight_ref, adj_ref, line_ref, returned_out, sources, slots, height)


def scatter_rows(slots, asked_ref, returned_ref, out_ref):
    me = own_place()
    runs = out_ref.shape[2] // LANES
    place = iota((8, LANES), 0)

    def one(s):
        block = returned_ref[s].astype(F32)
        for p in range(slots):
            row, run = block_at(asked_ref[s, me * slots + p], runs)
            within = lax.rem(row, jnp.int32(8))
            base = pl.multiple_of(row - within, 8)
            lanes = pl.ds(pl.multiple_of(run * LANES, LANES), LANES)
            held = [out_ref[k, pl.ds(base, 8), lanes] for k in range(3)]
            for k in range(3):
                line = block[3 * p + k : 3 * p + k + 1, :]
                held[k] = held[k] + jnp.where(place == within, line, 0.0)
            for k in range(3):
                out_ref[k, pl.ds(base, 8), lanes] = held[k]

    for_slots(returned_ref.shape[0], one)


def gather_gradient(slots, levels, asked_hbm, asked_ref, returned_ref, rest_hbm, rest, gradient_ref, gradient_hbm, sems):
    rows, width = gradient_ref.shape[1], gradient_ref.shape[2]
    cells = rows // levels
    copy = pltpu.make_async_copy(rest_hbm, rest, sems.at[cells])
    asking = ask(asked_hbm, asked_ref, sems.at[cells + 1])
    asking.start()
    copy.start()
    gradient_ref[...] = jnp.zeros_like(gradient_ref)
    asking.wait()
    scatter_rows(slots, asked_ref, returned_ref, gradient_ref)
    copy.wait()
    total = jnp.zeros((levels, width), F32)
    copies = []
    for x in range(cells):
        here = slice(x * levels, (x + 1) * levels)
        for k in range(3):
            piece = gradient_ref[k, here, :] + rest[k, here, :]
            gradient_ref[k, here, :] = piece
            total = total + piece * piece
        if gradient_hbm is not None:
            copies.append(pltpu.make_async_copy(gradient_ref.at[:, here], gradient_hbm.at[:, here], sems.at[x]))
            copies[-1].start()
    return sum_rows(total), copies


def seen_cost(returned_ref, slots):
    cost = returned_ref[:, 3 * slots : 3 * slots + 2, :].astype(F32)
    return jnp.sum(jnp.sum(cost, axis=0), axis=0, keepdims=True)


def first_owner_kernel(slots, levels, asked_hbm, returned_ref, push_hbm, spread_cost_ref, gradient_hbm, give_out, left_out, right_out, up_out, down_out, push, gradient, asked_ref, scratch, sems):
    squares, copies = gather_gradient(
        slots, levels, asked_hbm, asked_ref, returned_ref, push_hbm, push, gradient, gradient_hbm, sems
    )
    sources = give_out.shape[0]
    sums = paired(squares, seen_cost(returned_ref, slots) + spread_cost_ref[0:1, :])
    give_out[...] = jnp.zeros_like(give_out)
    give_out[:, 3 * slots, :] = jnp.broadcast_to(sums, (sources, LANES))
    me = own_place()
    runs = gradient.shape[2] // LANES

    def one(s):
        for p in range(slots):
            row, run = block_at(asked_ref[s, me * slots + p], runs)
            for k in range(3):
                give_out[s, 3 * p + k : 3 * p + k + 1, :] = read_block(gradient, k, row, run)

    for_slots(sources, one)
    for (along_tile, along_radar), line in zip(CORNERS, corner_lines(gradient, levels)):
        exists, place = neighbour(along_tile, along_radar)

        @pl.when(exists)
        def _():
            give_out[place, 3 * slots + 1 : 3 * slots + 2, :] = line

    edges_kernel(levels, gradient, left_out, right_out, up_out, down_out, scratch)
    for copy in copies:
        copy.wait()


def second_owner_kernel(slots, levels, asked_hbm, returned_ref, rest_hbm, rest_cost_ref, gradient_out, give_out, rest, asked_ref, sems):
    squares, _ = gather_gradient(
        slots, levels, asked_hbm, asked_ref, returned_ref, rest_hbm, rest, gradient_out, None, sems
    )
    sums = paired(squares, seen_cost(returned_ref, slots) + rest_cost_ref[0:1, :])
    give_out[...] = jnp.broadcast_to(sums, give_out.shape)


def final_edges_kernel(levels, wind_ref, gradient_ref, up_out, down_out, left_out, right_out, scratch):
    rows, width = wind_ref.shape[1], wind_ref.shape[2]
    fields = [(wind_ref, k) for k in range(3)] + [(gradient_ref, k) for k in range(3)]
    for f, (ref, k) in enumerate(fields):
        up_out[f] = ref[k, 0:levels, :]
        down_out[f] = ref[k, rows - levels : rows, :]
    lane = iota((levels, LANES), 1)
    for x in range(rows // levels):
        here = slice(x * levels, (x + 1) * levels)
        packed = jnp.zeros((levels, LANES), F32)
        for f, (ref, k) in enumerate(fields):
            packed = lane_column(packed, lane, ref[k, here, :LANES], 0, f)
            packed = lane_column(packed, lane, ref[k, here, width - LANES :], LANES - 1, LANES - 8 + f)
        scratch[here, :] = packed
    turned = scratch[...].T
    left_out[...] = turned[0:8]
    right_out[...] = turned[LANES - 8 : LANES]


def final_kernel(levels, total_cells, total_gates, sums_ref, first_cost_hbm, wind_hbm, gradient_ref, left_ref, right_ref, above_ref, below_ref, wind_out, strain_out, cost_out, left_rows, right_rows, wind, strain, first_cost_ref, sems, cost_sem):
    rows = gradient_ref.shape[1]
    cells = rows // levels
    winds = Pieces(wind_hbm, wind, sems.at[0], FINAL_PARTS).start()
    cost_copy = pltpu.make_async_copy(first_cost_hbm, first_cost_ref, cost_sem)
    cost_copy.start()
    wind_outs = OutPieces(wind, wind_out, sems.at[1], FINAL_PARTS)
    strain_outs = OutPieces(strain, strain_out, sems.at[2], FINAL_PARTS)
    squares, cost = halves(jnp.sum(sums_ref[:, 0, :], axis=0, keepdims=True))
    step = STEP_LENGTH / jnp.sqrt(squares / total_cells + EPSILON)
    cost_out[1] = (cost / total_gates)[0, 0]
    left_rows[...] = to_rows(left_ref[...])
    right_rows[...] = to_rows(right_ref[...])

    def settle(x):
        here = slice(x * levels, (x + 1) * levels)
        winds.until(here.stop)
        for k in range(3):
            wind[k, here, :] = wind[k, here, :] - step * gradient_ref[k, here, :]
        wind_outs.filled(here.stop)

    settle(0)
    for x in range(cells):
        here = slice(x * levels, (x + 1) * levels)
        if x + 1 < cells:
            settle(x + 1)
        along = []
        for k in range(3):
            value = wind[k, here, :]
            if x + 1 < cells:
                after = wind[k, (x + 1) * levels : (x + 2) * levels, :]
            else:
                after = below_ref[k] - step * below_ref[3 + k]
            if x > 0:
                before = wind[k, (x - 1) * levels : x * levels, :]
            else:
                before = above_ref[k] - step * above_ref[3 + k]
            left = left_rows[here, k : k + 1] - step * left_rows[here, 3 + k : 4 + k]
            right = right_rows[here, k : k + 1] - step * right_rows[here, 3 + k : 4 + k]
            along.append((after - before, diff_columns(value, left, right), diff_levels(value, levels)))
        (xx, xy, xz), (yx, yy, yz), (zx, zy, zz) = along
        strain[0, here, :] = 0.5 * xx
        strain[1, here, :] = 0.5 * yy
        strain[2, here, :] = 0.5 * zz
        strain[3, here, :] = 0.25 * (xy + yx)
        strain[4, here, :] = 0.25 * (xz + zx)
        strain[5, here, :] = 0.25 * (yz + zy)
        strain_outs.filled(here.stop)
    cost_copy.wait()
    cost_out[0] = first_cost_ref[0, 0]
    wind_outs.finish()
    strain_outs.finish()


def shape(*dims, dtype=F32):
    return jax.ShapeDtypeStruct(dims, dtype)


VMEM = pl.BlockSpec(memory_space=pltpu.VMEM)
SMEM = pl.BlockSpec(memory_space=pltpu.SMEM)
ANY = pl.BlockSpec(memory_space=pl.ANY)


def call(kernel, out_shape, args, scratch=(), scalars=0, raw=(), out_raw=(), chip=(), out_chip=(), out_smem=(), out_vmem=False, flops=2000000, limit=16):
    single = not isinstance(out_shape, tuple)
    outs = (out_shape,) if single else out_shape
    held = [
        x if i < scalars or i in chip else pltpu.with_memory_space_constraint(x, pltpu.HBM)
        for i, x in enumerate(args)
    ]
    placed = tuple(o if i in out_chip or i in out_smem else pltpu.HBM(o.shape, o.dtype) for i, o in enumerate(outs))
    if out_vmem:
        placed = tuple(pltpu.VMEM(o.shape, o.dtype) for o in outs)
    specs = tuple(ANY if i in out_raw else SMEM if i in out_smem else VMEM for i in range(len(outs)))
    return pl.pallas_call(
        kernel,
        out_shape=placed[0] if single else placed,
        in_specs=[SMEM if i < scalars else ANY if i in raw else VMEM for i in range(len(args))],
        out_specs=specs[0] if single else specs,
        scratch_shapes=list(scratch),
        compiler_params=pltpu.CompilerParams(vmem_limit_bytes=limit * 1024 * 1024),
        cost_estimate=pl.CostEstimate(flops=flops, bytes_accessed=1 << 20, transcendentals=0),
    )(*held)


def shards(background, interp, beam, observed, cell_block, sweep_count):
    radar_count = lax.axis_size("radar")
    tile_count = lax.axis_size("tile")
    devices = radar_count * tile_count
    width_x, levels, width_y = background.shape[1:]
    slots = interp.shape[0] // devices
    gate_size = interp.shape[1]
    rows = width_x * levels
    height = -(-(3 * slots + 2) // 8) * 8
    total_cells = float(3 * rows * width_y * devices)
    total_gates = float(interp.shape[0] * devices * gate_size)
    field = background.reshape(3, rows, width_y)
    lanes = -(-devices * slots // LANES) * LANES
    asked = call(ask_kernel, shape(devices, 8, lanes, dtype=jnp.int32), (cell_block.reshape(1, -1),), chip=(0,))
    asked = exchange(asked)

    live = (jnp.arange(slots, dtype=jnp.int32)[:, None, None] < sweep_count.reshape(1, devices, 1)).astype(F32)
    sight = beam.reshape(devices, slots, 3, gate_size).transpose(1, 2, 0, 3).astype(F32) * live[:, None]
    seen = observed.reshape(devices, slots, gate_size).transpose(1, 0, 2).astype(F32) * live
    sight = jnp.concatenate([sight.reshape(3 * slots, devices, gate_size), seen], axis=0)

    edges = (shape(8, rows), shape(8, rows))
    row_edges = (shape(2, levels, width_y), shape(2, levels, width_y))
    grid = shape(3, rows, width_y)
    line_out = shape(8, LANES)
    side = pltpu.VMEM((rows, LANES), F32)
    whole = pltpu.VMEM((3, rows, width_y), F32)
    plane = pltpu.VMEM((rows, width_y), F32)
    ring = pltpu.VMEM((rows + 2 * levels, width_y), F32)
    strip = pltpu.VMEM((levels, width_y), F32)
    semaphores = pltpu.SemaphoreType.DMA
    places = pltpu.SMEM((devices, lanes), jnp.int32)

    def halo(left, right, up, down):
        from_left = shifted(right, "radar", 1)
        from_right = shifted(left, "radar", -1)
        above = shifted(down, "tile", 1)
        below = shifted(up, "tile", -1)
        return from_left, from_right, above, below

    def edges_of(values):
        out = call(functools.partial(edges_kernel, levels), edges + row_edges, (values,), (side,), chip=(0,))
        return halo(*out)

    around = edges_of(field)
    cells = call(
        functools.partial(pick_kernel, slots, levels),
        shape(devices, height, LANES, dtype=BF16),
        (asked, field),
        (pltpu.VMEM((devices, height, LANES), F32), places, semaphores),
        chip=(0, 1),
        raw=(0,),
    )
    cells = exchange(cells)
    products = (
        pltpu.VMEM((slots, devices * height, LANES), F32),
        pltpu.VMEM((slots, devices * height, LANES), F32),
        pltpu.VMEM((devices * height, LANES), F32),
    )
    weights = call(weights_kernel, shape(*interp.shape, dtype=BF16), (interp,), (semaphores,), raw=(0,), out_vmem=True)
    returned, misfit = call(
        functools.partial(first_source_kernel, slots),
        (shape(devices, height, LANES, dtype=BF16), shape(slots, devices, LANES)),
        (cells, weights, sight),
        products,
        chip=(0, 1, 2),
        out_chip=(1,),
    )
    returned = exchange(returned)
    push, spread, spread_cost = call(
        functools.partial(first_cycle_kernel, levels, slots),
        (grid, shape(rows, width_y), line_out),
        (field,) + around + (cells,),
        (whole, whole, ring, side, side, strip, semaphores((3, PARTS))),
        chip=(1, 2, 3, 4, 5),
        raw=(0,),
        out_raw=(0, 1),
        out_chip=(2,),
    )
    gradient, give, *sides = call(
        functools.partial(first_owner_kernel, slots, levels),
        (grid, shape(devices, height, LANES)) + edges + row_edges,
        (asked, returned, push, spread_cost),
        (whole, whole, places, side, semaphores((width_x + 2,))),
        chip=(0, 1, 3),
        raw=(0, 2),
        out_raw=(0,),
    )
    got = exchange(give)
    around = halo(*sides)
    returned, step, first_cost = call(
        functools.partial(second_source_kernel, slots, total_cells, total_gates),
        (shape(devices, height, LANES, dtype=BF16), line_out, line_out),
        (got, weights, sight, misfit),
        products,
        chip=(0, 1, 2, 3),
        out_chip=(1,),
    )
    returned = exchange(returned)
    rest, wind, rest_cost = call(
        functools.partial(second_cycle_kernel, levels, slots),
        (grid, grid, line_out),
        (gradient,) + around + (got, field, push, spread, step),
        (whole, whole, whole, plane, ring, side, side, strip, semaphores((6, PARTS))),
        chip=(1, 2, 3, 4, 5, 9),
        raw=(0, 6, 7, 8),
        out_raw=(0, 1),
        out_chip=(2,),
    )
    gradient, give = call(
        functools.partial(second_owner_kernel, slots, levels),
        (grid, shape(devices, 8, LANES)),
        (asked, returned, rest, rest_cost),
        (whole, places, semaphores((width_x + 2,))),
        chip=(0, 1, 3),
        raw=(0, 2),
        out_chip=(0,),
    )
    sums = exchange(give)
    six_rows = (shape(6, levels, width_y), shape(6, levels, width_y))
    up, down, left, right = call(
        functools.partial(final_edges_kernel, levels), six_rows + edges, (wind, gradient), (side,), chip=(0, 1)
    )
    around = halo(left, right, up, down)
    wind, strain, costs = call(
        functools.partial(final_kernel, levels, total_cells, total_gates),
        (grid, shape(6, rows, width_y), shape(2)),
        (sums, first_cost, wind, gradient) + around,
        (
            side,
            side,
            pltpu.VMEM((3, rows, width_y), F32),
            pltpu.VMEM((6, rows, width_y), F32),
            pltpu.SMEM((8, LANES), F32),
            semaphores((3, FINAL_PARTS)),
            semaphores,
        ),
        chip=(0, 3, 4, 5, 6, 7),
        raw=(1, 2),
        out_raw=(0, 1),
        out_smem=(2,),
    )
    return (
        wind.reshape(background.shape),
        strain.reshape(6, width_x, levels, width_y),
        costs,
    )


def solution(mesh):
    placed = (
        P(None, "tile", None, "radar"),
        P(("radar", "tile"), None, None),
        P(("radar", "tile"), None, None),
        P(("radar", "tile"), None),
        P(("radar", "tile")),
        P(("radar", "tile"), None),
    )

    return jax.shard_map(
        shards,
        mesh=mesh,
        in_specs=placed,
        out_specs=(P(None, "tile", None, "radar"), P(None, "tile", None, "radar"), P()),
        check_vma=False,
    )
```

```python
import functools

import jax
import jax.numpy as jnp
from jax import lax
from jax.experimental import pallas as pl
from jax.experimental.pallas import tpu as pltpu
from jax.sharding import PartitionSpec as P


BACKGROUND_WEIGHT = 0.5
DIVERGENCE_WEIGHT = 1.0
STEP_LENGTH = 0.3
EPSILON = 1e-06

AXES = ("radar", "tile")
LANES = 128
PARTS = 4
SPLIT = 3
FINAL_PARTS = 8
F32 = jnp.float32
BF16 = jnp.bfloat16

COL_WY, COL_WX, COL_PART, COL_WZ = 0, 1, 2, 3
COL_WIND = (COL_WX, COL_WY, COL_WZ)
ROW_WX, ROW_PART, ROW_WY, ROW_WZ = 0, 1, 2, 3
ROW_WIND = (ROW_WX, ROW_WY, ROW_WZ)
CORNERS = ((-1, -1), (-1, 1), (1, -1), (1, 1))


def exchange(x):
    return lax.all_to_all(x, AXES, split_axis=0, concat_axis=0, tiled=True)


def shifted(x, axis, step):
    size = lax.axis_size(axis)
    pairs = [(i, i + step) for i in range(size) if 0 <= i + step < size]
    return lax.ppermute(x, axis, pairs)


class Pieces:
    def __init__(self, source, target, sems, parts, at=0):
        rows = source.shape[-2]
        self.share = rows // parts
        self.copies = []
        self.seen = 0
        for i in range(parts):
            here = pl.ds(i * self.share, self.share)
            there = pl.ds(at + i * self.share, self.share)
            lead = (slice(None),) * (len(source.shape) - 2)
            self.copies.append(pltpu.make_async_copy(source.at[lead + (here,)], target.at[lead + (there,)], sems.at[i]))

    def start(self):
        for copy in self.copies:
            copy.start()
        return self

    def until(self, row):
        while self.seen < len(self.copies) and self.seen * self.share < row:
            self.copies[self.seen].wait()
            self.seen += 1

    def filled(self, row):
        while self.seen < len(self.copies) and (self.seen + 1) * self.share <= row:
            self.copies[self.seen].start()
            self.seen += 1

    def finish(self):
        for copy in self.copies:
            copy.wait()


class OutPieces(Pieces):
    def __init__(self, source, target, sems, parts, at=0):
        rows = target.shape[-2]
        self.share = rows // parts
        self.copies = []
        self.seen = 0
        for i in range(parts):
            here = pl.ds(at + i * self.share, self.share)
            there = pl.ds(i * self.share, self.share)
            lead = (slice(None),) * (len(source.shape) - 2)
            self.copies.append(pltpu.make_async_copy(source.at[lead + (here,)], target.at[lead + (there,)], sems.at[i]))


def iota(shape, dim):
    return lax.broadcasted_iota(jnp.int32, shape, dim)


def diff_levels(a, period):
    rows = a.shape[0]
    level = lax.rem(iota(a.shape, 0), jnp.int32(period))
    above = jnp.where(level == period - 1, 0.0, pltpu.roll(a, rows - 1, 0))
    below = jnp.where(level == 0, 0.0, pltpu.roll(a, 1, 0))
    return above - below


def diff_columns(a, left, right):
    width = a.shape[1]
    lane = iota(a.shape, 1)
    after = jnp.where(lane == width - 1, right, pltpu.roll(a, width - 1, 1))
    before = jnp.where(lane == 0, left, pltpu.roll(a, 1, 1))
    return after - before


def to_rows(columns):
    fill = jnp.zeros((LANES - columns.shape[0], columns.shape[1]), F32)
    return jnp.concatenate([columns, fill], axis=0).T


def sum_rows(a):
    total = a[:, :LANES]
    for start in range(LANES, a.shape[1], LANES):
        total = total + a[:, start : start + LANES]
    return jnp.sum(total, axis=0, keepdims=True)


def paired(first, second):
    half = LANES // 2
    lower = iota((1, LANES), 1) < half
    return jnp.where(lower, first + pltpu.roll(first, half, 1), second + pltpu.roll(second, half, 1))


def halves(line):
    lower = iota((1, LANES), 1) < LANES // 2
    return (
        jnp.sum(jnp.where(lower, line, 0.0), axis=1, keepdims=True),
        jnp.sum(jnp.where(lower, 0.0, line), axis=1, keepdims=True),
    )


def own_place():
    return lax.axis_index("radar") * lax.axis_size("tile") + lax.axis_index("tile")


def neighbour(along_tile, along_radar):
    tile = lax.axis_index("tile") + along_tile
    radar = lax.axis_index("radar") + along_radar
    exists = (tile >= 0) & (tile < lax.axis_size("tile")) & (radar >= 0) & (radar < lax.axis_size("radar"))
    return exists, jnp.where(exists, radar * lax.axis_size("tile") + tile, own_place())


def corner_lines(w_ref, levels):
    rows, width = w_ref.shape[1], w_ref.shape[2]
    lane = iota((levels, LANES), 1)
    packed = jnp.zeros((levels, LANES), F32)
    for c, (along_tile, along_radar) in enumerate(CORNERS):
        here = slice(0, levels) if along_tile < 0 else slice(rows - levels, rows)
        lanes, at = (slice(0, LANES), 0) if along_radar < 0 else (slice(width - LANES, width), LANES - 1)
        for k in range(2):
            packed = lane_column(packed, lane, w_ref[k, here, lanes], at, 2 * c + k)
    turned = jnp.concatenate([packed, jnp.zeros((LANES - levels, LANES), F32)], axis=0).T
    return [
        turned[2 * c : 2 * c + 1] + pltpu.roll(turned[2 * c + 1 : 2 * c + 2], levels, 1) for c in range(len(CORNERS))
    ]


def corner_columns(line_from, levels):
    lines = []
    for along_tile, along_radar in CORNERS:
        exists, place = neighbour(along_tile, along_radar)
        lines.append(jnp.where(exists, line_from(place), 0.0))
    fill = jnp.zeros((LANES - len(CORNERS), LANES), F32)
    turned = jnp.concatenate(lines + [fill], axis=0).T
    return [(turned[0:levels, c : c + 1], turned[levels : 2 * levels, c : c + 1]) for c in range(len(CORNERS))]


def block_at(index, runs):
    if runs & (runs - 1) == 0:
        return lax.shift_right_logical(index, jnp.int32(runs.bit_length() - 1)), index & (runs - 1)
    return lax.div(index, jnp.int32(runs)), lax.rem(index, jnp.int32(runs))


def read_block(ref, k, row, run):
    line = ref[k, pl.ds(row, 1), :]
    out = line[:, :LANES]
    for h in range(1, ref.shape[2] // LANES):
        out = jnp.where(run == h, line[:, h * LANES : (h + 1) * LANES], out)
    return out


def lane_column(packed, lane, tile, at, to):
    moved = tile if at == to else pltpu.roll(tile, (to - at) % LANES, 1)
    return jnp.where(lane == to, moved, packed)


def streamed_edges_kernel(levels, w_hbm, left_out, right_out, up_out, down_out, scratch, w_ref, sems):
    fields = Pieces(w_hbm, w_ref, sems, PARTS).start()
    edges_kernel(levels, w_ref, left_out, right_out, up_out, down_out, scratch, fields.until)


def edges_kernel(levels, w_ref, left_out, right_out, up_out, down_out, scratch, need=lambda row: None):
    rows, width = w_ref.shape[1], w_ref.shape[2]
    lane = iota((levels, LANES), 1)
    last = slice(width - LANES, width)
    for x in range(rows // levels):
        here = slice(x * levels, (x + 1) * levels)
        need(here.stop)
        packed = jnp.where(lane < LANES // 2, w_ref[1, here, :LANES], w_ref[1, here, last])
        packed = lane_column(packed, lane, w_ref[0, here, :LANES], 0, 2)
        packed = lane_column(packed, lane, w_ref[2, here, :LANES], 0, 3)
        packed = lane_column(packed, lane, w_ref[0, here, last], LANES - 1, LANES - 3)
        packed = lane_column(packed, lane, w_ref[2, here, last], LANES - 1, LANES - 4)
        scratch[here, :] = packed
    turned = scratch[...].T
    place = iota((1, rows), 1)
    level = lax.rem(place, jnp.int32(levels))

    def partial(wx, wz):
        part = jnp.where(level == levels - 1, 0.0, pltpu.roll(wz, rows - 1, 1))
        part = part - jnp.where(level == 0, 0.0, pltpu.roll(wz, 1, 1))
        part = part + jnp.where(place >= rows - levels, 0.0, pltpu.roll(wx, rows - levels, 1))
        return part - jnp.where(place < levels, 0.0, pltpu.roll(wx, levels, 1))

    near, far = turned[0:8], turned[LANES - 8 : LANES]
    for out, wy, inner, wx, wz in (
        (left_out, near[0:1], near[1:2], near[2:3], near[3:4]),
        (right_out, far[7:8], -far[6:7], far[5:6], far[4:5]),
    ):
        out[...] = jnp.zeros_like(out)
        out[COL_WY : COL_WY + 1, :] = wy
        out[COL_WX : COL_WX + 1, :] = wx
        out[COL_PART : COL_PART + 1, :] = 0.5 * (inner + partial(wx, wz))
        out[COL_WZ : COL_WZ + 1, :] = wz
    for out, first in ((up_out, 0), (down_out, rows - levels)):
        here = slice(first, first + levels)
        part = diff_levels(w_ref[2, here, :], levels) + diff_columns(w_ref[1, here, :], 0.0, 0.0)
        if first > 0:
            part = part - w_ref[0, first - levels : first, :]
        else:
            part = part + w_ref[0, levels : 2 * levels, :]
        out[ROW_WX] = w_ref[0, here, :]
        out[ROW_PART] = 0.5 * part
        out[ROW_WY] = w_ref[1, here, :]
        out[ROW_WZ] = w_ref[2, here, :]


def cycle(levels, w_ref, left_ref, right_ref, above_ref, below_ref, corners, ring, left_rows, right_rows, need, take_spread, take_push):
    rows, width = w_ref.shape[1], w_ref.shape[2]
    cells = rows // levels
    left_rows[...] = to_rows(left_ref[...])
    right_rows[...] = to_rows(right_ref[...])
    has_left = jnp.where(lax.axis_index("radar") > 0, 1.0, 0.0)
    has_right = jnp.where(lax.axis_index("radar") < lax.axis_size("radar") - 1, 1.0, 0.0)
    has_above = jnp.where(lax.axis_index("tile") > 0, 1.0, 0.0)
    has_below = jnp.where(lax.axis_index("tile") < lax.axis_size("tile") - 1, 1.0, 0.0)
    above_left, above_right, below_left, below_right = corners
    lane = iota((levels, width), 1)

    def ends(left, right):
        return jnp.where(lane == 0, -0.5 * left, jnp.where(lane == width - 1, 0.5 * right, 0.0))

    first, last = slice(0, levels), slice(rows - levels, rows)
    for x in range(cells):
        here = slice(x * levels, (x + 1) * levels)
        need(min(rows, (x + 2) * levels))
        after = w_ref[0, (x + 1) * levels : (x + 2) * levels, :] if x + 1 < cells else below_ref[ROW_WX]
        before = w_ref[0, (x - 1) * levels : x * levels, :] if x > 0 else above_ref[ROW_WX]
        spread = 0.5 * (
            (after - before)
            + diff_columns(
                w_ref[1, here, :],
                left_rows[here, COL_WY : COL_WY + 1],
                right_rows[here, COL_WY : COL_WY + 1],
            )
            + diff_levels(w_ref[2, here, :], levels)
        )
        ring[(x + 1) * levels : (x + 2) * levels, :] = spread
        take_spread(here, spread)
    above = above_ref[ROW_PART] + 0.5 * w_ref[0, first, :] + ends(above_left[1], above_right[1])
    below = below_ref[ROW_PART] - 0.5 * w_ref[0, last, :] + ends(below_left[1], below_right[1])
    ring[0:levels, :] = has_above * above
    ring[rows + levels : rows + 2 * levels, :] = has_below * below
    for x in range(cells):
        here = slice(x * levels, (x + 1) * levels)
        left = left_rows[here, COL_PART : COL_PART + 1] + 0.5 * w_ref[1, here, 0:1]
        right = right_rows[here, COL_PART : COL_PART + 1] - 0.5 * w_ref[1, here, width - 1 : width]
        if x == 0:
            left = left - 0.5 * above_left[0]
            right = right - 0.5 * above_right[0]
        if x == cells - 1:
            left = left + 0.5 * below_left[0]
            right = right + 0.5 * below_right[0]
        spread = ring[(x + 1) * levels : (x + 2) * levels, :]
        after = ring[(x + 2) * levels : (x + 3) * levels, :]
        before = ring[x * levels : (x + 1) * levels, :]
        take_push(0, here, (-0.5 * DIVERGENCE_WEIGHT) * (after - before))
        take_push(1, here, (-0.5 * DIVERGENCE_WEIGHT) * diff_columns(spread, has_left * left, has_right * right))
        take_push(2, here, (-0.5 * DIVERGENCE_WEIGHT) * diff_levels(spread, levels))


def first_cycle_kernel(levels, slots, w_hbm, left_ref, right_ref, above_ref, below_ref, cells_ref, push_hbm, spread_hbm, total_out, w_ref, push, ring, left_rows, right_rows, total, sems):
    fields = Pieces(w_hbm, w_ref, sems.at[0], PARTS).start()
    total[...] = jnp.zeros_like(total)
    spreads = OutPieces(ring, spread_hbm, sems.at[1], PARTS, levels)
    pushes = OutPieces(push, push_hbm, sems.at[2], PARTS)

    def line_from(place):
        block = cells_ref[pl.ds(place, 1)].reshape(cells_ref.shape[1:]).astype(F32)
        first = block[3 * slots : 3 * slots + 1]
        return first + pltpu.roll(first, LANES // 2, 1) + block[3 * slots + 1 : 3 * slots + 2]

    def take_spread(here, spread):
        total[...] += spread * spread
        spreads.filled(here.stop)

    def take_push(k, here, value):
        push[k, here, :] = value
        if k == 2:
            pushes.filled(here.stop)

    corners = corner_columns(line_from, levels)
    cycle(levels, w_ref, left_ref, right_ref, above_ref, below_ref, corners, ring, left_rows, right_rows, fields.until, take_spread, take_push)
    total_out[...] = jnp.broadcast_to(0.5 * DIVERGENCE_WEIGHT * sum_rows(total[...]), total_out.shape)
    spreads.finish()
    pushes.finish()


def second_cycle_kernel(levels, slots, w_hbm, left_ref, right_ref, above_ref, below_ref, got_ref, background_hbm, push_hbm, spread_hbm, step_ref, rest_hbm, wind_hbm, total_out, w_ref, background, push, spread, ring, left_rows, right_rows, total, sems):
    fields = Pieces(w_hbm, w_ref, sems.at[0], PARTS).start()
    spreads = Pieces(spread_hbm, spread, sems.at[1], PARTS).start()
    pushes = Pieces(push_hbm, push, sems.at[2], PARTS).start()
    backgrounds = Pieces(background_hbm, background, sems.at[3], PARTS).start()
    rests = OutPieces(push, rest_hbm, sems.at[4], PARTS)
    winds = OutPieces(background, wind_hbm, sems.at[5], PARTS)
    total[...] = jnp.zeros_like(total)
    step = step_ref[0:1, 0:1]

    def line_from(place):
        return got_ref[place, 3 * slots + 1 : 3 * slots + 2, :]

    def take_spread(here, bent):
        spreads.until(here.stop)
        value = spread[here, :] - step * bent
        total[...] += (0.5 * DIVERGENCE_WEIGHT) * (value * value)

    def take_push(k, here, bent):
        pushes.until(here.stop)
        backgrounds.until(here.stop)
        offset = step * w_ref[k, here, :]
        total[...] += (0.5 * BACKGROUND_WEIGHT) * (offset * offset)
        background[k, here, :] = background[k, here, :] - offset
        push[k, here, :] = push[k, here, :] - (BACKGROUND_WEIGHT * offset + step * bent)
        if k == 2:
            rests.filled(here.stop)
            winds.filled(here.stop)

    corners = corner_columns(line_from, levels)
    cycle(levels, w_ref, left_ref, right_ref, above_ref, below_ref, corners, ring, left_rows, right_rows, fields.until, take_spread, take_push)
    total_out[...] = jnp.broadcast_to(sum_rows(total[...]), total_out.shape)
    rests.finish()
    winds.finish()


def for_slots(count, body, step=8):
    step = min(step, count)

    def run(i, carry):
        for j in range(step):
            body(i * step + j)
        return carry

    lax.fori_loop(0, count // step, run, 0)


def ask_kernel(places_ref, out_ref):
    line = places_ref[...]
    if line.shape[1] < out_ref.shape[2]:
        line = jnp.concatenate([line, jnp.zeros((1, out_ref.shape[2] - line.shape[1]), jnp.int32)], axis=1)
    out_ref[...] = jnp.broadcast_to(line[None], out_ref.shape)


def ask(asked_hbm, asked_ref, sem):
    return pltpu.make_async_copy(asked_hbm.at[:, 0, :], asked_ref, sem)


def pick_kernel(slots, levels, asked_hbm, w_ref, out_ref, rows_ref, asked_ref, ask_sem):
    asking = ask(asked_hbm, asked_ref, ask_sem)
    asking.start()
    me = own_place()
    runs = w_ref.shape[2] // LANES
    rows_ref[...] = jnp.zeros_like(rows_ref)
    asking.wait()

    def one(s):
        for p in range(slots):
            row, run = block_at(asked_ref[s, me * slots + p], runs)
            for k in range(3):
                rows_ref[s, 3 * p + k : 3 * p + k + 1, :] = read_block(w_ref, k, row, run)

    for_slots(out_ref.shape[0], one)
    for (along_tile, along_radar), line in zip(CORNERS, corner_lines(w_ref, levels)):
        exists, place = neighbour(along_tile, along_radar)
        high = line.astype(BF16).astype(F32)
        middle = (line - high).astype(BF16).astype(F32)

        @pl.when(exists)
        def _():
            rows_ref[place, 3 * slots : 3 * slots + 1, :] = high + pltpu.roll(middle, LANES // 2, 1)
            rows_ref[place, 3 * slots + 1 : 3 * slots + 2, :] = line - high - middle

    out_ref[...] = rows_ref[...].astype(out_ref.dtype)


def source_kernel(slots, weights_hbm, beam_hbm, observed_hbm, count_hbm, weights_out, sight_out, beam_ref, observed_ref, count_ref, wide_ref, sems):
    pairs = (
        (count_hbm, count_ref),
        (beam_hbm, beam_ref),
        (observed_hbm, observed_ref),
        (weights_hbm, weights_out),
    )
    copies = [pltpu.make_async_copy(source, target, sems.at[i]) for i, (source, target) in enumerate(pairs)]
    for copy in copies:
        copy.start()
    sources = sight_out.shape[1]
    diagonal = iota((sources, sources), 0) == iota((sources, sources), 1)
    for copy in copies[:3]:
        copy.wait()
    counts = jnp.sum(jnp.where(diagonal, count_ref[...].astype(F32), 0.0), axis=1, keepdims=True)
    for k in range(4):
        wide_ref[k] = (beam_ref[k] if k < 3 else observed_ref[...]).astype(F32)
        for p in range(slots):
            live = jnp.where(counts > p, wide_ref[k, pl.ds(p, sources, stride=slots), :], 0.0)
            sight_out[3 * p + k if k < 3 else 3 * slots + p] = live
    copies[3].wait()


def project(cells_of, weights_ref, proj_ref, sources, slots, height):
    def one(s):
        weights = weights_ref[pl.ds(s * slots, slots)].reshape(slots * LANES, LANES)
        seen = lax.dot_general(cells_of(s), weights, (((1,), (1,)), ((), ())), preferred_element_type=F32)
        here = pl.ds(pl.multiple_of(s * height, height), height)
        for p in range(slots):
            proj_ref[p, here, :] = seen[:, p * LANES : (p + 1) * LANES]

    for_slots(sources, one, 16)


def radial(proj_ref, sight_ref, p, sources, height):
    total = jnp.zeros((sources, LANES), F32)
    for k in range(3):
        total = total + sight_ref[3 * p + k] * proj_ref[p, pl.ds(3 * p + k, sources, stride=height), :]
    return total


def give_back(misfits, weights_ref, sight_ref, adj_ref, line_ref, out_ref, sources, slots, height):
    adj_ref[...] = jnp.zeros_like(adj_ref)
    cost = jnp.zeros((sources, LANES), F32)
    for p in range(slots):
        cost = cost + 0.5 * (misfits[p] * misfits[p])
        for k in range(3):
            adj_ref[p, pl.ds(3 * p + k, sources, stride=height), :] = sight_ref[3 * p + k] * misfits[p]
    high = cost.astype(BF16).astype(F32)
    line_ref[...] = jnp.zeros_like(line_ref)
    line_ref[pl.ds(3 * slots, sources, stride=height), :] = high
    line_ref[pl.ds(3 * slots + 1, sources, stride=height), :] = cost - high

    def one(s):
        weights = weights_ref[pl.ds(s * slots, slots)].reshape(slots * LANES, LANES)
        here = pl.ds(pl.multiple_of(s * height, height), height)
        adjoint = jnp.concatenate([adj_ref[p, here, :] for p in range(slots)], axis=1).astype(BF16)
        product = lax.dot_general(adjoint, weights, (((1,), (0,)), ((), ())), preferred_element_type=F32)
        out_ref[s] = (product + line_ref[here, :]).astype(out_ref.dtype)

    for_slots(sources, one, 16)


def first_source_kernel(slots, cells_ref, weights_ref, sight_ref, returned_out, misfit_out, proj_ref, adj_ref, line_ref):
    sources, height = cells_ref.shape[0], cells_ref.shape[1]
    project(lambda s: cells_ref[s].astype(BF16), weights_ref, proj_ref, sources, slots, height)
    misfits = []
    for p in range(slots):
        misfit = radial(proj_ref, sight_ref, p, sources, height) - sight_ref[3 * slots + p]
        misfit_out[p] = misfit
        misfits.append(misfit)
    give_back(misfits, weights_ref, sight_ref, adj_ref, line_ref, returned_out, sources, slots, height)


def second_source_kernel(slots, total_cells, total_gates, got_ref, weights_ref, sight_ref, misfit_ref, returned_out, step_out, cost_out, proj_ref, adj_ref, line_ref):
    sources, height = got_ref.shape[0], got_ref.shape[1]
    project(lambda s: got_ref[s].astype(BF16), weights_ref, proj_ref, sources, slots, height)
    squares, costs = halves(jnp.sum(got_ref[:, 3 * slots, :], axis=0, keepdims=True))
    step = STEP_LENGTH / jnp.sqrt(squares / total_cells + EPSILON)
    step_out[...] = jnp.broadcast_to(step, step_out.shape)
    cost_out[...] = jnp.broadcast_to(costs / total_gates, cost_out.shape)
    misfits = [
        misfit_ref[p] - step * radial(proj_ref, sight_ref, p, sources, height) for p in range(slots)
    ]
    give_back(misfits, weights_ref, sight_ref, adj_ref, line_ref, returned_out, sources, slots, height)


def scatter_rows(slots, asked_ref, returned_ref, out_ref):
    me = own_place()
    runs = out_ref.shape[2] // LANES
    place = iota((8, LANES), 0)

    def one(s):
        block = returned_ref[s].astype(F32)
        for p in range(slots):
            row, run = block_at(asked_ref[s, me * slots + p], runs)
            within = lax.rem(row, jnp.int32(8))
            base = pl.multiple_of(row - within, 8)
            lanes = pl.ds(pl.multiple_of(run * LANES, LANES), LANES)
            held = [out_ref[k, pl.ds(base, 8), lanes] for k in range(3)]
            for k in range(3):
                line = block[3 * p + k : 3 * p + k + 1, :]
                held[k] = held[k] + jnp.where(place == within, line, 0.0)
            for k in range(3):
                out_ref[k, pl.ds(base, 8), lanes] = held[k]

    for_slots(returned_ref.shape[0], one)


def gather_gradient(slots, levels, asked_hbm, asked_ref, returned_ref, rest_hbm, rest, gradient_ref, gradient_hbm, sems):
    rows, width = gradient_ref.shape[1], gradient_ref.shape[2]
    cells = rows // levels
    copy = pltpu.make_async_copy(rest_hbm, rest, sems.at[cells])
    asking = ask(asked_hbm, asked_ref, sems.at[cells + 1])
    asking.start()
    copy.start()
    gradient_ref[...] = jnp.zeros_like(gradient_ref)
    asking.wait()
    scatter_rows(slots, asked_ref, returned_ref, gradient_ref)
    copy.wait()
    total = jnp.zeros((levels, width), F32)
    copies = []
    for x in range(cells):
        here = slice(x * levels, (x + 1) * levels)
        for k in range(3):
            piece = gradient_ref[k, here, :] + rest[k, here, :]
            gradient_ref[k, here, :] = piece
            total = total + piece * piece
        if gradient_hbm is not None:
            copies.append(pltpu.make_async_copy(gradient_ref.at[:, here], gradient_hbm.at[:, here], sems.at[x]))
            copies[-1].start()
    return sum_rows(total), copies


def seen_cost(returned_ref, slots):
    cost = returned_ref[:, 3 * slots : 3 * slots + 2, :].astype(F32)
    return jnp.sum(jnp.sum(cost, axis=0), axis=0, keepdims=True)


def first_owner_kernel(slots, levels, asked_hbm, returned_ref, push_hbm, spread_cost_ref, gradient_hbm, give_out, left_out, right_out, up_out, down_out, push, gradient, asked_ref, scratch, sems):
    squares, copies = gather_gradient(
        slots, levels, asked_hbm, asked_ref, returned_ref, push_hbm, push, gradient, gradient_hbm, sems
    )
    sources = give_out.shape[0]
    sums = paired(squares, seen_cost(returned_ref, slots) + spread_cost_ref[0:1, :])
    give_out[...] = jnp.zeros_like(give_out)
    give_out[:, 3 * slots, :] = jnp.broadcast_to(sums, (sources, LANES))
    me = own_place()
    runs = gradient.shape[2] // LANES

    def one(s):
        for p in range(slots):
            row, run = block_at(asked_ref[s, me * slots + p], runs)
            for k in range(3):
                give_out[s, 3 * p + k : 3 * p + k + 1, :] = read_block(gradient, k, row, run)

    for_slots(sources, one)
    for (along_tile, along_radar), line in zip(CORNERS, corner_lines(gradient, levels)):
        exists, place = neighbour(along_tile, along_radar)

        @pl.when(exists)
        def _():
            give_out[place, 3 * slots + 1 : 3 * slots + 2, :] = line

    edges_kernel(levels, gradient, left_out, right_out, up_out, down_out, scratch)
    for copy in copies:
        copy.wait()


def second_owner_kernel(slots, levels, asked_hbm, returned_ref, rest_hbm, rest_cost_ref, gradient_out, give_out, up_out, down_out, rest, asked_ref, scratch, give_ref, sems):
    rows, width = gradient_out.shape[1], gradient_out.shape[2]
    squares, _ = gather_gradient(
        slots, levels, asked_hbm, asked_ref, returned_ref, rest_hbm, rest, gradient_out, None, sems
    )
    sums = paired(squares, seen_cost(returned_ref, slots) + rest_cost_ref[0:1, :])
    give_ref[...] = jnp.zeros_like(give_ref)
    for i in range(SPLIT):
        part = sums.astype(BF16).astype(F32)
        give_ref[:, i, :] = jnp.broadcast_to(part, (give_ref.shape[0], LANES))
        sums = sums - part
    for k in range(3):
        up_out[k] = gradient_out[k, 0:levels, :].astype(BF16)
        down_out[k] = gradient_out[k, rows - levels : rows, :].astype(BF16)
    lane = iota((levels, LANES), 1)
    for x in range(rows // levels):
        here = slice(x * levels, (x + 1) * levels)
        packed = jnp.zeros((levels, LANES), F32)
        for k in range(3):
            packed = lane_column(packed, lane, gradient_out[k, here, :LANES], 0, k)
            packed = lane_column(packed, lane, gradient_out[k, here, width - LANES :], LANES - 1, LANES - 8 + k)
        scratch[here, :] = packed
    turned = scratch[...].T
    lines = rows // LANES
    for along_radar, first in ((-1, 0), (1, LANES - 8)):
        exists, place = neighbour(0, along_radar)

        @pl.when(exists)
        def _():
            for k in range(3):
                for q in range(lines):
                    row = SPLIT + k * lines + q
                    piece = turned[first + k : first + k + 1, q * LANES : (q + 1) * LANES]
                    give_ref[place, row : row + 1, :] = piece

    give_out[...] = give_ref[...].astype(BF16)


def final_kernel(levels, total_cells, total_gates, sums_ref, first_cost_hbm, step_ref, wind_hbm, gradient_ref, left_0, right_0, above_0, below_0, left_1, right_1, above_1, below_1, above_ref, below_ref, wind_out, strain_out, cost_out, left_rows, right_rows, wind, strain, first_cost_ref, sems, cost_sem):
    rows = gradient_ref.shape[1]
    cells = rows // levels
    winds = Pieces(wind_hbm, wind, sems.at[0], FINAL_PARTS).start()
    cost_copy = pltpu.make_async_copy(first_cost_hbm, first_cost_ref, cost_sem)
    cost_copy.start()
    wind_outs = OutPieces(wind, wind_out, sems.at[1], FINAL_PARTS)
    strain_outs = OutPieces(strain, strain_out, sems.at[2], FINAL_PARTS)
    squares, cost = halves(jnp.sum(jnp.sum(sums_ref[:, 0:SPLIT, :].astype(F32), axis=0), axis=0, keepdims=True))
    step = STEP_LENGTH / jnp.sqrt(squares / total_cells + EPSILON)
    cost_out[1] = (cost / total_gates)[0, 0]
    first_step = step_ref[0:1, 0:1]
    lines = rows // LANES
    for along_radar, out, background, bent in ((-1, left_rows, left_0, left_1), (1, right_rows, right_0, right_1)):
        exists, place = neighbour(0, along_radar)
        columns = []
        block = sums_ref[pl.ds(place, 1)].reshape(sums_ref.shape[1:]).astype(F32)
        for k in range(3):
            at = slice(COL_WIND[k], COL_WIND[k] + 1)
            sent = [block[SPLIT + k * lines + q : SPLIT + 1 + k * lines + q] for q in range(lines)]
            sent = jnp.where(exists, jnp.concatenate(sent, axis=1), 0.0)
            columns.append(background[at, :] - first_step * bent[at, :] - step * sent)
        out[...] = to_rows(jnp.concatenate(columns + [jnp.zeros((5, rows), F32)], axis=0))

    def settle(x):
        here = slice(x * levels, (x + 1) * levels)
        winds.until(here.stop)
        for k in range(3):
            wind[k, here, :] = wind[k, here, :] - step * gradient_ref[k, here, :]
        wind_outs.filled(here.stop)

    settle(0)
    for x in range(cells):
        here = slice(x * levels, (x + 1) * levels)
        if x + 1 < cells:
            settle(x + 1)
        along = []
        for k in range(3):
            value = wind[k, here, :]
            if x + 1 < cells:
                after = wind[k, (x + 1) * levels : (x + 2) * levels, :]
            else:
                after = below_0[ROW_WIND[k]] - first_step * below_1[ROW_WIND[k]] - step * below_ref[k].astype(F32)
            if x > 0:
                before = wind[k, (x - 1) * levels : x * levels, :]
            else:
                before = above_0[ROW_WIND[k]] - first_step * above_1[ROW_WIND[k]] - step * above_ref[k].astype(F32)
            left = left_rows[here, k : k + 1]
            right = right_rows[here, k : k + 1]
            along.append((after - before, diff_columns(value, left, right), diff_levels(value, levels)))
        (xx, xy, xz), (yx, yy, yz), (zx, zy, zz) = along
        strain[0, here, :] = 0.5 * xx
        strain[1, here, :] = 0.5 * yy
        strain[2, here, :] = 0.5 * zz
        strain[3, here, :] = 0.25 * (xy + yx)
        strain[4, here, :] = 0.25 * (xz + zx)
        strain[5, here, :] = 0.25 * (yz + zy)
        strain_outs.filled(here.stop)
    cost_copy.wait()
    cost_out[0] = first_cost_ref[0, 0]
    wind_outs.finish()
    strain_outs.finish()


def shape(*dims, dtype=F32):
    return jax.ShapeDtypeStruct(dims, dtype)


VMEM = pl.BlockSpec(memory_space=pltpu.VMEM)
SMEM = pl.BlockSpec(memory_space=pltpu.SMEM)
ANY = pl.BlockSpec(memory_space=pl.ANY)


def call(kernel, out_shape, args, scratch=(), scalars=0, raw=(), out_raw=(), chip=(), out_chip=(), out_smem=(), out_vmem=False, flops=2000000, limit=16):
    single = not isinstance(out_shape, tuple)
    outs = (out_shape,) if single else out_shape
    held = [
        x if i < scalars or i in chip else pltpu.with_memory_space_constraint(x, pltpu.HBM)
        for i, x in enumerate(args)
    ]
    placed = tuple(o if i in out_chip or i in out_smem else pltpu.HBM(o.shape, o.dtype) for i, o in enumerate(outs))
    if out_vmem:
        placed = tuple(pltpu.VMEM(o.shape, o.dtype) for o in outs)
    specs = tuple(ANY if i in out_raw else SMEM if i in out_smem else VMEM for i in range(len(outs)))
    return pl.pallas_call(
        kernel,
        out_shape=placed[0] if single else placed,
        in_specs=[SMEM if i < scalars else ANY if i in raw else VMEM for i in range(len(args))],
        out_specs=specs[0] if single else specs,
        scratch_shapes=list(scratch),
        compiler_params=pltpu.CompilerParams(vmem_limit_bytes=limit * 1024 * 1024),
        cost_estimate=pl.CostEstimate(flops=flops, bytes_accessed=1 << 20, transcendentals=0),
    )(*held)


def shards(background, interp, beam, observed, cell_block, sweep_count):
    radar_count = lax.axis_size("radar")
    tile_count = lax.axis_size("tile")
    devices = radar_count * tile_count
    width_x, levels, width_y = background.shape[1:]
    slots = interp.shape[0] // devices
    gate_size = interp.shape[1]
    rows = width_x * levels
    height = -(-(3 * slots + 2) // 8) * 8
    total_cells = float(3 * rows * width_y * devices)
    total_gates = float(interp.shape[0] * devices * gate_size)
    field = background.reshape(3, rows, width_y)
    lanes = -(-devices * slots // LANES) * LANES
    asked = call(ask_kernel, shape(devices, 1, lanes, dtype=jnp.int32), (cell_block.reshape(1, -1),), chip=(0,))
    asked = exchange(asked)

    edges = (shape(8, rows), shape(8, rows))
    row_edges = (shape(4, levels, width_y), shape(4, levels, width_y))
    grid = shape(3, rows, width_y)
    line_out = shape(8, LANES)
    side = pltpu.VMEM((rows, LANES), F32)
    whole = pltpu.VMEM((3, rows, width_y), F32)
    plane = pltpu.VMEM((rows, width_y), F32)
    ring = pltpu.VMEM((rows + 2 * levels, width_y), F32)
    strip = pltpu.VMEM((levels, width_y), F32)
    semaphores = pltpu.SemaphoreType.DMA
    places = pltpu.SMEM((devices, lanes), jnp.int32)

    def halo(left, right, up, down):
        from_left = shifted(right, "radar", 1)
        from_right = shifted(left, "radar", -1)
        above = shifted(down, "tile", 1)
        below = shifted(up, "tile", -1)
        return from_left, from_right, above, below

    def edges_of(values):
        out = call(
            functools.partial(streamed_edges_kernel, levels),
            edges + row_edges,
            (values,),
            (side, whole, semaphores((PARTS,))),
            raw=(0,),
        )
        return halo(*out)

    around = edges_of(field)
    around_0 = around
    cells = call(
        functools.partial(pick_kernel, slots, levels),
        shape(devices, height, LANES, dtype=BF16),
        (asked, field),
        (pltpu.VMEM((devices, height, LANES), F32), places, semaphores),
        chip=(0, 1),
        raw=(0,),
    )
    cells = exchange(cells)
    products = (
        pltpu.VMEM((slots, devices * height, LANES), F32),
        pltpu.VMEM((slots, devices * height, LANES), F32),
        pltpu.VMEM((devices * height, LANES), F32),
    )
    weights, sight = call(
        functools.partial(source_kernel, slots),
        (shape(*interp.shape, dtype=BF16), shape(4 * slots, devices, gate_size)),
        (interp, beam.transpose(1, 0, 2), observed, sweep_count),
        (
            pltpu.VMEM((3,) + observed.shape, BF16),
            pltpu.VMEM(observed.shape, BF16),
            pltpu.VMEM(sweep_count.shape, jnp.int32),
            pltpu.VMEM((4,) + observed.shape, F32),
            semaphores((4,)),
        ),
        raw=(0, 1, 2, 3),
        out_vmem=True,
    )
    returned, misfit = call(
        functools.partial(first_source_kernel, slots),
        (shape(devices, height, LANES, dtype=BF16), shape(slots, devices, LANES)),
        (cells, weights, sight),
        products,
        chip=(0, 1, 2),
        out_chip=(1,),
    )
    returned = exchange(returned)
    push, spread, spread_cost = call(
        functools.partial(first_cycle_kernel, levels, slots),
        (grid, shape(rows, width_y), line_out),
        (field,) + around + (cells,),
        (whole, whole, ring, side, side, strip, semaphores((3, PARTS))),
        chip=(1, 2, 3, 4, 5),
        raw=(0,),
        out_raw=(0, 1),
        out_chip=(2,),
    )
    gradient, give, *sides = call(
        functools.partial(first_owner_kernel, slots, levels),
        (grid, shape(devices, height, LANES)) + edges + row_edges,
        (asked, returned, push, spread_cost),
        (whole, whole, places, side, semaphores((width_x + 2,))),
        chip=(0, 1, 3),
        raw=(0, 2),
        out_raw=(0,),
    )
    got = exchange(give)
    around = halo(*sides)
    around_1 = around
    returned, step, first_cost = call(
        functools.partial(second_source_kernel, slots, total_cells, total_gates),
        (shape(devices, height, LANES, dtype=BF16), line_out, line_out),
        (got, weights, sight, misfit),
        products,
        chip=(0, 1, 2, 3),
        out_chip=(1,),
    )
    returned = exchange(returned)
    rest, wind, rest_cost = call(
        functools.partial(second_cycle_kernel, levels, slots),
        (grid, grid, line_out),
        (gradient,) + around + (got, field, push, spread, step),
        (whole, whole, whole, plane, ring, side, side, strip, semaphores((6, PARTS))),
        chip=(1, 2, 3, 4, 5, 9),
        raw=(0, 6, 7, 8),
        out_raw=(0, 1),
        out_chip=(2,),
    )
    last_rows = (shape(3, levels, width_y, dtype=BF16), shape(3, levels, width_y, dtype=BF16))
    sent = -(-(SPLIT + 3 * rows // LANES) // 8) * 8
    gradient, give, up, down = call(
        functools.partial(second_owner_kernel, slots, levels),
        (grid, shape(devices, sent, LANES, dtype=BF16)) + last_rows,
        (asked, returned, rest, rest_cost),
        (whole, places, side, pltpu.VMEM((devices, sent, LANES), F32), semaphores((width_x + 2,))),
        chip=(0, 1, 3),
        raw=(0, 2),
        out_chip=(0,),
    )
    sums = exchange(give)
    above = shifted(down, "tile", 1)
    below = shifted(up, "tile", -1)
    wind, strain, costs = call(
        functools.partial(final_kernel, levels, total_cells, total_gates),
        (grid, shape(6, rows, width_y), shape(2)),
        (sums, first_cost, step, wind, gradient) + around_0 + around_1 + (above, below),
        (
            side,
            side,
            pltpu.VMEM((3, rows, width_y), F32),
            pltpu.VMEM((6, rows, width_y), F32),
            pltpu.SMEM((8, LANES), F32),
            semaphores((3, FINAL_PARTS)),
            semaphores,
        ),
        chip=(0, 4, 13, 14),
        raw=(1, 3),
        out_raw=(0, 1),
        out_smem=(2,),
    )
    return (
        wind.reshape(background.shape),
        strain.reshape(6, width_x, levels, width_y),
        costs,
    )


def solution(mesh):
    placed = (
        P(None, "tile", None, "radar"),
        P(("radar", "tile"), None, None),
        P(("radar", "tile"), None, None),
        P(("radar", "tile"), None),
        P(("radar", "tile")),
        P(("radar", "tile"), None),
    )

    return jax.shard_map(
        shards,
        mesh=mesh,
        in_specs=placed,
        out_specs=(P(None, "tile", None, "radar"), P(None, "tile", None, "radar"), P()),
        check_vma=False,
    )
```

```python
import functools

import jax
import jax.numpy as jnp
from jax import lax
from jax.experimental import pallas as pl
from jax.experimental.pallas import tpu as pltpu
from jax.sharding import PartitionSpec as P


BACKGROUND_WEIGHT = 0.5
DIVERGENCE_WEIGHT = 1.0
STEP_LENGTH = 0.3
EPSILON = 1e-06

AXES = ("radar", "tile")
LANES = 128
PARTS = 4
SPLIT = 3
FINAL_PARTS = 8
F32 = jnp.float32
BF16 = jnp.bfloat16

COL_WY, COL_WX, COL_PART, COL_WZ = 0, 1, 2, 3
COL_WIND = (COL_WX, COL_WY, COL_WZ)
ROW_WX, ROW_PART, ROW_WY, ROW_WZ = 0, 1, 2, 3
ROW_WIND = (ROW_WX, ROW_WY, ROW_WZ)
CORNERS = ((-1, -1), (-1, 1), (1, -1), (1, 1))


def exchange(x):
    return lax.all_to_all(x, AXES, split_axis=0, concat_axis=0, tiled=True)


def shifted(x, axis, step):
    size = lax.axis_size(axis)
    pairs = [(i, i + step) for i in range(size) if 0 <= i + step < size]
    return lax.ppermute(x, axis, pairs)


class Pieces:
    def __init__(self, source, target, sems, parts, at=0):
        rows = source.shape[-2]
        self.share = rows // parts
        self.copies = []
        self.seen = 0
        for i in range(parts):
            here = pl.ds(i * self.share, self.share)
            there = pl.ds(at + i * self.share, self.share)
            lead = (slice(None),) * (len(source.shape) - 2)
            self.copies.append(pltpu.make_async_copy(source.at[lead + (here,)], target.at[lead + (there,)], sems.at[i]))

    def start(self):
        for copy in self.copies:
            copy.start()
        return self

    def until(self, row):
        while self.seen < len(self.copies) and self.seen * self.share < row:
            self.copies[self.seen].wait()
            self.seen += 1

    def filled(self, row):
        while self.seen < len(self.copies) and (self.seen + 1) * self.share <= row:
            self.copies[self.seen].start()
            self.seen += 1

    def finish(self):
        for copy in self.copies:
            copy.wait()


class OutPieces(Pieces):
    def __init__(self, source, target, sems, parts, at=0):
        rows = target.shape[-2]
        self.share = rows // parts
        self.copies = []
        self.seen = 0
        for i in range(parts):
            here = pl.ds(at + i * self.share, self.share)
            there = pl.ds(i * self.share, self.share)
            lead = (slice(None),) * (len(source.shape) - 2)
            self.copies.append(pltpu.make_async_copy(source.at[lead + (here,)], target.at[lead + (there,)], sems.at[i]))


def iota(shape, dim):
    return lax.broadcasted_iota(jnp.int32, shape, dim)


def diff_levels(a, period):
    rows = a.shape[0]
    level = lax.rem(iota(a.shape, 0), jnp.int32(period))
    above = jnp.where(level == period - 1, 0.0, pltpu.roll(a, rows - 1, 0))
    below = jnp.where(level == 0, 0.0, pltpu.roll(a, 1, 0))
    return above - below


def diff_columns(a, left, right):
    width = a.shape[1]
    lane = iota(a.shape, 1)
    after = jnp.where(lane == width - 1, right, pltpu.roll(a, width - 1, 1))
    before = jnp.where(lane == 0, left, pltpu.roll(a, 1, 1))
    return after - before


def to_rows(columns):
    fill = jnp.zeros((LANES - columns.shape[0], columns.shape[1]), F32)
    return jnp.concatenate([columns, fill], axis=0).T


def sum_rows(a):
    total = a[:, :LANES]
    for start in range(LANES, a.shape[1], LANES):
        total = total + a[:, start : start + LANES]
    return jnp.sum(total, axis=0, keepdims=True)


def paired(first, second):
    half = LANES // 2
    lower = iota((1, LANES), 1) < half
    return jnp.where(lower, first + pltpu.roll(first, half, 1), second + pltpu.roll(second, half, 1))


def halves(line):
    lower = iota((1, LANES), 1) < LANES // 2
    return (
        jnp.sum(jnp.where(lower, line, 0.0), axis=1, keepdims=True),
        jnp.sum(jnp.where(lower, 0.0, line), axis=1, keepdims=True),
    )


def in_parts(line, count):
    parts = []
    for _ in range(count):
        parts.append(line.astype(BF16).astype(F32))
        line = line - parts[-1]
    return parts


def put_columns(ref, place, row, columns, lines):
    for i, column in enumerate(columns):
        for q in range(lines):
            at = row + i * lines + q
            ref[place, at : at + 1, :] = column[:, q * LANES : (q + 1) * LANES]


def take_columns(block, row, count, lines):
    return [
        jnp.concatenate([block[row + i * lines + q : row + i * lines + q + 1] for q in range(lines)], axis=1)
        for i in range(count)
    ]


def block_of(ref, place):
    return ref[pl.ds(place, 1)].reshape(ref.shape[1:]).astype(F32)


def own_place():
    return lax.axis_index("radar") * lax.axis_size("tile") + lax.axis_index("tile")


def neighbour(along_tile, along_radar):
    tile = lax.axis_index("tile") + along_tile
    radar = lax.axis_index("radar") + along_radar
    exists = (tile >= 0) & (tile < lax.axis_size("tile")) & (radar >= 0) & (radar < lax.axis_size("radar"))
    return exists, jnp.where(exists, radar * lax.axis_size("tile") + tile, own_place())


def corner_lines(w_ref, levels):
    rows, width = w_ref.shape[1], w_ref.shape[2]
    lane = iota((levels, LANES), 1)
    packed = jnp.zeros((levels, LANES), F32)
    for c, (along_tile, along_radar) in enumerate(CORNERS):
        here = slice(0, levels) if along_tile < 0 else slice(rows - levels, rows)
        lanes, at = (slice(0, LANES), 0) if along_radar < 0 else (slice(width - LANES, width), LANES - 1)
        for k in range(2):
            packed = lane_column(packed, lane, w_ref[k, here, lanes], at, 2 * c + k)
    turned = jnp.concatenate([packed, jnp.zeros((LANES - levels, LANES), F32)], axis=0).T
    return [
        turned[2 * c : 2 * c + 1] + pltpu.roll(turned[2 * c + 1 : 2 * c + 2], levels, 1) for c in range(len(CORNERS))
    ]


def corner_columns(line_from, levels):
    lines = []
    for along_tile, along_radar in CORNERS:
        exists, place = neighbour(along_tile, along_radar)
        lines.append(jnp.where(exists, line_from(place), 0.0))
    fill = jnp.zeros((LANES - len(CORNERS), LANES), F32)
    turned = jnp.concatenate(lines + [fill], axis=0).T
    return [(turned[0:levels, c : c + 1], turned[levels : 2 * levels, c : c + 1]) for c in range(len(CORNERS))]


def block_at(index, runs):
    if runs & (runs - 1) == 0:
        return lax.shift_right_logical(index, jnp.int32(runs.bit_length() - 1)), index & (runs - 1)
    return lax.div(index, jnp.int32(runs)), lax.rem(index, jnp.int32(runs))


def read_block(ref, k, row, run):
    line = ref[k, pl.ds(row, 1), :]
    out = line[:, :LANES]
    for h in range(1, ref.shape[2] // LANES):
        out = jnp.where(run == h, line[:, h * LANES : (h + 1) * LANES], out)
    return out


def lane_column(packed, lane, tile, at, to):
    moved = tile if at == to else pltpu.roll(tile, (to - at) % LANES, 1)
    return jnp.where(lane == to, moved, packed)


def streamed_edges_kernel(levels, w_hbm, left_out, right_out, up_out, down_out, scratch, w_ref, sems):
    fields = Pieces(w_hbm, w_ref, sems, PARTS).start()
    edges_kernel(levels, w_ref, left_out, right_out, up_out, down_out, scratch, fields.until)


def edges_kernel(levels, w_ref, left_out, right_out, up_out, down_out, scratch, need=lambda row: None):
    rows, width = w_ref.shape[1], w_ref.shape[2]
    lane = iota((levels, LANES), 1)
    last = slice(width - LANES, width)
    for x in range(rows // levels):
        here = slice(x * levels, (x + 1) * levels)
        need(here.stop)
        packed = jnp.where(lane < LANES // 2, w_ref[1, here, :LANES], w_ref[1, here, last])
        packed = lane_column(packed, lane, w_ref[0, here, :LANES], 0, 2)
        packed = lane_column(packed, lane, w_ref[2, here, :LANES], 0, 3)
        packed = lane_column(packed, lane, w_ref[0, here, last], LANES - 1, LANES - 3)
        packed = lane_column(packed, lane, w_ref[2, here, last], LANES - 1, LANES - 4)
        scratch[here, :] = packed
    turned = scratch[...].T
    place = iota((1, rows), 1)
    level = lax.rem(place, jnp.int32(levels))

    def partial(wx, wz):
        part = jnp.where(level == levels - 1, 0.0, pltpu.roll(wz, rows - 1, 1))
        part = part - jnp.where(level == 0, 0.0, pltpu.roll(wz, 1, 1))
        part = part + jnp.where(place >= rows - levels, 0.0, pltpu.roll(wx, rows - levels, 1))
        return part - jnp.where(place < levels, 0.0, pltpu.roll(wx, levels, 1))

    near, far = turned[0:8], turned[LANES - 8 : LANES]
    for out, wy, inner, wx, wz in (
        (left_out, near[0:1], near[1:2], near[2:3], near[3:4]),
        (right_out, far[7:8], -far[6:7], far[5:6], far[4:5]),
    ):
        out[...] = jnp.zeros_like(out)
        out[COL_WY : COL_WY + 1, :] = wy
        out[COL_WX : COL_WX + 1, :] = wx
        out[COL_PART : COL_PART + 1, :] = 0.5 * (inner + partial(wx, wz))
        out[COL_WZ : COL_WZ + 1, :] = wz
    for out, first in ((up_out, 0), (down_out, rows - levels)):
        here = slice(first, first + levels)
        part = diff_levels(w_ref[2, here, :], levels) + diff_columns(w_ref[1, here, :], 0.0, 0.0)
        if first > 0:
            part = part - w_ref[0, first - levels : first, :]
        else:
            part = part + w_ref[0, levels : 2 * levels, :]
        out[ROW_WX] = w_ref[0, here, :]
        out[ROW_PART] = 0.5 * part
        out[ROW_WY] = w_ref[1, here, :]
        out[ROW_WZ] = w_ref[2, here, :]


def cycle(levels, w_ref, left, right, above_ref, below_ref, corners, ring, left_rows, right_rows, need, take_spread, take_push):
    rows, width = w_ref.shape[1], w_ref.shape[2]
    cells = rows // levels
    left_rows[...] = to_rows(left)
    right_rows[...] = to_rows(right)
    has_left = jnp.where(lax.axis_index("radar") > 0, 1.0, 0.0)
    has_right = jnp.where(lax.axis_index("radar") < lax.axis_size("radar") - 1, 1.0, 0.0)
    has_above = jnp.where(lax.axis_index("tile") > 0, 1.0, 0.0)
    has_below = jnp.where(lax.axis_index("tile") < lax.axis_size("tile") - 1, 1.0, 0.0)
    above_left, above_right, below_left, below_right = corners
    lane = iota((levels, width), 1)

    def ends(left, right):
        return jnp.where(lane == 0, -0.5 * left, jnp.where(lane == width - 1, 0.5 * right, 0.0))

    first, last = slice(0, levels), slice(rows - levels, rows)
    for x in range(cells):
        here = slice(x * levels, (x + 1) * levels)
        need(min(rows, (x + 2) * levels))
        after = w_ref[0, (x + 1) * levels : (x + 2) * levels, :] if x + 1 < cells else below_ref[ROW_WX]
        before = w_ref[0, (x - 1) * levels : x * levels, :] if x > 0 else above_ref[ROW_WX]
        spread = 0.5 * (
            (after - before)
            + diff_columns(
                w_ref[1, here, :],
                left_rows[here, COL_WY : COL_WY + 1],
                right_rows[here, COL_WY : COL_WY + 1],
            )
            + diff_levels(w_ref[2, here, :], levels)
        )
        ring[(x + 1) * levels : (x + 2) * levels, :] = spread
        take_spread(here, spread)
    above = above_ref[ROW_PART] + 0.5 * w_ref[0, first, :] + ends(above_left[1], above_right[1])
    below = below_ref[ROW_PART] - 0.5 * w_ref[0, last, :] + ends(below_left[1], below_right[1])
    ring[0:levels, :] = has_above * above
    ring[rows + levels : rows + 2 * levels, :] = has_below * below
    for x in range(cells):
        here = slice(x * levels, (x + 1) * levels)
        left = left_rows[here, COL_PART : COL_PART + 1] + 0.5 * w_ref[1, here, 0:1]
        right = right_rows[here, COL_PART : COL_PART + 1] - 0.5 * w_ref[1, here, width - 1 : width]
        if x == 0:
            left = left - 0.5 * above_left[0]
            right = right - 0.5 * above_right[0]
        if x == cells - 1:
            left = left + 0.5 * below_left[0]
            right = right + 0.5 * below_right[0]
        spread = ring[(x + 1) * levels : (x + 2) * levels, :]
        after = ring[(x + 2) * levels : (x + 3) * levels, :]
        before = ring[x * levels : (x + 1) * levels, :]
        take_push(0, here, (-0.5 * DIVERGENCE_WEIGHT) * (after - before))
        take_push(1, here, (-0.5 * DIVERGENCE_WEIGHT) * diff_columns(spread, has_left * left, has_right * right))
        take_push(2, here, (-0.5 * DIVERGENCE_WEIGHT) * diff_levels(spread, levels))


def first_cycle_kernel(levels, slots, w_hbm, left_ref, right_ref, above_ref, below_ref, cells_ref, push_hbm, spread_hbm, total_out, w_ref, push, ring, left_rows, right_rows, total, sems):
    fields = Pieces(w_hbm, w_ref, sems.at[0], PARTS).start()
    total[...] = jnp.zeros_like(total)
    spreads = OutPieces(ring, spread_hbm, sems.at[1], PARTS, levels)
    pushes = OutPieces(push, push_hbm, sems.at[2], PARTS)

    def line_from(place):
        block = cells_ref[pl.ds(place, 1)].reshape(cells_ref.shape[1:]).astype(F32)
        first = block[3 * slots : 3 * slots + 1]
        return first + pltpu.roll(first, LANES // 2, 1) + block[3 * slots + 1 : 3 * slots + 2]

    def take_spread(here, spread):
        total[...] += spread * spread
        spreads.filled(here.stop)

    def take_push(k, here, value):
        push[k, here, :] = value
        if k == 2:
            pushes.filled(here.stop)

    corners = corner_columns(line_from, levels)
    cycle(levels, w_ref, left_ref[...], right_ref[...], above_ref, below_ref, corners, ring, left_rows, right_rows, fields.until, take_spread, take_push)
    total_out[...] = jnp.broadcast_to(0.5 * DIVERGENCE_WEIGHT * sum_rows(total[...]), total_out.shape)
    spreads.finish()
    pushes.finish()


def second_cycle_kernel(levels, slots, w_hbm, above_ref, below_ref, got_ref, background_hbm, push_hbm, spread_hbm, step_ref, rest_hbm, wind_hbm, total_out, w_ref, background, push, spread, ring, left_rows, right_rows, total, sems):
    fields = Pieces(w_hbm, w_ref, sems.at[0], PARTS).start()
    spreads = Pieces(spread_hbm, spread, sems.at[1], PARTS).start()
    pushes = Pieces(push_hbm, push, sems.at[2], PARTS).start()
    backgrounds = Pieces(background_hbm, background, sems.at[3], PARTS).start()
    rests = OutPieces(push, rest_hbm, sems.at[4], PARTS)
    winds = OutPieces(background, wind_hbm, sems.at[5], PARTS)
    total[...] = jnp.zeros_like(total)
    step = step_ref[0:1, 0:1]

    def line_from(place):
        block = block_of(got_ref, place)
        first = block[3 * slots + SPLIT : 3 * slots + SPLIT + 1]
        return first + pltpu.roll(first, LANES // 2, 1) + block[3 * slots + SPLIT + 1 : 3 * slots + SPLIT + 2]

    lines = w_ref.shape[1] // LANES
    sides = []
    for along_radar in (-1, 1):
        exists, place = neighbour(0, along_radar)
        wy, part = take_columns(block_of(got_ref, place), 3 * slots + SPLIT + 2, 2, lines)
        fill = jnp.zeros_like(wy)
        columns = [fill] * 8
        columns[COL_WY], columns[COL_PART] = jnp.where(exists, wy, 0.0), jnp.where(exists, part, 0.0)
        sides.append(jnp.concatenate(columns, axis=0))

    def take_spread(here, bent):
        spreads.until(here.stop)
        value = spread[here, :] - step * bent
        total[...] += (0.5 * DIVERGENCE_WEIGHT) * (value * value)

    def take_push(k, here, bent):
        pushes.until(here.stop)
        backgrounds.until(here.stop)
        offset = step * w_ref[k, here, :]
        total[...] += (0.5 * BACKGROUND_WEIGHT) * (offset * offset)
        background[k, here, :] = background[k, here, :] - offset
        push[k, here, :] = push[k, here, :] - (BACKGROUND_WEIGHT * offset + step * bent)
        if k == 2:
            rests.filled(here.stop)
            winds.filled(here.stop)

    corners = corner_columns(line_from, levels)
    cycle(levels, w_ref, *sides, above_ref, below_ref, corners, ring, left_rows, right_rows, fields.until, take_spread, take_push)
    total_out[...] = jnp.broadcast_to(sum_rows(total[...]), total_out.shape)
    rests.finish()
    winds.finish()


def for_slots(count, body, step=8):
    step = min(step, count)

    def run(i, carry):
        for j in range(step):
            body(i * step + j)
        return carry

    lax.fori_loop(0, count // step, run, 0)


def ask_kernel(places_ref, out_ref):
    line = places_ref[...]
    if line.shape[1] < out_ref.shape[2]:
        line = jnp.concatenate([line, jnp.zeros((1, out_ref.shape[2] - line.shape[1]), jnp.int32)], axis=1)
    out_ref[...] = jnp.broadcast_to(line[None], out_ref.shape)


def ask(asked_hbm, asked_ref, sem):
    return pltpu.make_async_copy(asked_hbm.at[:, 0, :], asked_ref, sem)


def pick_kernel(slots, levels, asked_hbm, w_ref, out_ref, rows_ref, asked_ref, ask_sem):
    asking = ask(asked_hbm, asked_ref, ask_sem)
    asking.start()
    me = own_place()
    runs = w_ref.shape[2] // LANES
    rows_ref[...] = jnp.zeros_like(rows_ref)
    asking.wait()

    def one(s):
        for p in range(slots):
            row, run = block_at(asked_ref[s, me * slots + p], runs)
            for k in range(3):
                rows_ref[s, 3 * p + k : 3 * p + k + 1, :] = read_block(w_ref, k, row, run)

    for_slots(out_ref.shape[0], one)
    for (along_tile, along_radar), line in zip(CORNERS, corner_lines(w_ref, levels)):
        exists, place = neighbour(along_tile, along_radar)
        high = line.astype(BF16).astype(F32)
        middle = (line - high).astype(BF16).astype(F32)

        @pl.when(exists)
        def _():
            rows_ref[place, 3 * slots : 3 * slots + 1, :] = high + pltpu.roll(middle, LANES // 2, 1)
            rows_ref[place, 3 * slots + 1 : 3 * slots + 2, :] = line - high - middle

    out_ref[...] = rows_ref[...].astype(out_ref.dtype)


def source_kernel(slots, weights_hbm, beam_hbm, observed_hbm, count_hbm, weights_out, sight_out, beam_ref, observed_ref, count_ref, wide_ref, sems):
    pairs = (
        (count_hbm, count_ref),
        (beam_hbm, beam_ref),
        (observed_hbm, observed_ref),
        (weights_hbm, weights_out),
    )
    copies = [pltpu.make_async_copy(source, target, sems.at[i]) for i, (source, target) in enumerate(pairs)]
    for copy in copies:
        copy.start()
    sources = sight_out.shape[1]
    diagonal = iota((sources, sources), 0) == iota((sources, sources), 1)
    for copy in copies[:3]:
        copy.wait()
    counts = jnp.sum(jnp.where(diagonal, count_ref[...].astype(F32), 0.0), axis=1, keepdims=True)
    for k in range(4):
        wide_ref[k] = (beam_ref[k] if k < 3 else observed_ref[...]).astype(F32)
        for p in range(slots):
            live = jnp.where(counts > p, wide_ref[k, pl.ds(p, sources, stride=slots), :], 0.0)
            sight_out[3 * p + k if k < 3 else 3 * slots + p] = live
    copies[3].wait()


def project(cells_of, weights_ref, proj_ref, sources, slots, height):
    def one(s):
        weights = weights_ref[pl.ds(s * slots, slots)].reshape(slots * LANES, LANES)
        seen = lax.dot_general(cells_of(s), weights, (((1,), (1,)), ((), ())), preferred_element_type=F32)
        here = pl.ds(pl.multiple_of(s * height, height), height)
        for p in range(slots):
            proj_ref[p, here, :] = seen[:, p * LANES : (p + 1) * LANES]

    for_slots(sources, one, 16)


def radial(proj_ref, sight_ref, p, sources, height):
    total = jnp.zeros((sources, LANES), F32)
    for k in range(3):
        total = total + sight_ref[3 * p + k] * proj_ref[p, pl.ds(3 * p + k, sources, stride=height), :]
    return total


def give_back(misfits, weights_ref, sight_ref, adj_ref, line_ref, out_ref, sources, slots, height):
    adj_ref[...] = jnp.zeros_like(adj_ref)
    cost = jnp.zeros((sources, LANES), F32)
    for p in range(slots):
        cost = cost + 0.5 * (misfits[p] * misfits[p])
        for k in range(3):
            adj_ref[p, pl.ds(3 * p + k, sources, stride=height), :] = sight_ref[3 * p + k] * misfits[p]
    high = cost.astype(BF16).astype(F32)
    line_ref[...] = jnp.zeros_like(line_ref)
    line_ref[pl.ds(3 * slots, sources, stride=height), :] = high
    line_ref[pl.ds(3 * slots + 1, sources, stride=height), :] = cost - high

    def one(s):
        weights = weights_ref[pl.ds(s * slots, slots)].reshape(slots * LANES, LANES)
        here = pl.ds(pl.multiple_of(s * height, height), height)
        adjoint = jnp.concatenate([adj_ref[p, here, :] for p in range(slots)], axis=1).astype(BF16)
        product = lax.dot_general(adjoint, weights, (((1,), (0,)), ((), ())), preferred_element_type=F32)
        out_ref[s] = (product + line_ref[here, :]).astype(out_ref.dtype)

    for_slots(sources, one, 16)


def first_source_kernel(slots, cells_ref, weights_ref, sight_ref, returned_out, misfit_out, proj_ref, adj_ref, line_ref):
    sources, height = cells_ref.shape[0], cells_ref.shape[1]
    project(lambda s: cells_ref[s].astype(BF16), weights_ref, proj_ref, sources, slots, height)
    misfits = []
    for p in range(slots):
        misfit = radial(proj_ref, sight_ref, p, sources, height) - sight_ref[3 * slots + p]
        misfit_out[p] = misfit
        misfits.append(misfit)
    give_back(misfits, weights_ref, sight_ref, adj_ref, line_ref, returned_out, sources, slots, height)


def second_source_kernel(slots, total_cells, total_gates, got_ref, weights_ref, sight_ref, misfit_ref, returned_out, step_out, cost_out, proj_ref, adj_ref, line_ref):
    sources, height = returned_out.shape[0], returned_out.shape[1]
    project(lambda s: got_ref[s, 0:height], weights_ref, proj_ref, sources, slots, height)
    squares, costs = halves(
        jnp.sum(jnp.sum(got_ref[:, 3 * slots : 3 * slots + SPLIT, :].astype(F32), axis=0), axis=0, keepdims=True)
    )
    step = STEP_LENGTH / jnp.sqrt(squares / total_cells + EPSILON)
    step_out[...] = jnp.broadcast_to(step, step_out.shape)
    cost_out[...] = jnp.broadcast_to(costs / total_gates, cost_out.shape)
    misfits = [
        misfit_ref[p] - step * radial(proj_ref, sight_ref, p, sources, height) for p in range(slots)
    ]
    give_back(misfits, weights_ref, sight_ref, adj_ref, line_ref, returned_out, sources, slots, height)


def scatter_rows(slots, asked_ref, returned_ref, out_ref):
    me = own_place()
    runs = out_ref.shape[2] // LANES
    place = iota((8, LANES), 0)

    def one(s):
        block = returned_ref[s].astype(F32)
        for p in range(slots):
            row, run = block_at(asked_ref[s, me * slots + p], runs)
            within = lax.rem(row, jnp.int32(8))
            base = pl.multiple_of(row - within, 8)
            lanes = pl.ds(pl.multiple_of(run * LANES, LANES), LANES)
            held = [out_ref[k, pl.ds(base, 8), lanes] for k in range(3)]
            for k in range(3):
                line = block[3 * p + k : 3 * p + k + 1, :]
                held[k] = held[k] + jnp.where(place == within, line, 0.0)
            for k in range(3):
                out_ref[k, pl.ds(base, 8), lanes] = held[k]

    for_slots(returned_ref.shape[0], one)


def gather_gradient(slots, levels, asked_hbm, asked_ref, returned_ref, rest_hbm, rest, gradient_ref, gradient_hbm, sems):
    rows, width = gradient_ref.shape[1], gradient_ref.shape[2]
    cells = rows // levels
    copy = pltpu.make_async_copy(rest_hbm, rest, sems.at[cells])
    asking = ask(asked_hbm, asked_ref, sems.at[cells + 1])
    asking.start()
    copy.start()
    gradient_ref[...] = jnp.zeros_like(gradient_ref)
    asking.wait()
    scatter_rows(slots, asked_ref, returned_ref, gradient_ref)
    copy.wait()
    total = jnp.zeros((levels, width), F32)
    copies = []
    for x in range(cells):
        here = slice(x * levels, (x + 1) * levels)
        for k in range(3):
            piece = gradient_ref[k, here, :] + rest[k, here, :]
            gradient_ref[k, here, :] = piece
            total = total + piece * piece
        if gradient_hbm is not None:
            copies.append(pltpu.make_async_copy(gradient_ref.at[:, here], gradient_hbm.at[:, here], sems.at[x]))
            copies[-1].start()
    return sum_rows(total), copies


def seen_cost(returned_ref, slots):
    cost = returned_ref[:, 3 * slots : 3 * slots + 2, :].astype(F32)
    return jnp.sum(jnp.sum(cost, axis=0), axis=0, keepdims=True)


def first_owner_kernel(slots, levels, asked_hbm, returned_ref, push_hbm, spread_cost_ref, gradient_hbm, give_out, left_out, right_out, up_out, down_out, push, gradient, asked_ref, scratch, give_ref, sems):
    squares, copies = gather_gradient(
        slots, levels, asked_hbm, asked_ref, returned_ref, push_hbm, push, gradient, gradient_hbm, sems
    )
    sources = give_out.shape[0]
    sums = paired(squares, seen_cost(returned_ref, slots) + spread_cost_ref[0:1, :])
    give_ref[...] = jnp.zeros_like(give_ref)
    for i, part in enumerate(in_parts(sums, SPLIT)):
        give_ref[:, 3 * slots + i, :] = jnp.broadcast_to(part, (sources, LANES))
    me = own_place()
    runs = gradient.shape[2] // LANES

    def one(s):
        for p in range(slots):
            row, run = block_at(asked_ref[s, me * slots + p], runs)
            for k in range(3):
                give_ref[s, 3 * p + k : 3 * p + k + 1, :] = read_block(gradient, k, row, run)

    for_slots(sources, one)
    for (along_tile, along_radar), line in zip(CORNERS, corner_lines(gradient, levels)):
        exists, place = neighbour(along_tile, along_radar)
        high, middle, low = in_parts(line, 3)

        @pl.when(exists)
        def _():
            row = 3 * slots + SPLIT
            give_ref[place, row : row + 1, :] = high + pltpu.roll(middle, LANES // 2, 1)
            give_ref[place, row + 1 : row + 2, :] = low

    edges_kernel(levels, gradient, left_out, right_out, up_out, down_out, scratch)
    lines = gradient.shape[1] // LANES
    for along_radar, ref in ((-1, left_out), (1, right_out)):
        exists, place = neighbour(0, along_radar)

        @pl.when(exists)
        def _():
            columns = [ref[f : f + 1, :] for f in (COL_WY, COL_PART)]
            put_columns(give_ref, place, 3 * slots + SPLIT + 2, columns, lines)

    give_out[...] = give_ref[...].astype(BF16)
    for copy in copies:
        copy.wait()


def second_owner_kernel(slots, levels, asked_hbm, returned_ref, rest_hbm, rest_cost_ref, left_hbm, right_hbm, gradient_out, give_out, up_out, down_out, rest, asked_ref, scratch, give_ref, bent_ref, sems, bent_sems):
    rows, width = gradient_out.shape[1], gradient_out.shape[2]
    bents = [
        pltpu.make_async_copy(source, bent_ref.at[i], bent_sems.at[i]) for i, source in enumerate((left_hbm, right_hbm))
    ]
    for copy in bents:
        copy.start()
    squares, _ = gather_gradient(
        slots, levels, asked_hbm, asked_ref, returned_ref, rest_hbm, rest, gradient_out, None, sems
    )
    sums = paired(squares, seen_cost(returned_ref, slots) + rest_cost_ref[0:1, :])
    give_ref[...] = jnp.zeros_like(give_ref)
    for i, part in enumerate(in_parts(sums, SPLIT)):
        give_ref[:, i, :] = jnp.broadcast_to(part, (give_ref.shape[0], LANES))
    for k in range(3):
        up_out[k] = gradient_out[k, 0:levels, :].astype(BF16)
        down_out[k] = gradient_out[k, rows - levels : rows, :].astype(BF16)
    lane = iota((levels, LANES), 1)
    for x in range(rows // levels):
        here = slice(x * levels, (x + 1) * levels)
        packed = jnp.zeros((levels, LANES), F32)
        for k in range(3):
            packed = lane_column(packed, lane, gradient_out[k, here, :LANES], 0, k)
            packed = lane_column(packed, lane, gradient_out[k, here, width - LANES :], LANES - 1, LANES - 8 + k)
        scratch[here, :] = packed
    turned = scratch[...].T
    lines = rows // LANES
    for copy in bents:
        copy.wait()
    for i, (along_radar, first) in enumerate(((-1, 0), (1, LANES - 8))):
        exists, place = neighbour(0, along_radar)

        @pl.when(exists)
        def _():
            columns = [turned[first + k : first + k + 1] for k in range(3)]
            columns += [bent_ref[i, f : f + 1, :] for f in (COL_WX, COL_WZ)]
            put_columns(give_ref, place, SPLIT, columns, lines)

    give_out[...] = give_ref[...].astype(BF16)


def final_kernel(levels, slots, total_cells, total_gates, sums_ref, first_cost_hbm, step_ref, wind_hbm, gradient_ref, left_0, right_0, above_0, below_0, got_hbm, above_1, below_1, above_ref, below_ref, wind_out, strain_out, cost_out, left_rows, right_rows, wind, strain, first_cost_ref, got_ref, sems, cost_sem, got_sems):
    rows = gradient_ref.shape[1]
    cells = rows // levels
    winds = Pieces(wind_hbm, wind, sems.at[0], FINAL_PARTS).start()
    cost_copy = pltpu.make_async_copy(first_cost_hbm, first_cost_ref, cost_sem)
    cost_copy.start()
    got_copies = []
    for i, along_radar in enumerate((-1, 1)):
        _, place = neighbour(0, along_radar)
        got_copies.append(pltpu.make_async_copy(got_hbm.at[place], got_ref.at[i], got_sems.at[i]))
        got_copies[-1].start()
    wind_outs = OutPieces(wind, wind_out, sems.at[1], FINAL_PARTS)
    strain_outs = OutPieces(strain, strain_out, sems.at[2], FINAL_PARTS)
    squares, cost = halves(jnp.sum(jnp.sum(sums_ref[:, 0:SPLIT, :].astype(F32), axis=0), axis=0, keepdims=True))
    step = STEP_LENGTH / jnp.sqrt(squares / total_cells + EPSILON)
    cost_out[1] = (cost / total_gates)[0, 0]
    first_step = step_ref[0:1, 0:1]
    lines = rows // LANES
    for copy in got_copies:
        copy.wait()
    for i, (along_radar, out, background) in enumerate(((-1, left_rows, left_0), (1, right_rows, right_0))):
        exists, place = neighbour(0, along_radar)
        *sent, bent_x, bent_z = take_columns(block_of(sums_ref, place), SPLIT, 5, lines)
        (bent_y,) = take_columns(got_ref[i].astype(F32), 3 * slots + SPLIT + 2, 1, lines)
        columns = []
        for k, bent in enumerate((bent_x, bent_y, bent_z)):
            change = jnp.where(exists, first_step * bent + step * sent[k], 0.0)
            columns.append(background[COL_WIND[k] : COL_WIND[k] + 1, :] - change)
        out[...] = to_rows(jnp.concatenate(columns + [jnp.zeros((5, rows), F32)], axis=0))

    def settle(x):
        here = slice(x * levels, (x + 1) * levels)
        winds.until(here.stop)
        for k in range(3):
            wind[k, here, :] = wind[k, here, :] - step * gradient_ref[k, here, :]
        wind_outs.filled(here.stop)

    settle(0)
    for x in range(cells):
        here = slice(x * levels, (x + 1) * levels)
        if x + 1 < cells:
            settle(x + 1)
        along = []
        for k in range(3):
            value = wind[k, here, :]
            if x + 1 < cells:
                after = wind[k, (x + 1) * levels : (x + 2) * levels, :]
            else:
                after = below_0[ROW_WIND[k]] - first_step * below_1[ROW_WIND[k]] - step * below_ref[k].astype(F32)
            if x > 0:
                before = wind[k, (x - 1) * levels : x * levels, :]
            else:
                before = above_0[ROW_WIND[k]] - first_step * above_1[ROW_WIND[k]] - step * above_ref[k].astype(F32)
            left = left_rows[here, k : k + 1]
            right = right_rows[here, k : k + 1]
            along.append((after - before, diff_columns(value, left, right), diff_levels(value, levels)))
        (xx, xy, xz), (yx, yy, yz), (zx, zy, zz) = along
        strain[0, here, :] = 0.5 * xx
        strain[1, here, :] = 0.5 * yy
        strain[2, here, :] = 0.5 * zz
        strain[3, here, :] = 0.25 * (xy + yx)
        strain[4, here, :] = 0.25 * (xz + zx)
        strain[5, here, :] = 0.25 * (yz + zy)
        strain_outs.filled(here.stop)
    cost_copy.wait()
    cost_out[0] = first_cost_ref[0, 0]
    wind_outs.finish()
    strain_outs.finish()


def shape(*dims, dtype=F32):
    return jax.ShapeDtypeStruct(dims, dtype)


VMEM = pl.BlockSpec(memory_space=pltpu.VMEM)
SMEM = pl.BlockSpec(memory_space=pltpu.SMEM)
ANY = pl.BlockSpec(memory_space=pl.ANY)


def call(kernel, out_shape, args, scratch=(), scalars=0, raw=(), out_raw=(), chip=(), out_chip=(), out_smem=(), out_vmem=False, flops=2000000, limit=16):
    single = not isinstance(out_shape, tuple)
    outs = (out_shape,) if single else out_shape
    held = [
        x if i < scalars or i in chip else pltpu.with_memory_space_constraint(x, pltpu.HBM)
        for i, x in enumerate(args)
    ]
    placed = tuple(o if i in out_chip or i in out_smem else pltpu.HBM(o.shape, o.dtype) for i, o in enumerate(outs))
    if out_vmem:
        placed = tuple(pltpu.VMEM(o.shape, o.dtype) for o in outs)
    specs = tuple(ANY if i in out_raw else SMEM if i in out_smem else VMEM for i in range(len(outs)))
    return pl.pallas_call(
        kernel,
        out_shape=placed[0] if single else placed,
        in_specs=[SMEM if i < scalars else ANY if i in raw else VMEM for i in range(len(args))],
        out_specs=specs[0] if single else specs,
        scratch_shapes=list(scratch),
        compiler_params=pltpu.CompilerParams(vmem_limit_bytes=limit * 1024 * 1024),
        cost_estimate=pl.CostEstimate(flops=flops, bytes_accessed=1 << 20, transcendentals=0),
    )(*held)


def shards(background, interp, beam, observed, cell_block, sweep_count):
    radar_count = lax.axis_size("radar")
    tile_count = lax.axis_size("tile")
    devices = radar_count * tile_count
    width_x, levels, width_y = background.shape[1:]
    slots = interp.shape[0] // devices
    gate_size = interp.shape[1]
    rows = width_x * levels
    height = -(-(3 * slots + 2) // 8) * 8
    total_cells = float(3 * rows * width_y * devices)
    total_gates = float(interp.shape[0] * devices * gate_size)
    field = background.reshape(3, rows, width_y)
    lanes = -(-devices * slots // LANES) * LANES
    asked = call(ask_kernel, shape(devices, 1, lanes, dtype=jnp.int32), (cell_block.reshape(1, -1),), chip=(0,))
    asked = exchange(asked)

    edges = (shape(8, rows), shape(8, rows))
    row_edges = (shape(4, levels, width_y), shape(4, levels, width_y))
    grid = shape(3, rows, width_y)
    line_out = shape(8, LANES)
    side = pltpu.VMEM((rows, LANES), F32)
    whole = pltpu.VMEM((3, rows, width_y), F32)
    plane = pltpu.VMEM((rows, width_y), F32)
    ring = pltpu.VMEM((rows + 2 * levels, width_y), F32)
    strip = pltpu.VMEM((levels, width_y), F32)
    semaphores = pltpu.SemaphoreType.DMA
    places = pltpu.SMEM((devices, lanes), jnp.int32)

    def row_halo(up, down):
        above = shifted(down, "tile", 1)
        below = shifted(up, "tile", -1)
        return above, below

    def halo(left, right, up, down):
        from_left = shifted(right, "radar", 1)
        from_right = shifted(left, "radar", -1)
        return (from_left, from_right) + row_halo(up, down)

    def edges_of(values):
        out = call(
            functools.partial(streamed_edges_kernel, levels),
            edges + row_edges,
            (values,),
            (side, whole, semaphores((PARTS,))),
            raw=(0,),
        )
        return halo(*out)

    around = edges_of(field)
    around_0 = around
    cells = call(
        functools.partial(pick_kernel, slots, levels),
        shape(devices, height, LANES, dtype=BF16),
        (asked, field),
        (pltpu.VMEM((devices, height, LANES), F32), places, semaphores),
        chip=(0, 1),
        raw=(0,),
    )
    cells = exchange(cells)
    products = (
        pltpu.VMEM((slots, devices * height, LANES), F32),
        pltpu.VMEM((slots, devices * height, LANES), F32),
        pltpu.VMEM((devices * height, LANES), F32),
    )
    weights, sight = call(
        functools.partial(source_kernel, slots),
        (shape(*interp.shape, dtype=BF16), shape(4 * slots, devices, gate_size)),
        (interp, beam.transpose(1, 0, 2), observed, sweep_count),
        (
            pltpu.VMEM((3,) + observed.shape, BF16),
            pltpu.VMEM(observed.shape, BF16),
            pltpu.VMEM(sweep_count.shape, jnp.int32),
            pltpu.VMEM((4,) + observed.shape, F32),
            semaphores((4,)),
        ),
        raw=(0, 1, 2, 3),
        out_vmem=True,
    )
    returned, misfit = call(
        functools.partial(first_source_kernel, slots),
        (shape(devices, height, LANES, dtype=BF16), shape(slots, devices, LANES)),
        (cells, weights, sight),
        products,
        chip=(0, 1, 2),
        out_chip=(1,),
    )
    returned = exchange(returned)
    push, spread, spread_cost = call(
        functools.partial(first_cycle_kernel, levels, slots),
        (grid, shape(rows, width_y), line_out),
        (field,) + around + (cells,),
        (whole, whole, ring, side, side, strip, semaphores((3, PARTS))),
        chip=(1, 2, 3, 4, 5),
        raw=(0,),
        out_raw=(0, 1),
        out_chip=(2,),
    )
    given = -(-(3 * slots + SPLIT + 2 + 2 * rows // LANES) // 8) * 8
    gradient, give, *sides = call(
        functools.partial(first_owner_kernel, slots, levels),
        (grid, shape(devices, given, LANES, dtype=BF16)) + edges + row_edges,
        (asked, returned, push, spread_cost),
        (whole, whole, places, side, pltpu.VMEM((devices, given, LANES), F32), semaphores((width_x + 2,))),
        chip=(0, 1, 3),
        raw=(0, 2),
        out_raw=(0,),
    )
    got = exchange(give)
    around_1 = row_halo(*sides[2:])
    returned, step, first_cost = call(
        functools.partial(second_source_kernel, slots, total_cells, total_gates),
        (shape(devices, height, LANES, dtype=BF16), line_out, line_out),
        (got, weights, sight, misfit),
        products,
        chip=(0, 1, 2, 3),
        out_chip=(1,),
    )
    returned = exchange(returned)
    rest, wind, rest_cost = call(
        functools.partial(second_cycle_kernel, levels, slots),
        (grid, grid, line_out),
        (gradient,) + around_1 + (got, field, push, spread, step),
        (whole, whole, whole, plane, ring, side, side, strip, semaphores((6, PARTS))),
        chip=(1, 2, 3, 7),
        raw=(0, 4, 5, 6),
        out_raw=(0, 1),
        out_chip=(2,),
    )
    last_rows = (shape(3, levels, width_y, dtype=BF16), shape(3, levels, width_y, dtype=BF16))
    sent = -(-(SPLIT + 5 * rows // LANES) // 8) * 8
    gradient, give, up, down = call(
        functools.partial(second_owner_kernel, slots, levels),
        (grid, shape(devices, sent, LANES, dtype=BF16)) + last_rows,
        (asked, returned, rest, rest_cost) + tuple(sides[:2]),
        (
            whole,
            places,
            side,
            pltpu.VMEM((devices, sent, LANES), F32),
            pltpu.VMEM((2, 8, rows), F32),
            semaphores((width_x + 2,)),
            semaphores((2,)),
        ),
        chip=(0, 1, 3),
        raw=(0, 2, 4, 5),
        out_chip=(0,),
    )
    sums = exchange(give)
    around_2 = row_halo(up, down)
    wind, strain, costs = call(
        functools.partial(final_kernel, levels, slots, total_cells, total_gates),
        (grid, shape(6, rows, width_y), shape(2)),
        (sums, first_cost, step, wind, gradient) + around_0 + (got,) + around_1 + around_2,
        (
            side,
            side,
            pltpu.VMEM((3, rows, width_y), F32),
            pltpu.VMEM((6, rows, width_y), F32),
            pltpu.SMEM((8, LANES), F32),
            pltpu.VMEM((2, given, LANES), BF16),
            semaphores((3, FINAL_PARTS)),
            semaphores,
            semaphores((2,)),
        ),
        chip=(0, 4, 5, 6, 7, 8, 10, 11, 12, 13),
        raw=(1, 3, 9),
        out_raw=(0, 1),
        out_smem=(2,),
    )
    return (
        wind.reshape(background.shape),
        strain.reshape(6, width_x, levels, width_y),
        costs,
    )


def solution(mesh):
    placed = (
        P(None, "tile", None, "radar"),
        P(("radar", "tile"), None, None),
        P(("radar", "tile"), None, None),
        P(("radar", "tile"), None),
        P(("radar", "tile")),
        P(("radar", "tile"), None),
    )

    return jax.shard_map(
        shards,
        mesh=mesh,
        in_specs=placed,
        out_specs=(P(None, "tile", None, "radar"), P(None, "tile", None, "radar"), P()),
        check_vma=False,
    )
```

```python
import functools

import jax
import jax.numpy as jnp
from jax import lax
from jax.experimental import pallas as pl
from jax.experimental.pallas import tpu as pltpu
from jax.sharding import PartitionSpec as P


BACKGROUND_WEIGHT = 0.5
DIVERGENCE_WEIGHT = 1.0
STEP_LENGTH = 0.3
EPSILON = 1e-06

AXES = ("radar", "tile")
LANES = 128
PARTS = 4
SPLIT = 3
FINAL_PARTS = 8
F32 = jnp.float32
BF16 = jnp.bfloat16

COL_WY, COL_WX, COL_PART, COL_WZ = 0, 1, 2, 3
COL_WIND = (COL_WX, COL_WY, COL_WZ)
ROW_WX, ROW_PART, ROW_WY, ROW_WZ = 0, 1, 2, 3
ROW_WIND = (ROW_WX, ROW_WY, ROW_WZ)
CORNERS = ((-1, -1), (-1, 1), (1, -1), (1, 1))


def exchange(x):
    return lax.all_to_all(x, AXES, split_axis=0, concat_axis=0, tiled=True)


def shifted(x, axis, step):
    size = lax.axis_size(axis)
    pairs = [(i, i + step) for i in range(size) if 0 <= i + step < size]
    return lax.ppermute(x, axis, pairs)


class Pieces:
    def __init__(self, source, target, sems, parts, at=0):
        rows = source.shape[-2]
        self.share = rows // parts
        self.copies = []
        self.seen = 0
        for i in range(parts):
            here = pl.ds(i * self.share, self.share)
            there = pl.ds(at + i * self.share, self.share)
            lead = (slice(None),) * (len(source.shape) - 2)
            self.copies.append(pltpu.make_async_copy(source.at[lead + (here,)], target.at[lead + (there,)], sems.at[i]))

    def start(self):
        for copy in self.copies:
            copy.start()
        return self

    def until(self, row):
        while self.seen < len(self.copies) and self.seen * self.share < row:
            self.copies[self.seen].wait()
            self.seen += 1

    def filled(self, row):
        while self.seen < len(self.copies) and (self.seen + 1) * self.share <= row:
            self.copies[self.seen].start()
            self.seen += 1

    def finish(self):
        for copy in self.copies:
            copy.wait()


class OutPieces(Pieces):
    def __init__(self, source, target, sems, parts, at=0):
        rows = target.shape[-2]
        self.share = rows // parts
        self.copies = []
        self.seen = 0
        for i in range(parts):
            here = pl.ds(at + i * self.share, self.share)
            there = pl.ds(i * self.share, self.share)
            lead = (slice(None),) * (len(source.shape) - 2)
            self.copies.append(pltpu.make_async_copy(source.at[lead + (here,)], target.at[lead + (there,)], sems.at[i]))


def iota(shape, dim):
    return lax.broadcasted_iota(jnp.int32, shape, dim)


def diff_levels(a, period):
    rows = a.shape[0]
    level = lax.rem(iota(a.shape, 0), jnp.int32(period))
    above = jnp.where(level == period - 1, 0.0, pltpu.roll(a, rows - 1, 0))
    below = jnp.where(level == 0, 0.0, pltpu.roll(a, 1, 0))
    return above - below


def diff_columns(a, left, right):
    width = a.shape[1]
    lane = iota(a.shape, 1)
    after = jnp.where(lane == width - 1, right, pltpu.roll(a, width - 1, 1))
    before = jnp.where(lane == 0, left, pltpu.roll(a, 1, 1))
    return after - before


def to_rows(columns):
    fill = jnp.zeros((LANES - columns.shape[0], columns.shape[1]), F32)
    return jnp.concatenate([columns, fill], axis=0).T


def sum_rows(a):
    total = a[:, :LANES]
    for start in range(LANES, a.shape[1], LANES):
        total = total + a[:, start : start + LANES]
    return jnp.sum(total, axis=0, keepdims=True)


def paired(first, second):
    half = LANES // 2
    lower = iota((1, LANES), 1) < half
    return jnp.where(lower, first + pltpu.roll(first, half, 1), second + pltpu.roll(second, half, 1))


def halves(line):
    lower = iota((1, LANES), 1) < LANES // 2
    return (
        jnp.sum(jnp.where(lower, line, 0.0), axis=1, keepdims=True),
        jnp.sum(jnp.where(lower, 0.0, line), axis=1, keepdims=True),
    )


def in_parts(line, count):
    parts = []
    for _ in range(count):
        parts.append(line.astype(BF16).astype(F32))
        line = line - parts[-1]
    return parts


def put_columns(ref, place, row, columns, lines):
    for i, column in enumerate(columns):
        for q in range(lines):
            at = row + i * lines + q
            ref[place, at : at + 1, :] = column[:, q * LANES : (q + 1) * LANES]


def take_columns(block, row, count, lines):
    return [
        jnp.concatenate([block[row + i * lines + q : row + i * lines + q + 1] for q in range(lines)], axis=1)
        for i in range(count)
    ]


def block_of(ref, place):
    return ref[pl.ds(place, 1)].reshape(ref.shape[1:]).astype(F32)


def own_place():
    return lax.axis_index("radar") * lax.axis_size("tile") + lax.axis_index("tile")


def neighbour(along_tile, along_radar):
    tile = lax.axis_index("tile") + along_tile
    radar = lax.axis_index("radar") + along_radar
    exists = (tile >= 0) & (tile < lax.axis_size("tile")) & (radar >= 0) & (radar < lax.axis_size("radar"))
    return exists, jnp.where(exists, radar * lax.axis_size("tile") + tile, own_place())


def corner_lines(w_ref, levels):
    rows, width = w_ref.shape[1], w_ref.shape[2]
    lane = iota((levels, LANES), 1)
    packed = jnp.zeros((levels, LANES), F32)
    for c, (along_tile, along_radar) in enumerate(CORNERS):
        here = slice(0, levels) if along_tile < 0 else slice(rows - levels, rows)
        lanes, at = (slice(0, LANES), 0) if along_radar < 0 else (slice(width - LANES, width), LANES - 1)
        for k in range(2):
            packed = lane_column(packed, lane, w_ref[k, here, lanes], at, 2 * c + k)
    turned = jnp.concatenate([packed, jnp.zeros((LANES - levels, LANES), F32)], axis=0).T
    return [
        turned[2 * c : 2 * c + 1] + pltpu.roll(turned[2 * c + 1 : 2 * c + 2], levels, 1) for c in range(len(CORNERS))
    ]


def corner_columns(line_from, levels):
    lines = []
    for along_tile, along_radar in CORNERS:
        exists, place = neighbour(along_tile, along_radar)
        lines.append(jnp.where(exists, line_from(place), 0.0))
    fill = jnp.zeros((LANES - len(CORNERS), LANES), F32)
    turned = jnp.concatenate(lines + [fill], axis=0).T
    return [(turned[0:levels, c : c + 1], turned[levels : 2 * levels, c : c + 1]) for c in range(len(CORNERS))]


def block_at(index, runs):
    if runs & (runs - 1) == 0:
        return lax.shift_right_logical(index, jnp.int32(runs.bit_length() - 1)), index & (runs - 1)
    return lax.div(index, jnp.int32(runs)), lax.rem(index, jnp.int32(runs))


def read_block(ref, k, row, run):
    line = ref[k, pl.ds(row, 1), :]
    out = line[:, :LANES]
    for h in range(1, ref.shape[2] // LANES):
        out = jnp.where(run == h, line[:, h * LANES : (h + 1) * LANES], out)
    return out


def lane_column(packed, lane, tile, at, to):
    moved = tile if at == to else pltpu.roll(tile, (to - at) % LANES, 1)
    return jnp.where(lane == to, moved, packed)


def streamed_edges_kernel(levels, w_hbm, left_out, right_out, up_out, down_out, scratch, w_ref, sems):
    fields = Pieces(w_hbm, w_ref, sems, PARTS).start()
    edges_kernel(levels, w_ref, left_out, right_out, up_out, down_out, scratch, fields.until)


def edges_kernel(levels, w_ref, left_out, right_out, up_out, down_out, scratch, need=lambda row: None):
    rows, width = w_ref.shape[1], w_ref.shape[2]
    lane = iota((levels, LANES), 1)
    last = slice(width - LANES, width)
    for x in range(rows // levels):
        here = slice(x * levels, (x + 1) * levels)
        need(here.stop)
        packed = jnp.where(lane < LANES // 2, w_ref[1, here, :LANES], w_ref[1, here, last])
        packed = lane_column(packed, lane, w_ref[0, here, :LANES], 0, 2)
        packed = lane_column(packed, lane, w_ref[2, here, :LANES], 0, 3)
        packed = lane_column(packed, lane, w_ref[0, here, last], LANES - 1, LANES - 3)
        packed = lane_column(packed, lane, w_ref[2, here, last], LANES - 1, LANES - 4)
        scratch[here, :] = packed
    turned = scratch[...].T
    place = iota((1, rows), 1)
    level = lax.rem(place, jnp.int32(levels))

    def partial(wx, wz):
        part = jnp.where(level == levels - 1, 0.0, pltpu.roll(wz, rows - 1, 1))
        part = part - jnp.where(level == 0, 0.0, pltpu.roll(wz, 1, 1))
        part = part + jnp.where(place >= rows - levels, 0.0, pltpu.roll(wx, rows - levels, 1))
        return part - jnp.where(place < levels, 0.0, pltpu.roll(wx, levels, 1))

    near, far = turned[0:8], turned[LANES - 8 : LANES]
    for out, wy, inner, wx, wz in (
        (left_out, near[0:1], near[1:2], near[2:3], near[3:4]),
        (right_out, far[7:8], -far[6:7], far[5:6], far[4:5]),
    ):
        out[...] = jnp.zeros_like(out)
        out[COL_WY : COL_WY + 1, :] = wy
        out[COL_WX : COL_WX + 1, :] = wx
        out[COL_PART : COL_PART + 1, :] = 0.5 * (inner + partial(wx, wz))
        out[COL_WZ : COL_WZ + 1, :] = wz
    for out, first in ((up_out, 0), (down_out, rows - levels)):
        here = slice(first, first + levels)
        part = diff_levels(w_ref[2, here, :], levels) + diff_columns(w_ref[1, here, :], 0.0, 0.0)
        if first > 0:
            part = part - w_ref[0, first - levels : first, :]
        else:
            part = part + w_ref[0, levels : 2 * levels, :]
        out[ROW_WX] = w_ref[0, here, :]
        out[ROW_PART] = 0.5 * part
        out[ROW_WY] = w_ref[1, here, :]
        out[ROW_WZ] = w_ref[2, here, :]


def cycle(levels, w_ref, left, right, above_ref, below_ref, corners, ring, left_rows, right_rows, need, take_spread, take_push):
    rows, width = w_ref.shape[1], w_ref.shape[2]
    cells = rows // levels
    left_rows[...] = to_rows(left)
    right_rows[...] = to_rows(right)
    has_left = jnp.where(lax.axis_index("radar") > 0, 1.0, 0.0)
    has_right = jnp.where(lax.axis_index("radar") < lax.axis_size("radar") - 1, 1.0, 0.0)
    has_above = jnp.where(lax.axis_index("tile") > 0, 1.0, 0.0)
    has_below = jnp.where(lax.axis_index("tile") < lax.axis_size("tile") - 1, 1.0, 0.0)
    above_left, above_right, below_left, below_right = corners
    lane = iota((levels, width), 1)

    def ends(left, right):
        return jnp.where(lane == 0, -0.5 * left, jnp.where(lane == width - 1, 0.5 * right, 0.0))

    first, last = slice(0, levels), slice(rows - levels, rows)
    for x in range(cells):
        here = slice(x * levels, (x + 1) * levels)
        need(min(rows, (x + 2) * levels))
        after = w_ref[0, (x + 1) * levels : (x + 2) * levels, :] if x + 1 < cells else below_ref[ROW_WX]
        before = w_ref[0, (x - 1) * levels : x * levels, :] if x > 0 else above_ref[ROW_WX]
        spread = 0.5 * (
            (after - before)
            + diff_columns(
                w_ref[1, here, :],
                left_rows[here, COL_WY : COL_WY + 1],
                right_rows[here, COL_WY : COL_WY + 1],
            )
            + diff_levels(w_ref[2, here, :], levels)
        )
        ring[(x + 1) * levels : (x + 2) * levels, :] = spread
        take_spread(here, spread)
    above = above_ref[ROW_PART] + 0.5 * w_ref[0, first, :] + ends(above_left[1], above_right[1])
    below = below_ref[ROW_PART] - 0.5 * w_ref[0, last, :] + ends(below_left[1], below_right[1])
    ring[0:levels, :] = has_above * above
    ring[rows + levels : rows + 2 * levels, :] = has_below * below
    for x in range(cells):
        here = slice(x * levels, (x + 1) * levels)
        left = left_rows[here, COL_PART : COL_PART + 1] + 0.5 * w_ref[1, here, 0:1]
        right = right_rows[here, COL_PART : COL_PART + 1] - 0.5 * w_ref[1, here, width - 1 : width]
        if x == 0:
            left = left - 0.5 * above_left[0]
            right = right - 0.5 * above_right[0]
        if x == cells - 1:
            left = left + 0.5 * below_left[0]
            right = right + 0.5 * below_right[0]
        spread = ring[(x + 1) * levels : (x + 2) * levels, :]
        after = ring[(x + 2) * levels : (x + 3) * levels, :]
        before = ring[x * levels : (x + 1) * levels, :]
        take_push(0, here, (-0.5 * DIVERGENCE_WEIGHT) * (after - before))
        take_push(1, here, (-0.5 * DIVERGENCE_WEIGHT) * diff_columns(spread, has_left * left, has_right * right))
        take_push(2, here, (-0.5 * DIVERGENCE_WEIGHT) * diff_levels(spread, levels))


def first_cycle_kernel(levels, slots, w_hbm, left_ref, right_ref, above_ref, below_ref, cells_ref, push_hbm, spread_hbm, total_out, w_ref, push, ring, left_rows, right_rows, total, sems):
    fields = Pieces(w_hbm, w_ref, sems.at[0], PARTS).start()
    total[...] = jnp.zeros_like(total)
    spreads = OutPieces(ring, spread_hbm, sems.at[1], PARTS, levels)
    pushes = OutPieces(push, push_hbm, sems.at[2], PARTS)

    def line_from(place):
        block = cells_ref[pl.ds(place, 1)].reshape(cells_ref.shape[1:]).astype(F32)
        first = block[3 * slots : 3 * slots + 1]
        return first + pltpu.roll(first, LANES // 2, 1) + block[3 * slots + 1 : 3 * slots + 2]

    def take_spread(here, spread):
        total[...] += spread * spread
        spreads.filled(here.stop)

    def take_push(k, here, value):
        push[k, here, :] = value
        if k == 2:
            pushes.filled(here.stop)

    corners = corner_columns(line_from, levels)
    cycle(levels, w_ref, left_ref[...], right_ref[...], above_ref, below_ref, corners, ring, left_rows, right_rows, fields.until, take_spread, take_push)
    total_out[...] = jnp.broadcast_to(0.5 * DIVERGENCE_WEIGHT * sum_rows(total[...]), total_out.shape)
    spreads.finish()
    pushes.finish()


def second_cycle_kernel(levels, slots, w_hbm, above_ref, below_ref, got_ref, background_hbm, push_hbm, spread_hbm, step_ref, rest_hbm, wind_hbm, total_out, w_ref, background, push, spread, ring, left_rows, right_rows, total, sems):
    fields = Pieces(w_hbm, w_ref, sems.at[0], PARTS).start()
    spreads = Pieces(spread_hbm, spread, sems.at[1], PARTS).start()
    pushes = Pieces(push_hbm, push, sems.at[2], PARTS).start()
    backgrounds = Pieces(background_hbm, background, sems.at[3], PARTS).start()
    rests = OutPieces(push, rest_hbm, sems.at[4], PARTS)
    winds = OutPieces(background, wind_hbm, sems.at[5], PARTS)
    total[...] = jnp.zeros_like(total)
    step = step_ref[0:1, 0:1]

    def line_from(place):
        block = block_of(got_ref, place)
        first = block[3 * slots + SPLIT : 3 * slots + SPLIT + 1]
        return first + pltpu.roll(first, LANES // 2, 1) + block[3 * slots + SPLIT + 1 : 3 * slots + SPLIT + 2]

    lines = w_ref.shape[1] // LANES
    sides = []
    for along_radar in (-1, 1):
        exists, place = neighbour(0, along_radar)
        wy, part = take_columns(block_of(got_ref, place), 3 * slots + SPLIT + 2, 2, lines)
        fill = jnp.zeros_like(wy)
        columns = [fill] * 8
        columns[COL_WY], columns[COL_PART] = jnp.where(exists, wy, 0.0), jnp.where(exists, part, 0.0)
        sides.append(jnp.concatenate(columns, axis=0))

    def take_spread(here, bent):
        spreads.until(here.stop)
        value = spread[here, :] - step * bent
        total[...] += (0.5 * DIVERGENCE_WEIGHT) * (value * value)

    def take_push(k, here, bent):
        pushes.until(here.stop)
        backgrounds.until(here.stop)
        offset = step * w_ref[k, here, :]
        total[...] += (0.5 * BACKGROUND_WEIGHT) * (offset * offset)
        background[k, here, :] = background[k, here, :] - offset
        push[k, here, :] = push[k, here, :] - (BACKGROUND_WEIGHT * offset + step * bent)
        if k == 2:
            rests.filled(here.stop)
            winds.filled(here.stop)

    corners = corner_columns(line_from, levels)
    cycle(levels, w_ref, *sides, above_ref, below_ref, corners, ring, left_rows, right_rows, fields.until, take_spread, take_push)
    total_out[...] = jnp.broadcast_to(sum_rows(total[...]), total_out.shape)
    rests.finish()
    winds.finish()


def for_slots(count, body, step=16):
    step = min(step, count)

    def run(i, carry):
        for j in range(step):
            body(i * step + j)
        return carry

    lax.fori_loop(0, count // step, run, 0)


def ask_kernel(places_ref, out_ref):
    line = places_ref[...]
    if line.shape[1] < out_ref.shape[2]:
        line = jnp.concatenate([line, jnp.zeros((1, out_ref.shape[2] - line.shape[1]), jnp.int32)], axis=1)
    out_ref[...] = jnp.broadcast_to(line[None], out_ref.shape)


def ask(asked_hbm, asked_ref, sem):
    return pltpu.make_async_copy(asked_hbm.at[:, 0, :], asked_ref, sem)


def pick_kernel(slots, levels, asked_hbm, w_ref, out_ref, rows_ref, asked_ref, ask_sem):
    asking = ask(asked_hbm, asked_ref, ask_sem)
    asking.start()
    me = own_place()
    runs = w_ref.shape[2] // LANES
    rows_ref[...] = jnp.zeros_like(rows_ref)
    asking.wait()

    def one(s):
        for p in range(slots):
            row, run = block_at(asked_ref[s, me * slots + p], runs)
            for k in range(3):
                rows_ref[s, 3 * p + k : 3 * p + k + 1, :] = read_block(w_ref, k, row, run)

    for_slots(out_ref.shape[0], one)
    for (along_tile, along_radar), line in zip(CORNERS, corner_lines(w_ref, levels)):
        exists, place = neighbour(along_tile, along_radar)
        high = line.astype(BF16).astype(F32)
        middle = (line - high).astype(BF16).astype(F32)

        @pl.when(exists)
        def _():
            rows_ref[place, 3 * slots : 3 * slots + 1, :] = high + pltpu.roll(middle, LANES // 2, 1)
            rows_ref[place, 3 * slots + 1 : 3 * slots + 2, :] = line - high - middle

    out_ref[...] = rows_ref[...].astype(out_ref.dtype)


def source_kernel(slots, weights_hbm, beam_hbm, observed_hbm, count_hbm, weights_out, sight_out, beam_ref, observed_ref, count_ref, wide_ref, sems):
    pairs = (
        (count_hbm, count_ref),
        (beam_hbm, beam_ref),
        (observed_hbm, observed_ref),
        (weights_hbm, weights_out),
    )
    copies = [pltpu.make_async_copy(source, target, sems.at[i]) for i, (source, target) in enumerate(pairs)]
    for copy in copies:
        copy.start()
    sources = sight_out.shape[1]
    diagonal = iota((sources, sources), 0) == iota((sources, sources), 1)
    for copy in copies[:3]:
        copy.wait()
    counts = jnp.sum(jnp.where(diagonal, count_ref[...].astype(F32), 0.0), axis=1, keepdims=True)
    for k in range(4):
        wide_ref[k] = (beam_ref[k] if k < 3 else observed_ref[...]).astype(F32)
        for p in range(slots):
            live = jnp.where(counts > p, wide_ref[k, pl.ds(p, sources, stride=slots), :], 0.0)
            sight_out[3 * p + k if k < 3 else 3 * slots + p] = live
    copies[3].wait()


def project(cells_of, weights_ref, proj_ref, sources, slots, height):
    def one(s):
        weights = weights_ref[pl.ds(s * slots, slots)].reshape(slots * LANES, LANES)
        seen = lax.dot_general(cells_of(s), weights, (((1,), (1,)), ((), ())), preferred_element_type=F32)
        here = pl.ds(pl.multiple_of(s * height, height), height)
        for p in range(slots):
            proj_ref[p, here, :] = seen[:, p * LANES : (p + 1) * LANES]

    for_slots(sources, one, 32)


def radial(proj_ref, sight_ref, p, sources, height):
    total = jnp.zeros((sources, LANES), F32)
    for k in range(3):
        total = total + sight_ref[3 * p + k] * proj_ref[p, pl.ds(3 * p + k, sources, stride=height), :]
    return total


def give_back(misfits, weights_ref, sight_ref, adj_ref, line_ref, out_ref, sources, slots, height):
    adj_ref[...] = jnp.zeros_like(adj_ref)
    cost = jnp.zeros((sources, LANES), F32)
    for p in range(slots):
        cost = cost + 0.5 * (misfits[p] * misfits[p])
        for k in range(3):
            adj_ref[p, pl.ds(3 * p + k, sources, stride=height), :] = sight_ref[3 * p + k] * misfits[p]
    high = cost.astype(BF16).astype(F32)
    line_ref[...] = jnp.zeros_like(line_ref)
    line_ref[pl.ds(3 * slots, sources, stride=height), :] = high
    line_ref[pl.ds(3 * slots + 1, sources, stride=height), :] = cost - high

    def one(s):
        weights = weights_ref[pl.ds(s * slots, slots)].reshape(slots * LANES, LANES)
        here = pl.ds(pl.multiple_of(s * height, height), height)
        adjoint = jnp.concatenate([adj_ref[p, here, :] for p in range(slots)], axis=1).astype(BF16)
        product = lax.dot_general(adjoint, weights, (((1,), (0,)), ((), ())), preferred_element_type=F32)
        out_ref[s] = (product + line_ref[here, :]).astype(out_ref.dtype)

    for_slots(sources, one, 32)


def first_source_kernel(slots, cells_ref, weights_ref, sight_ref, returned_out, misfit_out, proj_ref, adj_ref, line_ref):
    sources, height = cells_ref.shape[0], cells_ref.shape[1]
    project(lambda s: cells_ref[s].astype(BF16), weights_ref, proj_ref, sources, slots, height)
    misfits = []
    for p in range(slots):
        misfit = radial(proj_ref, sight_ref, p, sources, height) - sight_ref[3 * slots + p]
        misfit_out[p] = misfit
        misfits.append(misfit)
    give_back(misfits, weights_ref, sight_ref, adj_ref, line_ref, returned_out, sources, slots, height)


def second_source_kernel(slots, total_cells, total_gates, got_ref, weights_ref, sight_ref, misfit_ref, returned_out, step_out, cost_out, proj_ref, adj_ref, line_ref):
    sources, height = returned_out.shape[0], returned_out.shape[1]
    project(lambda s: got_ref[s, 0:height], weights_ref, proj_ref, sources, slots, height)
    squares, costs = halves(
        jnp.sum(jnp.sum(got_ref[:, 3 * slots : 3 * slots + SPLIT, :].astype(F32), axis=0), axis=0, keepdims=True)
    )
    step = STEP_LENGTH / jnp.sqrt(squares / total_cells + EPSILON)
    step_out[...] = jnp.broadcast_to(step, step_out.shape)
    cost_out[...] = jnp.broadcast_to(costs / total_gates, cost_out.shape)
    misfits = [
        misfit_ref[p] - step * radial(proj_ref, sight_ref, p, sources, height) for p in range(slots)
    ]
    give_back(misfits, weights_ref, sight_ref, adj_ref, line_ref, returned_out, sources, slots, height)


def scatter_rows(slots, asked_ref, returned_ref, out_ref):
    me = own_place()
    runs = out_ref.shape[2] // LANES
    place = iota((8, LANES), 0)

    def one(s):
        block = returned_ref[s].astype(F32)
        for p in range(slots):
            row, run = block_at(asked_ref[s, me * slots + p], runs)
            within = lax.rem(row, jnp.int32(8))
            base = pl.multiple_of(row - within, 8)
            lanes = pl.ds(pl.multiple_of(run * LANES, LANES), LANES)
            held = [out_ref[k, pl.ds(base, 8), lanes] for k in range(3)]
            for k in range(3):
                line = block[3 * p + k : 3 * p + k + 1, :]
                held[k] = held[k] + jnp.where(place == within, line, 0.0)
            for k in range(3):
                out_ref[k, pl.ds(base, 8), lanes] = held[k]

    for_slots(returned_ref.shape[0], one)


def gather_gradient(slots, levels, asked_hbm, asked_ref, returned_ref, rest_hbm, rest, gradient_ref, gradient_hbm, sems):
    rows, width = gradient_ref.shape[1], gradient_ref.shape[2]
    cells = rows // levels
    copy = pltpu.make_async_copy(rest_hbm, rest, sems.at[cells])
    asking = ask(asked_hbm, asked_ref, sems.at[cells + 1])
    asking.start()
    copy.start()
    gradient_ref[...] = jnp.zeros_like(gradient_ref)
    asking.wait()
    scatter_rows(slots, asked_ref, returned_ref, gradient_ref)
    copy.wait()
    total = jnp.zeros((levels, width), F32)
    copies = []
    for x in range(cells):
        here = slice(x * levels, (x + 1) * levels)
        for k in range(3):
            piece = gradient_ref[k, here, :] + rest[k, here, :]
            gradient_ref[k, here, :] = piece
            total = total + piece * piece
        if gradient_hbm is not None:
            copies.append(pltpu.make_async_copy(gradient_ref.at[:, here], gradient_hbm.at[:, here], sems.at[x]))
            copies[-1].start()
    return sum_rows(total), copies


def seen_cost(returned_ref, slots):
    cost = returned_ref[:, 3 * slots : 3 * slots + 2, :].astype(F32)
    return jnp.sum(jnp.sum(cost, axis=0), axis=0, keepdims=True)


def first_owner_kernel(slots, levels, asked_hbm, returned_ref, push_hbm, spread_cost_ref, gradient_hbm, give_out, left_out, right_out, up_out, down_out, push, gradient, asked_ref, scratch, give_ref, sems):
    squares, copies = gather_gradient(
        slots, levels, asked_hbm, asked_ref, returned_ref, push_hbm, push, gradient, gradient_hbm, sems
    )
    sources = give_out.shape[0]
    sums = paired(squares, seen_cost(returned_ref, slots) + spread_cost_ref[0:1, :])
    give_ref[...] = jnp.zeros_like(give_ref)
    for i, part in enumerate(in_parts(sums, SPLIT)):
        give_ref[:, 3 * slots + i, :] = jnp.broadcast_to(part, (sources, LANES))
    me = own_place()
    runs = gradient.shape[2] // LANES

    def one(s):
        for p in range(slots):
            row, run = block_at(asked_ref[s, me * slots + p], runs)
            for k in range(3):
                give_ref[s, 3 * p + k : 3 * p + k + 1, :] = read_block(gradient, k, row, run)

    for_slots(sources, one)
    for (along_tile, along_radar), line in zip(CORNERS, corner_lines(gradient, levels)):
        exists, place = neighbour(along_tile, along_radar)
        high, middle, low = in_parts(line, 3)

        @pl.when(exists)
        def _():
            row = 3 * slots + SPLIT
            give_ref[place, row : row + 1, :] = high + pltpu.roll(middle, LANES // 2, 1)
            give_ref[place, row + 1 : row + 2, :] = low

    edges_kernel(levels, gradient, left_out, right_out, up_out, down_out, scratch)
    lines = gradient.shape[1] // LANES
    for along_radar, ref in ((-1, left_out), (1, right_out)):
        exists, place = neighbour(0, along_radar)

        @pl.when(exists)
        def _():
            columns = [ref[f : f + 1, :] for f in (COL_WY, COL_PART)]
            put_columns(give_ref, place, 3 * slots + SPLIT + 2, columns, lines)

    give_out[...] = give_ref[...].astype(BF16)
    for copy in copies:
        copy.wait()


def second_owner_kernel(slots, levels, asked_hbm, returned_ref, rest_hbm, rest_cost_ref, left_hbm, right_hbm, gradient_out, give_out, up_out, down_out, rest, asked_ref, scratch, give_ref, bent_ref, sems, bent_sems):
    rows, width = gradient_out.shape[1], gradient_out.shape[2]
    bents = [
        pltpu.make_async_copy(source, bent_ref.at[i], bent_sems.at[i]) for i, source in enumerate((left_hbm, right_hbm))
    ]
    for copy in bents:
        copy.start()
    squares, _ = gather_gradient(
        slots, levels, asked_hbm, asked_ref, returned_ref, rest_hbm, rest, gradient_out, None, sems
    )
    sums = paired(squares, seen_cost(returned_ref, slots) + rest_cost_ref[0:1, :])
    give_ref[...] = jnp.zeros_like(give_ref)
    for i, part in enumerate(in_parts(sums, SPLIT)):
        give_ref[:, i, :] = jnp.broadcast_to(part, (give_ref.shape[0], LANES))
    for k in range(3):
        up_out[k] = gradient_out[k, 0:levels, :].astype(BF16)
        down_out[k] = gradient_out[k, rows - levels : rows, :].astype(BF16)
    lane = iota((levels, LANES), 1)
    for x in range(rows // levels):
        here = slice(x * levels, (x + 1) * levels)
        packed = jnp.zeros((levels, LANES), F32)
        for k in range(3):
            packed = lane_column(packed, lane, gradient_out[k, here, :LANES], 0, k)
            packed = lane_column(packed, lane, gradient_out[k, here, width - LANES :], LANES - 1, LANES - 8 + k)
        scratch[here, :] = packed
    turned = scratch[...].T
    lines = rows // LANES
    for copy in bents:
        copy.wait()
    for i, (along_radar, first) in enumerate(((-1, 0), (1, LANES - 8))):
        exists, place = neighbour(0, along_radar)

        @pl.when(exists)
        def _():
            columns = [turned[first + k : first + k + 1] for k in range(3)]
            columns += [bent_ref[i, f : f + 1, :] for f in (COL_WX, COL_WZ)]
            put_columns(give_ref, place, SPLIT, columns, lines)

    give_out[...] = give_ref[...].astype(BF16)


def final_kernel(levels, slots, total_cells, total_gates, sums_ref, first_cost_hbm, step_hbm, wind_hbm, gradient_ref, left_0, right_0, above_0, below_0, got_hbm, above_1, below_1, above_ref, below_ref, wind_out, strain_out, cost_out, left_rows, right_rows, wind, strain, first_cost_ref, step_ref, got_ref, sems, cost_sem, step_sem, got_sems):
    rows = gradient_ref.shape[1]
    cells = rows // levels
    winds = Pieces(wind_hbm, wind, sems.at[0], FINAL_PARTS).start()
    cost_copy = pltpu.make_async_copy(first_cost_hbm, first_cost_ref, cost_sem)
    cost_copy.start()
    step_copy = pltpu.make_async_copy(step_hbm, step_ref, step_sem)
    step_copy.start()
    got_copies = []
    for i, along_radar in enumerate((-1, 1)):
        _, place = neighbour(0, along_radar)
        got_copies.append(pltpu.make_async_copy(got_hbm.at[place], got_ref.at[i], got_sems.at[i]))
        got_copies[-1].start()
    wind_outs = OutPieces(wind, wind_out, sems.at[1], FINAL_PARTS)
    strain_outs = OutPieces(strain, strain_out, sems.at[2], FINAL_PARTS)
    squares, cost = halves(jnp.sum(jnp.sum(sums_ref[:, 0:SPLIT, :].astype(F32), axis=0), axis=0, keepdims=True))
    step = STEP_LENGTH / jnp.sqrt(squares / total_cells + EPSILON)
    cost_out[1] = (cost / total_gates)[0, 0]
    step_copy.wait()
    first_step = step_ref[0:1, 0:1]
    lines = rows // LANES
    for copy in got_copies:
        copy.wait()
    for i, (along_radar, out, background) in enumerate(((-1, left_rows, left_0), (1, right_rows, right_0))):
        exists, place = neighbour(0, along_radar)
        *sent, bent_x, bent_z = take_columns(block_of(sums_ref, place), SPLIT, 5, lines)
        (bent_y,) = take_columns(got_ref[i].astype(F32), 3 * slots + SPLIT + 2, 1, lines)
        columns = []
        for k, bent in enumerate((bent_x, bent_y, bent_z)):
            change = jnp.where(exists, first_step * bent + step * sent[k], 0.0)
            columns.append(background[COL_WIND[k] : COL_WIND[k] + 1, :] - change)
        out[...] = to_rows(jnp.concatenate(columns + [jnp.zeros((5, rows), F32)], axis=0))

    def settle(x):
        here = slice(x * levels, (x + 1) * levels)
        winds.until(here.stop)
        for k in range(3):
            wind[k, here, :] = wind[k, here, :] - step * gradient_ref[k, here, :]
        wind_outs.filled(here.stop)

    settle(0)
    for x in range(cells):
        here = slice(x * levels, (x + 1) * levels)
        if x + 1 < cells:
            settle(x + 1)
        along = []
        for k in range(3):
            value = wind[k, here, :]
            if x + 1 < cells:
                after = wind[k, (x + 1) * levels : (x + 2) * levels, :]
            else:
                after = below_0[ROW_WIND[k]] - first_step * below_1[ROW_WIND[k]] - step * below_ref[k].astype(F32)
            if x > 0:
                before = wind[k, (x - 1) * levels : x * levels, :]
            else:
                before = above_0[ROW_WIND[k]] - first_step * above_1[ROW_WIND[k]] - step * above_ref[k].astype(F32)
            left = left_rows[here, k : k + 1]
            right = right_rows[here, k : k + 1]
            along.append((after - before, diff_columns(value, left, right), diff_levels(value, levels)))
        (xx, xy, xz), (yx, yy, yz), (zx, zy, zz) = along
        strain[0, here, :] = 0.5 * xx
        strain[1, here, :] = 0.5 * yy
        strain[2, here, :] = 0.5 * zz
        strain[3, here, :] = 0.25 * (xy + yx)
        strain[4, here, :] = 0.25 * (xz + zx)
        strain[5, here, :] = 0.25 * (yz + zy)
        strain_outs.filled(here.stop)
    cost_copy.wait()
    cost_out[0] = first_cost_ref[0, 0]
    wind_outs.finish()
    strain_outs.finish()


def shape(*dims, dtype=F32):
    return jax.ShapeDtypeStruct(dims, dtype)


VMEM = pl.BlockSpec(memory_space=pltpu.VMEM)
SMEM = pl.BlockSpec(memory_space=pltpu.SMEM)
ANY = pl.BlockSpec(memory_space=pl.ANY)


def call(kernel, out_shape, args, scratch=(), scalars=0, raw=(), out_raw=(), chip=(), out_chip=(), out_smem=(), out_vmem=False, flops=2000000, limit=16):
    single = not isinstance(out_shape, tuple)
    outs = (out_shape,) if single else out_shape
    held = [
        x if i < scalars or i in chip else pltpu.with_memory_space_constraint(x, pltpu.HBM)
        for i, x in enumerate(args)
    ]
    placed = tuple(o if i in out_chip or i in out_smem else pltpu.HBM(o.shape, o.dtype) for i, o in enumerate(outs))
    if out_vmem:
        placed = tuple(pltpu.VMEM(o.shape, o.dtype) for o in outs)
    specs = tuple(ANY if i in out_raw else SMEM if i in out_smem else VMEM for i in range(len(outs)))
    return pl.pallas_call(
        kernel,
        out_shape=placed[0] if single else placed,
        in_specs=[SMEM if i < scalars else ANY if i in raw else VMEM for i in range(len(args))],
        out_specs=specs[0] if single else specs,
        scratch_shapes=list(scratch),
        compiler_params=pltpu.CompilerParams(vmem_limit_bytes=limit * 1024 * 1024),
        cost_estimate=pl.CostEstimate(flops=flops, bytes_accessed=1 << 20, transcendentals=0),
    )(*held)


def shards(background, interp, beam, observed, cell_block, sweep_count):
    radar_count = lax.axis_size("radar")
    tile_count = lax.axis_size("tile")
    devices = radar_count * tile_count
    width_x, levels, width_y = background.shape[1:]
    slots = interp.shape[0] // devices
    gate_size = interp.shape[1]
    rows = width_x * levels
    height = -(-(3 * slots + 2) // 8) * 8
    total_cells = float(3 * rows * width_y * devices)
    total_gates = float(interp.shape[0] * devices * gate_size)
    field = background.reshape(3, rows, width_y)
    lanes = -(-devices * slots // LANES) * LANES
    asked = call(ask_kernel, shape(devices, 1, lanes, dtype=jnp.int32), (cell_block.reshape(1, -1),), chip=(0,))
    asked = exchange(asked)

    edges = (shape(8, rows), shape(8, rows))
    row_edges = (shape(4, levels, width_y), shape(4, levels, width_y))
    grid = shape(3, rows, width_y)
    line_out = shape(8, LANES)
    side = pltpu.VMEM((rows, LANES), F32)
    whole = pltpu.VMEM((3, rows, width_y), F32)
    plane = pltpu.VMEM((rows, width_y), F32)
    ring = pltpu.VMEM((rows + 2 * levels, width_y), F32)
    strip = pltpu.VMEM((levels, width_y), F32)
    semaphores = pltpu.SemaphoreType.DMA
    places = pltpu.SMEM((devices, lanes), jnp.int32)

    def row_halo(up, down):
        above = shifted(down, "tile", 1)
        below = shifted(up, "tile", -1)
        return above, below

    def halo(left, right, up, down):
        from_left = shifted(right, "radar", 1)
        from_right = shifted(left, "radar", -1)
        return (from_left, from_right) + row_halo(up, down)

    def edges_of(values):
        out = call(
            functools.partial(streamed_edges_kernel, levels),
            edges + row_edges,
            (values,),
            (side, whole, semaphores((PARTS,))),
            raw=(0,),
        )
        return halo(*out)

    around = edges_of(field)
    around_0 = around
    cells = call(
        functools.partial(pick_kernel, slots, levels),
        shape(devices, height, LANES, dtype=BF16),
        (asked, field),
        (pltpu.VMEM((devices, height, LANES), F32), places, semaphores),
        chip=(0, 1),
        raw=(0,),
    )
    cells = exchange(cells)
    products = (
        pltpu.VMEM((slots, devices * height, LANES), F32),
        pltpu.VMEM((slots, devices * height, LANES), F32),
        pltpu.VMEM((devices * height, LANES), F32),
    )
    weights, sight = call(
        functools.partial(source_kernel, slots),
        (shape(*interp.shape, dtype=BF16), shape(4 * slots, devices, gate_size)),
        (interp, beam.transpose(1, 0, 2), observed, sweep_count),
        (
            pltpu.VMEM((3,) + observed.shape, BF16),
            pltpu.VMEM(observed.shape, BF16),
            pltpu.VMEM(sweep_count.shape, jnp.int32),
            pltpu.VMEM((4,) + observed.shape, F32),
            semaphores((4,)),
        ),
        raw=(0, 1, 2, 3),
        out_vmem=True,
    )
    returned, misfit = call(
        functools.partial(first_source_kernel, slots),
        (shape(devices, height, LANES, dtype=BF16), shape(slots, devices, LANES)),
        (cells, weights, sight),
        products,
        chip=(0, 1, 2),
        out_chip=(1,),
    )
    returned = exchange(returned)
    push, spread, spread_cost = call(
        functools.partial(first_cycle_kernel, levels, slots),
        (grid, shape(rows, width_y), line_out),
        (field,) + around + (cells,),
        (whole, whole, ring, side, side, strip, semaphores((3, PARTS))),
        chip=(1, 2, 3, 4, 5),
        raw=(0,),
        out_raw=(0, 1),
        out_chip=(2,),
    )
    given = -(-(3 * slots + SPLIT + 2 + 2 * rows // LANES) // 8) * 8
    gradient, give, *sides = call(
        functools.partial(first_owner_kernel, slots, levels),
        (grid, shape(devices, given, LANES, dtype=BF16)) + edges + row_edges,
        (asked, returned, push, spread_cost),
        (whole, whole, places, side, pltpu.VMEM((devices, given, LANES), F32), semaphores((width_x + 2,))),
        chip=(0, 1, 3),
        raw=(0, 2),
        out_raw=(0,),
    )
    got = exchange(give)
    around_1 = row_halo(*sides[2:])
    returned, step, first_cost = call(
        functools.partial(second_source_kernel, slots, total_cells, total_gates),
        (shape(devices, height, LANES, dtype=BF16), line_out, line_out),
        (got, weights, sight, misfit),
        products,
        chip=(0, 1, 2, 3),
        out_chip=(1,),
    )
    returned = exchange(returned)
    rest, wind, rest_cost = call(
        functools.partial(second_cycle_kernel, levels, slots),
        (grid, grid, line_out),
        (gradient,) + around_1 + (got, field, push, spread, step),
        (whole, whole, whole, plane, ring, side, side, strip, semaphores((6, PARTS))),
        chip=(1, 2, 3, 7),
        raw=(0, 4, 5, 6),
        out_raw=(0, 1),
        out_chip=(2,),
    )
    last_rows = (shape(3, levels, width_y, dtype=BF16), shape(3, levels, width_y, dtype=BF16))
    sent = -(-(SPLIT + 5 * rows // LANES) // 8) * 8
    gradient, give, up, down = call(
        functools.partial(second_owner_kernel, slots, levels),
        (grid, shape(devices, sent, LANES, dtype=BF16)) + last_rows,
        (asked, returned, rest, rest_cost) + tuple(sides[:2]),
        (
            whole,
            places,
            side,
            pltpu.VMEM((devices, sent, LANES), F32),
            pltpu.VMEM((2, 8, rows), F32),
            semaphores((width_x + 2,)),
            semaphores((2,)),
        ),
        chip=(0, 1, 3),
        raw=(0, 2, 4, 5),
        out_chip=(0,),
    )
    sums = exchange(give)
    around_2 = row_halo(up, down)
    wind, strain, costs = call(
        functools.partial(final_kernel, levels, slots, total_cells, total_gates),
        (grid, shape(6, rows, width_y), shape(2)),
        (sums, first_cost, step, wind, gradient) + around_0 + (got,) + around_1 + around_2,
        (
            side,
            side,
            pltpu.VMEM((3, rows, width_y), F32),
            pltpu.VMEM((6, rows, width_y), F32),
            pltpu.SMEM((8, LANES), F32),
            pltpu.VMEM((8, LANES), F32),
            pltpu.VMEM((2, given, LANES), BF16),
            semaphores((3, FINAL_PARTS)),
            semaphores,
            semaphores,
            semaphores((2,)),
        ),
        chip=(0, 4, 5, 6, 7, 8, 10, 11, 12, 13),
        raw=(1, 2, 3, 9),
        out_raw=(0, 1),
        out_smem=(2,),
    )
    return (
        wind.reshape(background.shape),
        strain.reshape(6, width_x, levels, width_y),
        costs,
    )


def solution(mesh):
    placed = (
        P(None, "tile", None, "radar"),
        P(("radar", "tile"), None, None),
        P(("radar", "tile"), None, None),
        P(("radar", "tile"), None),
        P(("radar", "tile")),
        P(("radar", "tile"), None),
    )

    return jax.shard_map(
        shards,
        mesh=mesh,
        in_specs=placed,
        out_specs=(P(None, "tile", None, "radar"), P(None, "tile", None, "radar"), P()),
        check_vma=False,
    )
```
